768 devices in a mesh: replica: 8 (over x, core), fsdp: 24 (over y_lo, z), tensor: 4 (over y_hi).
Axes of the slice: x: 4, y: 8 (y_hi: 4, y_lo: 2; y = y_hi * 2 + y_lo), z: 12, core: 2. Of those that a mesh axis runs over, the one named last changes fastest.
Arguments:
- pseudo_grad: bfloat16 [8, 3072, 18432], P('replica', 'fsdp', 'tensor'), may hold values from -6 to 6
- compensation: float32 [8, 3072, 18432], P('replica', 'fsdp', 'tensor'), may hold values from -6 to 6
- params: float32 [3072, 18432], P(('fsdp', 'replica'), 'tensor'), may hold values from -6 to 6
- momentum: float32 [3072, 18432], P(('fsdp', 'replica'), 'tensor'), may hold values from -6 to 6
- probe: bfloat16 [1536, 18432], P('fsdp', 'tensor'), may hold values from -0.046875 to 0.046875
Outputs:
- new_params: float32 [3072, 18432], P(('fsdp', 'replica'), 'tensor')
- new_momentum: float32 [3072, 18432], P(('fsdp', 'replica'), 'tensor')
- probe_out: bfloat16 [1536, 3072], P('tensor', 'fsdp')
The draws below stay inside these ranges and needn't reach their ends.
All inputs are finite; a program needn't handle non-finite values.
Results may differ from the reference program's by a relative error of at most 0.014.
Values may be sent and summed in bfloat16 or wider, within the bound.
A program may use at most 64 MiB of HBM per device.

```python
import jax
import jax.numpy as jnp
from jax import lax

D = 3072
FW = 18432
PROBE = 1536
N_REPLICA = 8


def steps_of(key, shape, split, smallest, high):
    def one(axis_at, parts):
        draws = jax.random.uniform(jax.random.fold_in(jax.random.fold_in(key, 6), axis_at), (parts,), jnp.float32, smallest / len(split), high / len(split))
        return jnp.repeat(jnp.exp(draws), shape[axis_at] // parts).reshape((-1,) + (1,) * (len(shape) - axis_at - 1))

    loudness = one(*split[0])
    for cut in split[1:]:
        loudness = loudness * one(*cut)
    return loudness


def centred(rng, dims, deviation, limit, shards=(), held_as=jnp.bfloat16):
    entries = jax.random.normal(rng, dims, jnp.float32) * deviation
    if len(shards) > 0:
        entries = steps_of(rng, dims, shards, -0.22, 0.18) * entries
    return jnp.clip(entries, min=-limit, max=limit).astype(held_as)


def setup_inputs(seed: int = 0) -> dict:
    key_list = jax.random.split(jax.random.key(seed), 6)
    pseudo_grad = centred(key_list[0], (N_REPLICA, D, FW), 1.0, 6.0, ((0, 8), (1, 24), (2, 4)))
    compensation = centred(key_list[1], (N_REPLICA, D, FW), 1.0, 6.0, ((0, 8), (1, 24), (2, 4)), jnp.float32)
    params = centred(key_list[2], (D, FW), 1.0, 6.0, ((0, 192), (1, 4)), jnp.float32)
    momentum = centred(key_list[3], (D, FW), 1.0, 6.0, ((0, 192), (1, 4)), jnp.float32)
    probe = centred(key_list[4], (PROBE, FW), FW ** -0.5, 0.046875, ((0, 24), (1, 4)))
    return dict(pseudo_grad=pseudo_grad, compensation=compensation, params=params, momentum=momentum, probe=probe)


outer_rate = 0.7
nesterov = 0.9


def reference(pseudo_grad, compensation, params, momentum, probe):
    def accumulate(summed, pair):
        grads, carried = pair
        outgoing = (grads.astype(jnp.float32) + carried).astype(jnp.bfloat16)
        outgoing = lax.optimization_barrier(outgoing)
        return summed + outgoing.astype(jnp.float32), None

    start = jnp.zeros(params.shape, jnp.float32)
    summed, _ = lax.scan(accumulate, start, (pseudo_grad, compensation))
    average = summed / N_REPLICA
    new_momentum = nesterov * momentum + average
    new_params = params - outer_rate * (average + nesterov * new_momentum)
    weights = new_params.astype(jnp.bfloat16)
    probe_out = lax.dot_general(probe, weights, (((1,), (1,)), ((), ())), preferred_element_type=jnp.float32)
    return new_params, new_momentum, probe_out.astype(jnp.bfloat16)
```

```python
import jax
import jax.numpy as jnp
from jax import lax
from jax.experimental import pallas as pl
from jax.experimental.pallas import tpu as pltpu
from jax.sharding import PartitionSpec as P

MESH = pl.DeviceIdType.MESH
RATE = 0.7
NEST = 0.9
F32, BF16 = jnp.float32, jnp.bfloat16

NX, NY, NZ = 4, 8, 12
K = 4608
KC = K // 4
ORDER = (("O", 0), ("P", 0), ("P", 1), ("O", 1))
N_SEM = 192


class Keys:
    def __init__(self):
        self.at = {}

    def __call__(self, *key):
        return self.at.setdefault(key, len(self.at))


def kernel(
    pg_hbm, comp_hbm, prm_hbm, mom_hbm, probe_hbm,
    new_prm_hbm, new_mom_hbm, out_hbm,
    v_pg, v_comp, out_s, cs, r_opp, r_fin, t_acc, prm, mom, q_s, sum_s,
    w, wy, pb, b_send, part, y_in, outb, n_prm, n_mom,
    send_sem, recv_sem, loc_sem,
):
    rep = lax.axis_index("replica")
    fs = lax.axis_index("fsdp")
    t = lax.axis_index("tensor")
    x, core = rep // 2, rep % 2
    lo, z = fs // NZ, fs % NZ
    y = t * 2 + lo

    def dev(x_, core_, y_, z_):
        return (x_ * 2 + core_, (y_ % 2) * NZ + z_, y_ // 2)

    def xat(d):
        return lax.rem(x + d + NX, NX)

    def yat(d):
        return lax.rem(y + d + NY, NY)

    def zat(d):
        return lax.rem(z + d + NZ, NZ)

    rk, sk, lk = Keys(), Keys(), Keys()
    pending = []

    def send(src, dst, key, to, n=0):
        cp = pltpu.make_async_remote_copy(
            src_ref=src, dst_ref=dst, send_sem=send_sem.at[sk(key, to_name(key), n)],
            recv_sem=recv_sem.at[rk(key)], device_id=to, device_id_type=MESH,
        )
        cp.start()
        pending.append(cp)

    def to_name(key):
        return key

    def arrived(dst, key):
        pltpu.make_async_remote_copy(
            src_ref=dst, dst_ref=dst, send_sem=send_sem.at[0], recv_sem=recv_sem.at[rk(key)],
            device_id=dev(x, core, y, z), device_id_type=MESH,
        ).wait_recv()

    def local(src, dst, key):
        cp = pltpu.make_async_copy(src, dst, loc_sem.at[lk(key)])
        cp.start()
        return cp

    def koff(kind, kc):
        half = lo if kind == "O" else 1 - lo
        return pl.multiple_of((half * 2 + kc) * KC, KC)

    loads = []
    for i, (kind, kc) in enumerate(ORDER):
        at = pl.ds(koff(kind, kc), KC)
        loads.append(
            (
                local(pg_hbm.at[:, :, at], v_pg.at[i], ("pg", i)),
                local(comp_hbm.at[:, :, at], v_comp.at[i], ("comp", i)),
            )
        )
    load_prm = local(prm_hbm, prm, "prm")
    load_mom = local(mom_hbm, mom, "mom")

    barrier = pltpu.get_barrier_semaphore()

    def greet(devices):
        for d in devices:
            pl.semaphore_signal(barrier, inc=1, device_id=d, device_id_type=MESH)

    @pl.when(core == 0)
    def _():
        pending.clear()
        load_b = [
            local(probe_hbm.at[x, :, pl.ds(koff(kind, kc), KC)],
                  pb.at[lo, z, kc] if kind == "O" else b_send.at[kc], ("probe", kind, kc))
            for kind in "OP" for kc in (0, 1)
        ]
        peers = [dev(x, 1, y, z), dev(x, 0, y + 1 - 2 * lo, z)]
        peers += [dev(x, 0, y, zat(d)) for d in (1, -1, 2, -2)]
        peers += [dev(xat(d), 1, y, z) for d in (1, 2, 3)]
        greet(peers)

        def outgoing(i):
            for cp in loads[i]:
                cp.wait()
            out_s[i] = (v_pg[i].astype(F32) + v_comp[i]).astype(BF16)

        outgoing(0)
        for cp in load_b:
            cp.wait()
        pl.semaphore_wait(barrier, len(peers))

        def hop(slot, typ, at, sign, kc, step):
            d = at + step
            ref = pb.at[slot[0], slot[1], kc]
            send(ref, ref, ("z", typ, sign * d, kc), dev(x, 0, y, zat(sign * step)), 0)

        own = {"A": lo, "B": 1 - lo}

        def spread(typ, at, kc):
            for sign in (1, -1):
                src = zat(-sign * at)
                if at < 4:
                    hop((own[typ], src), typ, at, sign, kc, 2)
                    hop((own[typ], src), typ, at, sign, kc, 1)
                else:
                    hop((own[typ], src), typ, at, sign, kc, 1)
                    if (kc == 0) == (sign == 1):
                        hop((own[typ], src), typ, at, sign, kc, 2)

        def wait_z(typ, d, kc):
            arrived(pb.at[own[typ], zat(-d), kc], ("z", typ, d, kc))

        def forward(typ, d):
            ref = pb.at[own[typ], zat(-d)]
            send(ref, ref, ("fw", typ, d), dev(x, 1, y, z))

        for kc in (0, 1):
            ref = pb.at[lo, z, kc]
            send(b_send.at[kc], ref, ("bx", kc), dev(x, 0, y + 1 - 2 * lo, z))
        for kc in (0, 1):
            spread("A", 0, kc)

        def push(i):
            send(out_s.at[i], out_s.at[i], ("push", i), dev(x, 1, y, z))

        push(0)
        for i in (1, 2, 3):
            outgoing(i)
            push(i)
        load_prm.wait()
        load_mom.wait()
        q_s[...] = prm[...] - (RATE * NEST * NEST) * mom[...]
        send(q_s, q_s, ("q",), dev(x, 1, y, z))
        forward("A", 0)

        for kc in (0, 1):
            arrived(pb.at[1 - lo, z, kc], ("bx", kc))
            spread("B", 0, kc)
        forward("B", 0)
        for kc in (0, 1):
            for sign in (1, -1):
                wait_z("A", 2 * sign, kc)
            spread("A", 2, kc)
        for d in (1, -1):
            for kc in (0, 1):
                wait_z("A", d, kc)
            forward("A", d)
        forward("A", 2)
        forward("A", -2)
        for kc in (0, 1):
            for sign in (1, -1):
                wait_z("B", 2 * sign, kc)
            spread("B", 2, kc)
        for d in (1, -1):
            for kc in (0, 1):
                wait_z("B", d, kc)
            forward("B", d)
        forward("B", 2)
        forward("B", -2)
        for typ in "AB":
            for kc in (0, 1):
                for sign in (1, -1):
                    wait_z(typ, 4 * sign, kc)
                spread(typ, 4, kc)
            for d in (3, -3):
                for kc in (0, 1):
                    wait_z(typ, d, kc)
                forward(typ, d)
            forward(typ, 4)
            forward(typ, -4)
        for typ in "AB":
            for d in (5, -5):
                for kc in (0, 1):
                    wait_z(typ, d, kc)
                forward(typ, d)
            wait_z(typ, 6, 0)
            wait_z(typ, -6, 1)
            forward(typ, 6)

        stores = []
        for i, (kind, kc) in enumerate(ORDER):
            at = pl.ds(koff(kind, kc), KC)
            arrived(sum_s.at[i], ("sum", i))
            average = sum_s[i]
            m = NEST * mom[:, at] + average
            n_mom[i] = m
            n_prm[i] = prm[:, at] - RATE * (average + NEST * m)
            stores.append(local(n_mom.at[i], new_mom_hbm.at[:, at], ("nm", i)))
            stores.append(local(n_prm.at[i], new_prm_hbm.at[:, at], ("np", i)))
        for d in (0, 1, 2, 3):
            arrived(outb.at[:, xat(-d)], ("out", 0, d))
        stores.append(local(outb, out_hbm, "out"))
        for cp in stores:
            cp.wait()
        for cp in pending:
            cp.wait_send()

    @pl.when(core == 1)
    def _():
        pending.clear()
        right, left = xat(1), xat(-1)
        twin = dev(x, 1, y + 1 - 2 * lo, z)
        peers = [dev(x, 0, y, z)] + [dev(xat(d), 1, y, z) for d in (1, 2, 3)]
        peers += [dev(x, 1, yat(d), z) for d in range(1, NY)]
        peers += [dev(xat(d), 0, y, z) for d in (1, 2, 3)]
        greet(peers)
        pl.semaphore_wait(barrier, len(peers))
        rdev, ldev = dev(right, 1, y, z), dev(left, 1, y, z)
        far = xat(2)

        def chip_sum(i, s):
            return v_pg[i, s].astype(F32) + v_comp[i, s] + out_s[i, s].astype(F32)

        for i in range(4):
            for cp in loads[i]:
                cp.wait()
            arrived(out_s.at[i], ("push", i))
            for side, to in ((1, rdev), (0, ldev)):
                s = far * 2 + side
                cs[i, s] = chip_sum(i, s).astype(BF16)
                send(cs.at[i, s], r_opp.at[i, side], ("opp", i, side), to)
            for side, to, xx in ((0, rdev, right), (1, ldev, left)):
                s = xx * 2 + side
                cs[i, s] = chip_sum(i, s).astype(BF16)
                send(cs.at[i, s], r_fin.at[i, side, 0], ("dir", i, side), to)

        for i in range(4):
            for side, to, xx in ((1, rdev, right), (0, ldev, left)):
                arrived(r_opp.at[i, side], ("opp", i, side))
                s = xx * 2 + side
                t_acc[i, side] = (chip_sum(i, s) + r_opp[i, side].astype(F32)).astype(BF16)
                send(t_acc.at[i, side], r_fin.at[i, side, 1], ("acc", i, side), to)

        load_prm.wait()
        load_mom.wait()
        arrived(q_s, ("q",))
        stores = []

        def gather(kc, f):
            for side, to in ((1, rdev), (0, ldev), (0, rdev), (1, ldev)):
                ref = w.at[kc, f, x, side]
                sign = "r" if to is rdev else "l"
                rel = 0 if f is lo else 1
                send(ref, ref, ("ag", kc, rel, side, sign), to)

        def relay(kc, f):
            rel = 0 if f is lo else 1
            for side, to, xx, sign in ((1, rdev, left, "r"), (0, ldev, right, "l")):
                ref = w.at[kc, f, xx, side]
                arrived(ref, ("ag", kc, rel, side, sign))
                send(ref, ref, ("ag2", kc, rel, side), to)

        for i, (kind, kc) in enumerate(ORDER):
            at = pl.ds(koff(kind, kc), KC)
            for side in (1, 0):
                for j, tag in enumerate(("dir", "acc")):
                    arrived(r_fin.at[i, side, j], (tag, i, side))
                average = (
                    chip_sum(i, x * 2 + side)
                    + r_fin[i, side, 0].astype(F32)
                    + r_fin[i, side, 1].astype(F32)
                ) * 0.125
                if side == 1:
                    m = NEST * mom[:, at] + average
                    new = prm[:, at] - RATE * (average + NEST * m)
                    n_mom[i] = m
                    n_prm[i] = new
                else:
                    sum_s[i] = average
                    new = q_s[:, at] - (RATE * (1 + NEST)) * average
                if kind == "O":
                    w[kc, lo, x, side] = new.astype(BF16)
                else:
                    wy[kc, side] = new.astype(BF16)
            if kind == "O":
                gather(kc, lo)
            else:
                send(wy.at[kc], w.at[kc, lo, x], ("wy", kc), twin)
            send(sum_s.at[i], sum_s.at[i], ("sum", i), dev(x, 0, y, z))
            stores.append(local(n_mom.at[i], new_mom_hbm.at[:, at], ("nm", i)))
            stores.append(local(n_prm.at[i], new_prm_hbm.at[:, at], ("np", i)))

        other = 1 - lo
        relay(0, lo)
        for kc in (0, 1):
            arrived(w.at[kc, other, x], ("wy", kc))
            gather(kc, other)
        relay(1, lo)
        for kc in (0, 1):
            relay(kc, other)
        for kc in (0, 1):
            for rel, f in ((0, lo), (1, other)):
                arrived(w.at[kc, f, left, 0], ("ag", kc, rel, 0, "r"))
                arrived(w.at[kc, f, right, 1], ("ag", kc, rel, 1, "l"))
                for side in (0, 1):
                    arrived(w.at[kc, f, far, side], ("ag2", kc, rel, side))
        for typ, f in (("A", lo), ("B", other)):
            for d in range(-5, 7):
                arrived(pb.at[f, zat(-d)], ("fw", typ, d))

        for lp in (0, 1):
            rows = [pb[lp, :, kc].reshape(NZ * 16, KC) for kc in (0, 1)]
            for lw in (0, 1):
                acc = jnp.zeros((NZ * 16, 128), F32)
                for kc in (0, 1):
                    acc += lax.dot_general(
                        rows[kc], w[kc, lw].reshape(128, KC), (((1,), (1,)), ((), ())),
                        preferred_element_type=F32,
                    )
                part[lw, lp] = acc.astype(BF16).reshape(2, 6, 16, 128)

        for d in (4, 3, 5, 2, 6, 1, 7):
            yy = yat(d)
            tt, ll = yy // 2, yy % 2
            send(part.at[ll, tt // 2, tt % 2], y_in.at[d], ("y", d), dev(x, 1, yy, z))
        total = part[lo, t // 2, t % 2].astype(F32)
        for d in (1, 7, 2, 6, 3, 5, 4):
            arrived(y_in.at[d], ("y", d))
            total += y_in[d].astype(F32)
        outb[:, x] = total.astype(BF16)
        for d in (2, 1, 3):
            for cc in (1, 0):
                send(outb.at[:, x], outb.at[:, x], ("out", cc, d), dev(xat(d), cc, y, z))
        send(outb.at[:, x], outb.at[:, x], ("out", 0, 0), dev(x, 0, y, z))
        for d in (1, 3, 2):
            arrived(outb.at[:, xat(-d)], ("out", 1, d))
        stores.append(local(outb, out_hbm, "out"))
        for cp in stores:
            cp.wait()
        for cp in pending:
            cp.wait_send()

    assert max(len(k.at) for k in (rk, sk, lk)) <= N_SEM


def per_device(pseudo_grad, compensation, params, momentum, probe):
    any_space = pl.BlockSpec(memory_space=pl.ANY)
    new_params, new_momentum, out = pl.pallas_call(
        kernel,
        out_shape=(
            jax.ShapeDtypeStruct((16, K), F32),
            jax.ShapeDtypeStruct((16, K), F32),
            jax.ShapeDtypeStruct((6, NX, 16, 128), BF16),
        ),
        in_specs=[any_space] * 5,
        out_specs=[any_space] * 3,
        scratch_shapes=[
            pltpu.VMEM((4, 8, 16, KC), BF16),
            pltpu.VMEM((4, 8, 16, KC), F32),
            pltpu.VMEM((4, 8, 16, KC), BF16),
            pltpu.VMEM((4, 8, 16, KC), BF16),
            pltpu.VMEM((4, 2, 16, KC), BF16),
            pltpu.VMEM((4, 2, 2, 16, KC), BF16),
            pltpu.VMEM((4, 2, 16, KC), BF16),
            pltpu.VMEM((16, K), F32),
            pltpu.VMEM((16, K), F32),
            pltpu.VMEM((16, K), F32),
            pltpu.VMEM((4, 16, KC), F32),
            pltpu.VMEM((2, 2, NX, 2, 16, KC), BF16),
            pltpu.VMEM((2, 2, 16, KC), BF16),
            pltpu.VMEM((2, NZ, 2, 16, KC), BF16),
            pltpu.VMEM((2, 16, KC), BF16),
            pltpu.VMEM((2, 2, 2, 6, 16, 128), BF16),
            pltpu.VMEM((NY, 6, 16, 128), BF16),
            pltpu.VMEM((6, NX, 16, 128), BF16),
            pltpu.VMEM((4, 16, KC), F32),
            pltpu.VMEM((4, 16, KC), F32),
            pltpu.SemaphoreType.DMA((N_SEM,)),
            pltpu.SemaphoreType.DMA((N_SEM,)),
            pltpu.SemaphoreType.DMA((N_SEM,)),
        ],
        compiler_params=pltpu.CompilerParams(
            collective_id=0, has_side_effects=True, vmem_limit_bytes=40 * 2**20
        ),
    )(
        pseudo_grad.reshape(8, 16, K),
        compensation.reshape(8, 16, K),
        params,
        momentum,
        probe.reshape(NX, 16, K),
    )
    return new_params, new_momentum, out.reshape(384, 128)


def solution(mesh):
    in_specs = (
        P("replica", "fsdp", "tensor"),
        P("replica", "fsdp", "tensor"),
        P(("fsdp", "replica"), "tensor"),
        P(("fsdp", "replica"), "tensor"),
        P("fsdp", "tensor"),
    )
    out_specs = (
        P(("fsdp", "replica"), "tensor"),
        P(("fsdp", "replica"), "tensor"),
        P("tensor", "fsdp"),
    )
    return jax.shard_map(
        per_device, mesh=mesh, in_specs=in_specs, out_specs=out_specs, check_vma=False
    )
```

```python
import jax
import jax.numpy as jnp
from jax import lax
from jax.experimental import pallas as pl
from jax.experimental.pallas import tpu as pltpu
from jax.sharding import PartitionSpec as P

MESH = pl.DeviceIdType.MESH
RATE = 0.7
NEST = 0.9
F32, BF16 = jnp.float32, jnp.bfloat16

NX, NY, NZ = 4, 8, 12
K = 4608
KC = K // 4
ORDER = (("O", 0), ("P", 0), ("P", 1), ("O", 1))
N_SEM = 192


class Keys:
    def __init__(self):
        self.at = {}

    def __call__(self, *key):
        return self.at.setdefault(key, len(self.at))


def kernel(
    pg_hbm, comp_hbm, prm_hbm, mom_hbm, probe_hbm,
    new_prm_hbm, new_mom_hbm, out_hbm,
    v_pg, v_comp, out_s, cs, r_opp, r_fin, t_acc, prm, mom, q_s, sum_s,
    w, wy, pb, b_send, part, y_in, outb, n_prm, n_mom,
    send_sem, recv_sem, loc_sem, go,
):
    rep = lax.axis_index("replica")
    fs = lax.axis_index("fsdp")
    t = lax.axis_index("tensor")
    x, core = rep // 2, rep % 2
    lo, z = fs // NZ, fs % NZ
    y = t * 2 + lo

    def dev(x_, core_, y_, z_):
        return (x_ * 2 + core_, (y_ % 2) * NZ + z_, y_ // 2)

    def xat(d):
        return lax.rem(x + d + NX, NX)

    def yat(d):
        return lax.rem(y + d + NY, NY)

    def zat(d):
        return lax.rem(z + d + NZ, NZ)

    rk, sk, lk = Keys(), Keys(), Keys()
    pending = []

    def send(src, dst, key, to, n=0):
        cp = pltpu.make_async_remote_copy(
            src_ref=src, dst_ref=dst, send_sem=send_sem.at[sk(key, to_name(key), n)],
            recv_sem=recv_sem.at[rk(key)], device_id=to, device_id_type=MESH,
        )
        cp.start()
        pending.append(cp)

    def to_name(key):
        return key

    def arrived(dst, key):
        pltpu.make_async_remote_copy(
            src_ref=dst, dst_ref=dst, send_sem=send_sem.at[0], recv_sem=recv_sem.at[rk(key)],
            device_id=dev(x, core, y, z), device_id_type=MESH,
        ).wait_recv()

    def local(src, dst, key):
        cp = pltpu.make_async_copy(src, dst, loc_sem.at[lk(key)])
        cp.start()
        return cp

    def koff(kind, kc):
        half = lo if kind == "O" else 1 - lo
        return pl.multiple_of((half * 2 + kc) * KC, KC)

    loads = []
    for i, (kind, kc) in enumerate(ORDER):
        at = pl.ds(koff(kind, kc), KC)
        loads.append(
            (
                local(pg_hbm.at[:, :, at], v_pg.at[i], ("pg", i)),
                local(comp_hbm.at[:, :, at], v_comp.at[i], ("comp", i)),
            )
        )
    load_prm = local(prm_hbm, prm, "prm")
    load_mom = local(mom_hbm, mom, "mom")

    barrier = pltpu.get_barrier_semaphore()

    def greet(devices):
        for d in devices:
            pl.semaphore_signal(barrier, inc=1, device_id=d, device_id_type=MESH)

    @pl.when(core == 1)
    def _():
        pending.clear()
        right, left = xat(1), xat(-1)
        twin = dev(x, 1, y + 1 - 2 * lo, z)
        peers = [dev(xat(d), 1, y, z) for d in (1, 2, 3)]
        peers += [dev(x, 1, yat(d), z) for d in range(1, NY)]
        greet(peers)
        pl.semaphore_wait(barrier, len(peers) + 4)
        pl.semaphore_signal(go, inc=1, device_id=dev(x, 0, y, z), device_id_type=MESH)
        rdev, ldev = dev(right, 1, y, z), dev(left, 1, y, z)
        far = xat(2)

        def chip_sum(i, s):
            return v_pg[i, s].astype(F32) + v_comp[i, s] + out_s[i, s].astype(F32)

        for i in range(4):
            for cp in loads[i]:
                cp.wait()
            arrived(out_s.at[i], ("push", i))
            for side, to in ((1, rdev), (0, ldev)):
                s = far * 2 + side
                cs[i, s] = chip_sum(i, s).astype(BF16)
                send(cs.at[i, s], r_opp.at[i, side], ("opp", i, side), to)
            for side, to, xx in ((0, rdev, right), (1, ldev, left)):
                s = xx * 2 + side
                cs[i, s] = chip_sum(i, s).astype(BF16)
                send(cs.at[i, s], r_fin.at[i, side, 0], ("dir", i, side), to)

        for i in range(4):
            for side, to, xx in ((1, rdev, right), (0, ldev, left)):
                arrived(r_opp.at[i, side], ("opp", i, side))
                s = xx * 2 + side
                t_acc[i, side] = (chip_sum(i, s) + r_opp[i, side].astype(F32)).astype(BF16)
                send(t_acc.at[i, side], r_fin.at[i, side, 1], ("acc", i, side), to)

        load_prm.wait()
        load_mom.wait()
        arrived(q_s, ("q",))
        stores = []

        def gather(kc, f):
            for side, to in ((1, rdev), (0, ldev), (0, rdev), (1, ldev)):
                ref = w.at[kc, f, x, side]
                sign = "r" if to is rdev else "l"
                rel = 0 if f is lo else 1
                send(ref, ref, ("ag", kc, rel, side, sign), to)

        def relay(kc, f):
            rel = 0 if f is lo else 1
            for side, to, xx, sign in ((1, rdev, left, "r"), (0, ldev, right, "l")):
                ref = w.at[kc, f, xx, side]
                arrived(ref, ("ag", kc, rel, side, sign))
                send(ref, ref, ("ag2", kc, rel, side), to)

        for i, (kind, kc) in enumerate(ORDER):
            at = pl.ds(koff(kind, kc), KC)
            for side in (1, 0):
                for j, tag in enumerate(("dir", "acc")):
                    arrived(r_fin.at[i, side, j], (tag, i, side))
                average = (
                    chip_sum(i, x * 2 + side)
                    + r_fin[i, side, 0].astype(F32)
                    + r_fin[i, side, 1].astype(F32)
                ) * 0.125
                if side == 1:
                    m = NEST * mom[:, at] + average
                    new = prm[:, at] - RATE * (average + NEST * m)
                    n_mom[i] = m
                    n_prm[i] = new
                else:
                    sum_s[i] = average
                    new = q_s[:, at] - (RATE * (1 + NEST)) * average
                if kind == "O":
                    w[kc, lo, x, side] = new.astype(BF16)
                else:
                    wy[kc, side] = new.astype(BF16)
            if kind == "O":
                gather(kc, lo)
            else:
                send(wy.at[kc], w.at[kc, lo, x], ("wy", kc), twin)
            send(sum_s.at[i], sum_s.at[i], ("sum", i), dev(x, 0, y, z))
            stores.append(local(n_mom.at[i], new_mom_hbm.at[:, at], ("nm", i)))
            stores.append(local(n_prm.at[i], new_prm_hbm.at[:, at], ("np", i)))

        other = 1 - lo
        relay(0, lo)
        for kc in (0, 1):
            arrived(w.at[kc, other, x], ("wy", kc))
            gather(kc, other)
        relay(1, lo)
        for kc in (0, 1):
            relay(kc, other)
        for kc in (0, 1):
            for rel, f in ((0, lo), (1, other)):
                arrived(w.at[kc, f, left, 0], ("ag", kc, rel, 0, "r"))
                arrived(w.at[kc, f, right, 1], ("ag", kc, rel, 1, "l"))
                for side in (0, 1):
                    arrived(w.at[kc, f, far, side], ("ag2", kc, rel, side))
        for typ, f in (("A", lo), ("B", other)):
            for d in range(-5, 7):
                arrived(pb.at[f, zat(-d)], ("fw", typ, d))

        for lp in (0, 1):
            rows = [pb[lp, :, kc].reshape(NZ * 16, KC) for kc in (0, 1)]
            for lw in (0, 1):
                acc = jnp.zeros((NZ * 16, 128), F32)
                for kc in (0, 1):
                    acc += lax.dot_general(
                        rows[kc], w[kc, lw].reshape(128, KC), (((1,), (1,)), ((), ())),
                        preferred_element_type=F32,
                    )
                part[lw, lp] = acc.astype(BF16).reshape(2, 6, 16, 128)

        for d in (4, 3, 5, 2, 6, 1, 7):
            yy = yat(d)
            tt, ll = yy // 2, yy % 2
            send(part.at[ll, tt // 2, tt % 2], y_in.at[d], ("y", d), dev(x, 1, yy, z))
        total = part[lo, t // 2, t % 2].astype(F32)
        for d in (1, 7, 2, 6, 3, 5, 4):
            arrived(y_in.at[d], ("y", d))
            total += y_in[d].astype(F32)
        outb[:, x] = total.astype(BF16)
        for d in (2, 1, 3):
            for cc in (1, 0):
                send(outb.at[:, x], outb.at[:, x], ("out", cc, d), dev(xat(d), cc, y, z))
        send(outb.at[:, x], outb.at[:, x], ("out", 0, 0), dev(x, 0, y, z))
        for d in (1, 3, 2):
            arrived(outb.at[:, xat(-d)], ("out", 1, d))
        stores.append(local(outb, out_hbm, "out"))
        for cp in stores:
            cp.wait()
        for cp in pending:
            cp.wait_send()

    @pl.when(core == 0)
    def _():
        pending.clear()
        load_b = [
            local(probe_hbm.at[x, :, pl.ds(koff(kind, kc), KC)],
                  pb.at[lo, z, kc] if kind == "O" else b_send.at[kc], ("probe", kind, kc))
            for kind in "OP" for kc in (0, 1)
        ]
        mate = y + 1 - 2 * lo
        greet([dev(xat(d), 1, y, z) for d in (0, 1, 2, 3)])
        peers = [dev(x, 0, mate, z)]
        peers += [dev(x, 0, yy, zat(d)) for d in (1, -1, 2, -2) for yy in (y, mate)]
        greet(peers)

        def outgoing(i):
            for cp in loads[i]:
                cp.wait()
            out_s[i] = (v_pg[i].astype(F32) + v_comp[i]).astype(BF16)

        def push(i):
            send(out_s.at[i], out_s.at[i], ("push", i), dev(x, 1, y, z))

        outgoing(0)
        pl.semaphore_wait(go, 1)
        push(0)
        for i in (1, 2, 3):
            outgoing(i)
            push(i)
        load_prm.wait()
        load_mom.wait()
        q_s[...] = prm[...] - (RATE * NEST * NEST) * mom[...]
        send(q_s, q_s, ("q",), dev(x, 1, y, z))
        for cp in load_b:
            cp.wait()
        pl.semaphore_wait(barrier, len(peers))

        def hop(slot, typ, at, sign, kc, step):
            d = at + step
            ref = pb.at[slot[0], slot[1], kc]
            send(ref, ref, ("z", typ, sign * d, kc), dev(x, 0, y, zat(sign * step)), 0)

        own = {"A": lo, "B": 1 - lo}

        def spread(typ, at, kc):
            for sign in (1, -1):
                src = zat(-sign * at)
                if at < 4:
                    hop((own[typ], src), typ, at, sign, kc, 2)
                    hop((own[typ], src), typ, at, sign, kc, 1)
                else:
                    hop((own[typ], src), typ, at, sign, kc, 1)
                    if (kc == 0) == (sign == 1):
                        hop((own[typ], src), typ, at, sign, kc, 2)

        def wait_z(typ, d, kc):
            arrived(pb.at[own[typ], zat(-d), kc], ("z", typ, d, kc))

        def forward(typ, d):
            ref = pb.at[own[typ], zat(-d)]
            send(ref, ref, ("fw", typ, d), dev(x, 1, y, z))

        for kc in (0, 1):
            ref = pb.at[lo, z, kc]
            for d in (2, -2, 1, -1):
                send(ref, ref, ("z", "A", d, kc), dev(x, 0, y, zat(d)))
            for d in (2, -2, 1, -1, 0):
                send(b_send.at[kc], ref, ("z", "B", d, kc), dev(x, 0, mate, zat(d)))
        forward("A", 0)
        for kc in (0, 1):
            wait_z("B", 0, kc)
        forward("B", 0)
        for kc in (0, 1):
            for sign in (1, -1):
                wait_z("A", 2 * sign, kc)
            spread("A", 2, kc)
        for d in (1, -1):
            for kc in (0, 1):
                wait_z("A", d, kc)
            forward("A", d)
        forward("A", 2)
        forward("A", -2)
        for kc in (0, 1):
            for sign in (1, -1):
                wait_z("B", 2 * sign, kc)
            spread("B", 2, kc)
        for d in (1, -1):
            for kc in (0, 1):
                wait_z("B", d, kc)
            forward("B", d)
        forward("B", 2)
        forward("B", -2)
        for typ in "AB":
            for kc in (0, 1):
                for sign in (1, -1):
                    wait_z(typ, 4 * sign, kc)
                spread(typ, 4, kc)
            for d in (3, -3):
                for kc in (0, 1):
                    wait_z(typ, d, kc)
                forward(typ, d)
            forward(typ, 4)
            forward(typ, -4)
        for typ in "AB":
            for d in (5, -5):
                for kc in (0, 1):
                    wait_z(typ, d, kc)
                forward(typ, d)
            wait_z(typ, 6, 0)
            wait_z(typ, -6, 1)
            forward(typ, 6)

        stores = []
        for i, (kind, kc) in enumerate(ORDER):
            at = pl.ds(koff(kind, kc), KC)
            arrived(sum_s.at[i], ("sum", i))
            average = sum_s[i]
            m = NEST * mom[:, at] + average
            n_mom[i] = m
            n_prm[i] = prm[:, at] - RATE * (average + NEST * m)
            stores.append(local(n_mom.at[i], new_mom_hbm.at[:, at], ("nm", i)))
            stores.append(local(n_prm.at[i], new_prm_hbm.at[:, at], ("np", i)))
        for d in (0, 1, 2, 3):
            arrived(outb.at[:, xat(-d)], ("out", 0, d))
        stores.append(local(outb, out_hbm, "out"))
        for cp in stores:
            cp.wait()
        for cp in pending:
            cp.wait_send()

    assert max(len(k.at) for k in (rk, sk, lk)) <= N_SEM


def per_device(pseudo_grad, compensation, params, momentum, probe):
    any_space = pl.BlockSpec(memory_space=pl.ANY)
    new_params, new_momentum, out = pl.pallas_call(
        kernel,
        out_shape=(
            jax.ShapeDtypeStruct((16, K), F32),
            jax.ShapeDtypeStruct((16, K), F32),
            jax.ShapeDtypeStruct((6, NX, 16, 128), BF16),
        ),
        in_specs=[any_space] * 5,
        out_specs=[any_space] * 3,
        scratch_shapes=[
            pltpu.VMEM((4, 8, 16, KC), BF16),
            pltpu.VMEM((4, 8, 16, KC), F32),
            pltpu.VMEM((4, 8, 16, KC), BF16),
            pltpu.VMEM((4, 8, 16, KC), BF16),
            pltpu.VMEM((4, 2, 16, KC), BF16),
            pltpu.VMEM((4, 2, 2, 16, KC), BF16),
            pltpu.VMEM((4, 2, 16, KC), BF16),
            pltpu.VMEM((16, K), F32),
            pltpu.VMEM((16, K), F32),
            pltpu.VMEM((16, K), F32),
            pltpu.VMEM((4, 16, KC), F32),
            pltpu.VMEM((2, 2, NX, 2, 16, KC), BF16),
            pltpu.VMEM((2, 2, 16, KC), BF16),
            pltpu.VMEM((2, NZ, 2, 16, KC), BF16),
            pltpu.VMEM((2, 16, KC), BF16),
            pltpu.VMEM((2, 2, 2, 6, 16, 128), BF16),
            pltpu.VMEM((NY, 6, 16, 128), BF16),
            pltpu.VMEM((6, NX, 16, 128), BF16),
            pltpu.VMEM((4, 16, KC), F32),
            pltpu.VMEM((4, 16, KC), F32),
            pltpu.SemaphoreType.DMA((N_SEM,)),
            pltpu.SemaphoreType.DMA((N_SEM,)),
            pltpu.SemaphoreType.DMA((N_SEM,)),
            pltpu.SemaphoreType.REGULAR,
        ],
        compiler_params=pltpu.CompilerParams(
            collective_id=0, has_side_effects=True, vmem_limit_bytes=60 * 2**20
        ),
    )(
        pseudo_grad.reshape(8, 16, K),
        compensation.reshape(8, 16, K),
        params,
        momentum,
        probe.reshape(NX, 16, K),
    )
    return new_params, new_momentum, out.reshape(384, 128)


def solution(mesh):
    in_specs = (
        P("replica", "fsdp", "tensor"),
        P("replica", "fsdp", "tensor"),
        P(("fsdp", "replica"), "tensor"),
        P(("fsdp", "replica"), "tensor"),
        P("fsdp", "tensor"),
    )
    out_specs = (
        P(("fsdp", "replica"), "tensor"),
        P(("fsdp", "replica"), "tensor"),
        P("tensor", "fsdp"),
    )
    return jax.shard_map(
        per_device, mesh=mesh, in_specs=in_specs, out_specs=out_specs, check_vma=False
    )
```

```python
import jax
import jax.numpy as jnp
from jax import lax
from jax.experimental import pallas as pl
from jax.experimental.pallas import tpu as pltpu
from jax.sharding import PartitionSpec as P

MESH = pl.DeviceIdType.MESH
RATE = 0.7
NEST = 0.9
F32, BF16 = jnp.float32, jnp.bfloat16

NX, NY, NZ = 4, 8, 12
K = 4608
KC = K // 4
HALF = NZ // 2
FIRST = 6
EARLY = 6
ORDER = (("P", 0), ("P", 1), ("O", 0), ("O", 1))
SPREAD = {0: (-3, 1, -1), 1: (1,), 2: (1,), 3: (1,), 4: (1,), -1: (-1,), -3: (-1, -3), -4: (-1,)}
LEAVES = (5, -2, -5, -6)
INNER = (1, -1, -3, 2, -4, 3, 4)
N_RECV, N_SEND, N_LOCAL = 88, 12, 10


class Keys:
    def __init__(self):
        self.at = {}

    def __call__(self, *key):
        return self.at.setdefault(key, len(self.at))


def kernel(
    pg_hbm, comp_hbm, prm_hbm, mom_hbm, probe_hbm,
    n_prm, n_mom, outb,
    v_pg, v_comp, out_s, cs, r_opp, r_fin, t_acc, prm, mom, q_s, sum_s,
    w, wy, pb, b_send, part, y_in,
    send_sem, recv_sem, loc_sem, go,
):
    rep = lax.axis_index("replica")
    fs = lax.axis_index("fsdp")
    t = lax.axis_index("tensor")
    x, core = rep // 2, rep % 2
    lo, z = fs // NZ, fs % NZ
    other = 1 - lo
    y = t * 2 + lo
    mate = t * 2 + other

    def dev(x_, core_, y_, z_):
        return (x_ * 2 + core_, (y_ % 2) * NZ + z_, y_ // 2)

    def xat(d):
        return lax.rem(x + d + NX, NX)

    def yat(d):
        return lax.rem(y + d + NY, NY)

    def zat(d):
        return lax.rem(z + d + NZ, NZ)

    def w_core(z_):
        return jnp.where(z_ < FIRST, 1, 0)

    wc = w_core(z)
    hc = 1 - wc
    w_dev, h_dev, me = dev(x, wc, y, z), dev(x, hc, y, z), dev(x, core, y, z)

    rk, sk, lk = Keys(), Keys(), Keys()

    def rsem(*key):
        return recv_sem.at[rk(*key)]

    def ssem(group):
        return send_sem.at[sk(group)]

    def send(src, dst, key, to, group):
        pltpu.make_async_remote_copy(
            src_ref=src, dst_ref=dst, send_sem=ssem(group), recv_sem=rsem(*key),
            device_id=to, device_id_type=MESH,
        ).start()

    def arrived(like, *key):
        pltpu.make_async_remote_copy(
            src_ref=like, dst_ref=like, send_sem=send_sem.at[0], recv_sem=rsem(*key),
            device_id=me, device_id_type=MESH,
        ).wait_recv()

    def sent(like, group):
        pltpu.make_async_remote_copy(
            src_ref=like, dst_ref=like, send_sem=ssem(group), recv_sem=recv_sem.at[0],
            device_id=me, device_id_type=MESH,
        ).wait_send()

    def load(src, dst, key):
        pltpu.make_async_copy(src, dst, loc_sem.at[lk(key)]).start()

    def loaded(like, key):
        pltpu.make_async_remote_copy(
            src_ref=like, dst_ref=like, send_sem=send_sem.at[0], recv_sem=loc_sem.at[lk(key)],
            device_id=me, device_id_type=MESH,
        ).wait_recv()

    def columns(kind, kc):
        half = lo if kind == "O" else other
        return pl.ds(pl.multiple_of((half * 2 + kc) * KC, KC), KC)

    for i, (kind, kc) in enumerate(ORDER):
        at = columns(kind, kc)
        load(pg_hbm.at[:, :, at], v_pg.at[i], ("in", i))
        load(comp_hbm.at[:, :, at], v_comp.at[i], ("in", i))

    barrier = pltpu.get_barrier_semaphore()

    def greet(to):
        pl.semaphore_signal(barrier, inc=1, device_id=to, device_id_type=MESH)

    for d in (1, 2, 3):
        greet(dev(xat(d), wc, y, z))
    for d in range(1, NY):
        greet(dev(x, wc, yat(d), z))

    def p_dev(y_, d):
        return dev(x, 1 - w_core(zat(d)), y_, zat(d))

    @pl.when(core == hc)
    def _():
        greet(w_dev)
        for kc in (0, 1):
            load(probe_hbm.at[x, :, columns("O", kc)], pb.at[lo, z, kc], "own")
            load(probe_hbm.at[x, :, columns("P", kc)], b_send.at[kc], "own")
        for yy in (y, mate):
            for d in (1, -1, 3):
                greet(p_dev(yy, d))
        greet(p_dev(mate, 0))

    @pl.when(core == wc)
    def _():
        @pl.when(wc == 1)
        def _():
            for d in (1, -1, 3):
                greet(p_dev(y, d))

        @pl.when(z >= EARLY)
        def _():
            greet(h_dev)

    load(prm_hbm, prm, "state")
    load(mom_hbm, mom, "state")

    @pl.when(core == wc)
    def _():
        right, left, far = xat(1), xat(-1), xat(2)
        rdev, ldev = dev(right, wc, y, z), dev(left, wc, y, z)
        pl.semaphore_wait(barrier, 7 + 14)

        @pl.when(z < EARLY)
        def _():
            pl.semaphore_signal(go, inc=1, device_id=h_dev, device_id_type=MESH)

        def chip_sum(i, s):
            return v_pg[i, s].astype(F32) + v_comp[i, s] + out_s[i, s].astype(F32)

        def opposite(i):
            loaded(pb.at[0], ("in", i))
            arrived(out_s.at[i], "push", i)
            for side, to in ((1, rdev), (0, ldev)):
                s = far * 2 + side
                cs[i, s] = chip_sum(i, s).astype(BF16)
                send(cs.at[i, s], r_opp.at[i, side], ("opp", i, side), to, "rs")

        def direct(i):
            for side, to, xx in ((0, rdev, right), (1, ldev, left)):
                s = xx * 2 + side
                cs[i, s] = chip_sum(i, s).astype(BF16)
                send(cs.at[i, s], r_fin.at[i, side, 0], ("fin", i), to, "rs")

        def on_the_way(i):
            for side, to, xx in ((1, rdev, right), (0, ldev, left)):
                s = xx * 2 + side
                arrived(r_opp.at[i, side], "opp", i, side)
                t_acc[i, side] = (chip_sum(i, s) + r_opp[i, side].astype(F32)).astype(BF16)
                send(t_acc.at[i, side], r_fin.at[i, side, 1], ("fin", i), to, "rs")

        opposite(0)
        opposite(1)
        direct(0)
        direct(1)
        opposite(2)
        opposite(3)
        on_the_way(0)
        on_the_way(1)
        direct(2)
        direct(3)
        on_the_way(2)
        on_the_way(3)

        loaded(v_comp.at[0], "state")
        arrived(q_s, "q")

        def gather(kc, f, rel):
            for side, to, first in ((1, rdev, True), (0, ldev, True), (0, rdev, False), (1, ldev, False)):
                ref = w.at[kc, f, x, side]
                send(ref, ref, ("ag", kc, rel, side) if first else ("rest", kc, rel), to, "ag")

        def relay(kc, f, rel):
            for side, to, xx in ((1, rdev, left), (0, ldev, right)):
                ref = w.at[kc, f, xx, side]
                arrived(ref, "ag", kc, rel, side)
                send(ref, ref, ("rest", kc, rel), to, "ag")

        for i, (kind, kc) in enumerate(ORDER):
            at = columns(kind, kc)
            arrived(r_fin.at[i], "fin", i)

            def average(side):
                return (
                    chip_sum(i, x * 2 + side)
                    + r_fin[i, side, 0].astype(F32)
                    + r_fin[i, side, 1].astype(F32)
                ) * 0.125

            avg = average(wc)
            m = NEST * mom[:, at] + avg
            new = prm[:, at] - RATE * (avg + NEST * m)
            n_mom[:, at] = m
            n_prm[:, at] = new
            avg = average(hc)
            sum_s[i] = avg
            new_h = q_s[:, at] - (RATE * (1 + NEST)) * avg
            if kind == "O":
                w[kc, lo, x, wc] = new.astype(BF16)
                w[kc, lo, x, hc] = new_h.astype(BF16)
                gather(kc, lo, 0)
            else:
                wy[kc, wc] = new.astype(BF16)
                wy[kc, hc] = new_h.astype(BF16)
                for side in (1, 0):
                    send(wy.at[kc, side], w.at[kc, lo, x, side], ("wy", kc), dev(x, wc, mate, z), "ag")
            send(sum_s.at[i], sum_s.at[i], ("sum",), h_dev, "sum")

        for kc in (0, 1):
            arrived(w.at[kc, other, x], "wy", kc)
            gather(kc, other, 1)
        for rel, f in ((0, lo), (1, other)):
            for kc in (0, 1):
                relay(kc, f, rel)
        for rel, f in ((0, lo), (1, other)):
            for kc in (0, 1):
                arrived(w.at[kc, f, 0:2], "rest", kc, rel)

                @pl.when(wc == 0)
                def _():
                    send(w.at[kc, f], w.at[kc, f], ("wf",), h_dev, "wf")

    @pl.when(core == hc)
    def _():
        def pushes():
            for i in range(4):
                loaded(pb.at[0], ("in", i))
                out_s[i] = (v_pg[i].astype(F32) + v_comp[i]).astype(BF16)
                send(out_s.at[i], out_s.at[i], ("push", i), w_dev, "push")
            loaded(v_comp.at[0], "state")
            q_s[...] = prm[...] - (RATE * NEST * NEST) * mom[...]
            send(q_s, q_s, ("q",), w_dev, "q")

        early = jnp.where(z < EARLY, 1, 0)
        greeted = 8 - early
        for d in (1, -1, -3):
            greeted += w_core(zat(d))

        @pl.when(early == 1)
        def _():
            pl.semaphore_wait(go, 1)
            pushes()

        loaded(pb.at[0, 0:2], "own")
        pl.semaphore_wait(barrier, greeted)
        own = {"A": lo, "B": other}

        def place(typ, d, step):
            zz = zat(step)
            if d in LEAVES:
                return dev(x, 1, y, zz), ("leaf", typ, d)
            return dev(x, 1 - w_core(zz), y, zz), None

        def spread(typ, at, kc):
            ref = pb.at[own[typ], zat(-at), kc]
            for step in SPREAD[at]:
                d = at + step
                to, key = place(typ, d, step)
                send(ref, ref, key or ("z", typ, d, kc), to, "relay" if at else "own")

        for kc in (0, 1):
            spread("A", 0, kc)
            for step in (*SPREAD[0], 0):
                ref = pb.at[lo, z, kc]
                send(b_send.at[kc], ref, ("z", "B", step, kc), p_dev(mate, step), "own")

        @pl.when(early == 0)
        def _():
            pushes()

        def wait_z(typ, d, kc):
            arrived(pb.at[own[typ], zat(-d), kc], "z", typ, d, kc)

        def forward(d):
            @pl.when(hc == 0)
            def _():
                for typ in "AB":
                    ref = pb.at[own[typ], zat(-d)]
                    send(ref, ref, ("fw", d), w_dev, "fw")

        for kc in (0, 1):
            wait_z("B", 0, kc)
        forward(0)
        for level in ((1, -1, -3), (2, -4), (3,), (4,)):
            for kc in (0, 1):
                for typ in "AB":
                    for d in level:
                        wait_z(typ, d, kc)
                        spread(typ, d, kc)
            for d in level:
                forward(d)

    @pl.when(core == 1)
    def _():
        near = z // HALF

        @pl.when(wc == 0)
        def _():
            arrived(w, "wf")

        def wait_blocks(want_near):
            for d in (0, *INNER, *LEAVES):
                is_near = zat(-d) // HALF == near
                for typ in "AB" if d in LEAVES else "A":
                    cond = is_near if want_near else jnp.logical_not(is_near)
                    if d in LEAVES:
                        key, like = ("leaf", typ, d), pb.at[0, 0]
                    else:
                        key, like = ("fw", d), pb.at[0, 0:2]
                        cond = jnp.logical_and(cond, wc == 1)

                    @pl.when(cond)
                    def _():
                        arrived(like, *key)

        for phase in (0, 1):
            h = near if phase == 0 else 1 - near
            wait_blocks(phase == 0)
            acc = jnp.zeros((2 * HALF * 16, 256), F32)
            for kc in (0, 1):
                rows = pb[:, pl.ds(h * HALF, HALF), kc].reshape(2 * HALF * 16, KC)
                acc += lax.dot_general(
                    rows, w[kc].reshape(256, KC), (((1,), (1,)), ((), ())),
                    preferred_element_type=F32,
                )
            for lp in (0, 1):
                for lw in (0, 1):
                    piece = acc[lp * 96 : lp * 96 + 96, lw * 128 : lw * 128 + 128]
                    part[phase, lp, lw] = piece.astype(BF16).reshape(HALF, 16, 128)
            for lp in (0, 1):
                for lw in (0, 1):
                    to = 4 * lp + 2 * h + lw

                    @pl.when(to != y)
                    def _():
                        send(part.at[phase, lp, lw], y_in.at[y], ("y",), dev(x, 1, to, z), "y")

                    @pl.when(to == y)
                    def _():
                        y_in[y] = part[phase, lp, lw]

        arrived(y_in.at[0:7], "y")
        total = y_in[0].astype(F32)
        for i in range(1, NY):
            total += y_in[i].astype(F32)
        outb[:, x] = total.astype(BF16)
        mine = outb.at[:, x]
        for d in (2, 1, 3):
            for cc in (1, 0):
                send(mine, mine, ("out",), dev(xat(d), cc, y, z), "out")
        send(mine, mine, ("out",), dev(x, 0, y, z), "out")

    @pl.when(core == hc)
    def _():
        arrived(sum_s, "sum")
        for i, (kind, kc) in enumerate(ORDER):
            at = columns(kind, kc)
            avg = sum_s[i]
            m = NEST * mom[:, at] + avg
            n_mom[:, at] = m
            n_prm[:, at] = prm[:, at] - RATE * (avg + NEST * m)
        sent(out_s, "push")
        sent(q_s, "q")
        sent(pb.at[0, 0:7], "own")
        sent(pb.at[:, 0:8], "relay")

        @pl.when(hc == 0)
        def _():
            sent(pb.at[:, 0:8], "fw")

    @pl.when(core == wc)
    def _():
        sent(pb.at[0], "rs")
        sent(pb.at[:, 0:7], "ag")
        sent(sum_s, "sum")

        @pl.when(wc == 0)
        def _():
            sent(w, "wf")

    @pl.when(core == 1)
    def _():
        sent(y_in.at[0:7], "y")
        sent(y_in.at[0:7], "out")
        arrived(y_in.at[0:3], "out")

    @pl.when(core == 0)
    def _():
        arrived(y_in.at[0:4], "out")

    assert len(rk.at) <= N_RECV and len(sk.at) <= N_SEND and len(lk.at) <= N_LOCAL


def store(a, b, c, a_out, b_out, c_out, sem):
    copies = [
        pltpu.make_async_copy(src, dst, sem.at[i])
        for i, (src, dst) in enumerate(((a, a_out), (b, b_out), (c, c_out)))
    ]
    for cp in copies:
        cp.start()
    for cp in copies:
        cp.wait()


def per_device(pseudo_grad, compensation, params, momentum, probe):
    any_space = pl.BlockSpec(memory_space=pl.ANY)
    vmem = pl.BlockSpec(memory_space=pltpu.VMEM)
    shapes = (
        jax.ShapeDtypeStruct((16, K), F32),
        jax.ShapeDtypeStruct((16, K), F32),
        jax.ShapeDtypeStruct((6, NX, 16, 128), BF16),
    )
    outs = pl.pallas_call(
        kernel,
        out_shape=tuple(pltpu.VMEM(s.shape, s.dtype) for s in shapes),
        in_specs=[any_space] * 5,
        out_specs=[vmem] * 3,
        scratch_shapes=[
            pltpu.VMEM((4, 8, 16, KC), BF16),
            pltpu.VMEM((4, 8, 16, KC), F32),
            pltpu.VMEM((4, 8, 16, KC), BF16),
            pltpu.VMEM((4, 8, 16, KC), BF16),
            pltpu.VMEM((4, 2, 16, KC), BF16),
            pltpu.VMEM((4, 2, 2, 16, KC), BF16),
            pltpu.VMEM((4, 2, 16, KC), BF16),
            pltpu.VMEM((16, K), F32),
            pltpu.VMEM((16, K), F32),
            pltpu.VMEM((16, K), F32),
            pltpu.VMEM((4, 16, KC), F32),
            pltpu.VMEM((2, 2, NX, 2, 16, KC), BF16),
            pltpu.VMEM((2, 2, 16, KC), BF16),
            pltpu.VMEM((2, NZ, 2, 16, KC), BF16),
            pltpu.VMEM((2, 16, KC), BF16),
            pltpu.VMEM((2, 2, 2, HALF, 16, 128), BF16),
            pltpu.VMEM((NY, HALF, 16, 128), BF16),
            pltpu.SemaphoreType.DMA((N_SEND,)),
            pltpu.SemaphoreType.DMA((N_RECV,)),
            pltpu.SemaphoreType.DMA((N_LOCAL,)),
            pltpu.SemaphoreType.REGULAR,
        ],
        compiler_params=pltpu.CompilerParams(
            collective_id=0, has_side_effects=True, vmem_limit_bytes=60 * 2**20
        ),
    )(
        pseudo_grad.reshape(8, 16, K),
        compensation.reshape(8, 16, K),
        params,
        momentum,
        probe.reshape(NX, 16, K),
    )
    new_params, new_momentum, out = pl.pallas_call(
        store,
        out_shape=shapes,
        in_specs=[any_space] * 3,
        out_specs=[any_space] * 3,
        scratch_shapes=[pltpu.SemaphoreType.DMA((3,))],
        compiler_params=pltpu.CompilerParams(vmem_limit_bytes=2**20),
    )(*outs)
    return new_params, new_momentum, out.reshape(384, 128)


def solution(mesh):
    in_specs = (
        P("replica", "fsdp", "tensor"),
        P("replica", "fsdp", "tensor"),
        P(("fsdp", "replica"), "tensor"),
        P(("fsdp", "replica"), "tensor"),
        P("fsdp", "tensor"),
    )
    out_specs = (
        P(("fsdp", "replica"), "tensor"),
        P(("fsdp", "replica"), "tensor"),
        P("tensor", "fsdp"),
    )
    return jax.shard_map(
        per_device, mesh=mesh, in_specs=in_specs, out_specs=out_specs, check_vma=False
    )
```

```python
import jax
import jax.numpy as jnp
from jax import lax
from jax.experimental import pallas as pl
from jax.experimental.pallas import tpu as pltpu
from jax.sharding import PartitionSpec as P

MESH = pl.DeviceIdType.MESH
RATE = 0.7
NEST = 0.9
F32, BF16 = jnp.float32, jnp.bfloat16

NX, NY, NZ = 4, 8, 12
K = 4608
KC = K // 4
HALF = NZ // 2
FIRST = 1
EARLY = 6
ORDER = (("P", 0), ("P", 1), ("O", 0), ("O", 1))
TREE = {
    0: {0: (1, 11,), 1: (2,), 2: (3,), 3: (4,), 4: (5,), 5: (6,), 8: (9, 7,), 10: (8,), 11: (10,)},
    1: {0: (11,), 1: (2, 0,), 2: (3,), 3: (4,), 4: (5,), 5: (6,), 6: (7,), 9: (8, 10,), 11: (9,)},
    2: {0: (11,), 1: (0,), 2: (1, 3,), 3: (4,), 4: (5,), 5: (6,), 6: (7,), 7: (8,), 10: (9,), 11: (10,)},
    3: {0: (11,), 1: (0,), 2: (1,), 3: (2, 4,), 4: (5,), 5: (6,), 6: (7,), 7: (8,), 10: (9,), 11: (10,)},
    4: {0: (11,), 1: (0,), 2: (1,), 3: (2,), 4: (3, 5,), 5: (6,), 6: (7,), 7: (8,), 8: (9,), 9: (10,)},
    5: {1: (0,), 2: (1,), 3: (2,), 4: (3,), 5: (4, 6,), 6: (7,), 7: (8,), 8: (11, 9,), 9: (10,)},
    6: {1: (0, 2,), 2: (3,), 4: (5,), 6: (4, 8, 7, 1,), 8: (9,), 9: (10,), 10: (11,)},
    7: {2: (1,), 3: (2, 4,), 4: (5,), 6: (3,), 7: (8, 6,), 8: (9, 10,), 10: (11, 0,)},
    8: {0: (1, 11,), 3: (2,), 4: (5, 3,), 5: (6,), 7: (4,), 8: (7, 9,), 9: (0,), 11: (10,)},
    9: {0: (11, 1,), 1: (2,), 4: (3, 5,), 6: (4,), 7: (6, 8,), 9: (7, 0,), 11: (10,)},
    10: {0: (1,), 1: (2,), 4: (3,), 6: (5,), 7: (6,), 8: (7,), 9: (4,), 10: (9, 8, 11,), 11: (0,)},
    11: {1: (0, 2,), 2: (3,), 3: (4,), 6: (5, 7,), 9: (8,), 10: (9, 6,), 11: (1, 10,)},
}
WAITS = (
    (4, 6, 5, 7, 8, 10, 9, 11, -1, 12, 14, 13, 15, 36, 40, 16, 38, 37, 42, 18, 41, 32, 17, 39, 43, 34, 19, 33, 35),
    (0, 8, 2, 1, 10, 9, 3, 11, 12, 14, 13, 15, 16, 44, 18, 46, 45, 17, 24, 47, 19, 25, 26, 20, 22, 27, 36, 21, 40, 23, 38, 37, 42, 41, 39, 43),
    (4, 6, 5, 12, 7, 0, 14, 2, 13, 1, 15, 3, 16, 18, 17, 19, 20, 22, 21, 44, 23, 46, 45, 24, 47, 28, 30, 25, 26, 29, 31, 27),
    (8, 10, 9, 11, 4, 16, 6, 5, 18, 17, 7, 0, 19, 2, 1, 3, 20, 22, 21, 23, 28, 30, 29, 31, 44, 32, 46, 34, 45, 33, 47, 35),
    (12, 14, 13, 8, 15, 10, 20, 9, 22, 11, 21, 4, 23, 24, 6, 5, 7, 0, 25, 26, 2, 1, 27, 3, 32, 34, 33, 35, 28, 40, 30, 36, 29, 41, 42, 31, 38, 37, 39, 43),
    (16, 18, 17, 12, -1, 19, 14, 13, 8, 15, 10, 9, 11, 4, 6, 5, 0, 7, 2, 1, 32, 3, 34, 33, 35),
    (28, 30, 20, 29, 22, 31, 21, 16, 23, 18, 17, 12, 19, 36, 14, 13, 8, 38, 15, 37, 10, 9, 39, 4, 11, 40, 6, 44, 5, 46, 7, 41, 42, 45, 47, 43),
    (32, 34, 33, 36, 35, 38, 37, 20, 39, 22, 21, 16, 40, 23, 18, 17, 41, 12, 42, 19, 14, 13, 8, 43, 15, 10, 9, 11),
    (28, 30, 29, 24, 31, 26, 25, 40, 27, 41, 42, 43, 20, 22, 21, 16, 23, 18, 17, 0, 19, 2, 1, 3),
    (32, 40, 34, 33, 35, 41, 42, 43, 24, 44, 46, 45, 26, 25, 47, 27, 4, 20, 6, 22, 5, 21, 7, 16, 23, 18, 17, 19),
    (44, 46, 45, 47, 28, 30, 0, 29, 2, 31, 1, 24, 3, 8, 26, 10, 25, 9, 27, 11, 12, 14, 13, 15),
    (40, 42, 41, 43, 0, 2, 1, 3, 4, 6, 8, 5, 7, 10, 9, 11, 12, 14, 13, 15, 36, 38, 37, 32, 39, 34, 33, 35),
)
LINKS = {0: NZ - 1, EARLY - 1: EARLY}
SHARED = 50
N_RECV, N_SEND, N_LOCAL = SHARED + 16, 12, 6


class Keys:
    def __init__(self):
        self.at = {}

    def __call__(self, *key):
        return self.at.setdefault(key, len(self.at))


def kernel(
    pg_hbm, comp_hbm, prm_hbm, mom_hbm, probe_hbm,
    n_prm, n_mom, outb,
    v_pg, v_comp, out_s, cs, r_opp, r_fin, t_acc, prm, mom, q_s, sum_s,
    w, w_t, wy, pb, b_send, part, y_in,
    send_sem, recv_sem, loc_sem, go, go_late,
):
    rep = lax.axis_index("replica")
    fs = lax.axis_index("fsdp")
    t = lax.axis_index("tensor")
    x, core = rep // 2, rep % 2
    lo, z = fs // NZ, fs % NZ
    other = 1 - lo
    y = t * 2 + lo
    mate = t * 2 + other

    def dev(x_, core_, y_, z_):
        return (x_ * 2 + core_, (y_ % 2) * NZ + z_, y_ // 2)

    def xat(d):
        return lax.rem(x + d + NX, NX)

    def yat(d):
        return lax.rem(y + d + NY, NY)

    def zat(d):
        return lax.rem(z + d + NZ, NZ)

    def w_core(z_):
        return jnp.where(z_ < FIRST, 1, 0)

    wc = w_core(z)
    hc = 1 - wc
    w_dev, h_dev, me = dev(x, wc, y, z), dev(x, hc, y, z), dev(x, core, y, z)

    keys, sk, lk = {group: Keys() for group in "wpt"}, Keys(), Keys()

    def rsem(group, *key):
        at = keys[group](*key)
        return recv_sem.at[SHARED + at if group == "t" else at]

    def ssem(group):
        return send_sem.at[sk(group)]

    def send(src, dst, key, to, group):
        pltpu.make_async_remote_copy(
            src_ref=src, dst_ref=dst, send_sem=ssem(group), recv_sem=rsem(*key),
            device_id=to, device_id_type=MESH,
        ).start()

    def arrived(like, *key):
        pltpu.make_async_remote_copy(
            src_ref=like, dst_ref=like, send_sem=send_sem.at[0], recv_sem=rsem(*key),
            device_id=me, device_id_type=MESH,
        ).wait_recv()

    def sent(like, group):
        pltpu.make_async_remote_copy(
            src_ref=like, dst_ref=like, send_sem=ssem(group), recv_sem=recv_sem.at[0],
            device_id=me, device_id_type=MESH,
        ).wait_send()

    def load(src, dst, key):
        pltpu.make_async_copy(src, dst, loc_sem.at[lk(key)]).start()

    def loaded(like, key):
        pltpu.make_async_remote_copy(
            src_ref=like, dst_ref=like, send_sem=send_sem.at[0], recv_sem=loc_sem.at[lk(key)],
            device_id=me, device_id_type=MESH,
        ).wait_recv()

    def columns(kind, kc):
        half = lo if kind == "O" else other
        return pl.ds(pl.multiple_of((half * 2 + kc) * KC, KC), KC)

    def load_chunk(i):
        at = columns(*ORDER[i])
        load(pg_hbm.at[:, :, at], v_pg.at[i], ("in", i))
        load(comp_hbm.at[:, :, at], v_comp.at[i], ("in", i))

    barrier = pltpu.get_barrier_semaphore()

    def greet(to):
        pl.semaphore_signal(barrier, inc=1, device_id=to, device_id_type=MESH)

    def core_of_probe(zz):
        return 0 if zz < FIRST else 1

    def p_dev(y_, zz):
        return dev(x, core_of_probe(zz), y_, zz)

    def goes_to(src, zz):
        return core_of_probe(zz) if TREE[src].get(zz) else 1

    def senders(zz, to_core):
        found = {}
        for src in TREE:
            for q, to in TREE[src].items():
                if zz in to and goes_to(src, zz) == to_core:
                    found[0, q] = y
                    if q == src:
                        found[1, q] = mate
        if to_core == 1:
            found[1, zz] = mate
        if zz in LINKS and to_core == core_of_probe(zz):
            found[0, LINKS[zz]], found[1, LINKS[zz]] = y, mate
        return [(found[key], key[1]) for key in sorted(found)]

    late = z >= EARLY

    @pl.when(core == hc)
    def _():
        @pl.when(jnp.logical_not(late))
        def _():
            load_chunk(0)

        greet(w_dev)
        for zz in range(NZ):

            @pl.when(z == zz)
            def _():
                for yy, q in senders(zz, core_of_probe(zz)):
                    if not (q < EARLY <= zz):
                        greet(p_dev(yy, q))

        for kc in (0, 1):
            load(probe_hbm.at[x, :, columns("O", kc)], pb.at[lo, z, kc], "own")
            load(probe_hbm.at[x, :, columns("P", kc)], b_send.at[kc], "own")

        @pl.when(late)
        def _():
            load_chunk(0)

    @pl.when(core == wc)
    def _():
        for d in (1, -1):
            greet(dev(xat(d), wc, y, z))
            greet(dev(xat(d), wc, mate, z))

        @pl.when(wc == 0)
        def _():
            greet(dev(x, wc, mate, z))

        for zz in range(FIRST):

            @pl.when(z == zz)
            def _():
                for yy, q in senders(zz, 1):
                    greet(p_dev(yy, q))

        @pl.when(wc == 1)
        def _():
            for kc in (0, 1):
                load(probe_hbm.at[x, :, columns("O", kc)], pb.at[lo, z, kc], "own")

        @pl.when(late)
        def _():
            greet(h_dev)

        load_chunk(0)

    @pl.when(core == 1)
    def _():
        for d in range(1, NY):
            greet(dev(x, wc, yat(d), z))

    for i in (1, 2, 3):
        load_chunk(i)
    load(prm_hbm, prm, "state")
    load(mom_hbm, mom, "state")

    @pl.when(core == wc)
    def _():
        right, left, far = xat(1), xat(-1), xat(2)
        rdev, ldev = dev(right, wc, y, z), dev(left, wc, y, z)
        pl.semaphore_wait(barrier, 1 + 4 + 7 + hc)

        @pl.when(jnp.logical_not(late))
        def _():
            pl.semaphore_signal(go, inc=1, device_id=h_dev, device_id_type=MESH)

        def chip_sum(i, s):
            return v_pg[i, s].astype(F32) + v_comp[i, s] + out_s[i, s].astype(F32)

        def opposite(i):
            loaded(pb.at[0], ("in", i))
            arrived(out_s.at[i], "w", "push", i)
            for side, to in ((1, rdev), (0, ldev)):
                s = far * 2 + side
                cs[i, s] = chip_sum(i, s).astype(BF16)
                send(cs.at[i, s], r_opp.at[i, side], ("w", "opp", i, side), to, "rs")

        def direct(i):
            for side, to, xx in ((0, rdev, right), (1, ldev, left)):
                s = xx * 2 + side
                cs[i, s] = chip_sum(i, s).astype(BF16)
                send(cs.at[i, s], r_fin.at[i, side, 0], ("w", "fin", i), to, "rs")

        def on_the_way(i):
            for side, to, xx in ((1, rdev, right), (0, ldev, left)):
                s = xx * 2 + side
                arrived(r_opp.at[i, side], "w", "opp", i, side)
                t_acc[i, side] = (chip_sum(i, s) + r_opp[i, side].astype(F32)).astype(BF16)
                send(t_acc.at[i, side], r_fin.at[i, side, 1], ("w", "fin", i), to, "rs")

        opposite(0)
        opposite(1)
        direct(0)
        direct(1)
        opposite(2)
        opposite(3)
        on_the_way(0)
        on_the_way(1)
        direct(2)
        direct(3)
        on_the_way(2)
        on_the_way(3)

        loaded(v_comp.at[0], "state")
        arrived(q_s, "w", "q")

        def gather(src, kc, y_, rel):
            for side, to, first in ((1, right, True), (0, left, True), (0, right, False), (1, left, False)):
                key = ("w", "ag", kc, rel, side) if first else ("w", "rest", kc, rel)
                send(src.at[side], w.at[kc, lo, x, side], key, dev(to, wc, y_, z), "ag")

        def relay(kc, f, rel):
            for side, to, xx in ((1, rdev, left), (0, ldev, right)):
                ref = w.at[kc, f, xx, side]
                arrived(ref, "w", "ag", kc, rel, side)
                send(ref, ref, ("w", "rest", kc, rel), to, "ag")

        for i, (kind, kc) in enumerate(ORDER):
            at = columns(kind, kc)
            arrived(r_fin.at[i], "w", "fin", i)

            def average(side):
                return (
                    chip_sum(i, x * 2 + side)
                    + r_fin[i, side, 0].astype(F32)
                    + r_fin[i, side, 1].astype(F32)
                ) * 0.125

            avg = average(wc)
            m = NEST * mom[:, at] + avg
            new = prm[:, at] - RATE * (avg + NEST * m)
            n_mom[:, at] = m
            n_prm[:, at] = new
            avg = average(hc)
            sum_s[i] = avg
            new_h = q_s[:, at] - (RATE * (1 + NEST)) * avg
            if kind == "O":
                w[kc, lo, x, wc] = new.astype(BF16)
                w[kc, lo, x, hc] = new_h.astype(BF16)
                gather(w.at[kc, lo, x], kc, y, 0)
            else:
                wy[kc, wc] = new.astype(BF16)
                wy[kc, hc] = new_h.astype(BF16)
                gather(wy.at[kc], kc, mate, 1)
                for side in (0, 1):
                    send(wy.at[kc, side], w.at[kc, lo, x, side], ("w", "rest", kc, 1), dev(x, wc, mate, z), "ag")
            send(sum_s.at[i], sum_s.at[i], ("p", "sum"), h_dev, "sum")

        for rel, f in ((1, other), (0, lo)):
            for kc in (0, 1):
                relay(kc, f, rel)
        for rel, f in ((1, other), (0, lo)):
            for kc in (0, 1):
                arrived(w.at[kc, f, 0 : 2 + rel], "w", "rest", kc, rel)

                @pl.when(wc == 0)
                def _():
                    send(w.at[kc, f], w.at[kc, f], ("t", "wf"), h_dev, "wf")

    lane = {"A": lo, "B": other}

    def receivers(zz):
        found = set()
        for src in TREE:
            for to in TREE[src].get(zz, ()):
                if not (zz < EARLY <= to):
                    found.add((to, 0, goes_to(src, to)))
                    if src == zz:
                        found.add((to, 1, goes_to(src, to)))
        found.add((zz, 1, 1))
        for early_plane, late_plane in LINKS.items():
            if late_plane == zz:
                found |= {(early_plane, i, core_of_probe(early_plane)) for i in (0, 1)}
        return len(found)

    def hop(typ, src, kc, zz, to):
        ref = pb.at[lane[typ], src, kc]
        target = dev(x, goes_to(src, to), y, to)
        if TREE[src].get(to):
            send(ref, ref, ("p", "z", typ, src, kc), target, "relay")
        else:
            send(ref, ref, ("t", "in", src), target, "relay")

    def start(kc, zz, to):
        ref = pb.at[lo, zz, kc]
        core_ = goes_to(zz, to)
        for typ, from_, lane_ in (("A", ref, y), ("B", b_send.at[kc], mate)):
            key = ("p", "z", typ, zz, kc) if TREE[zz].get(to) else ("t", "in", zz)
            send(from_, ref, key, dev(x, core_, lane_, to), "own")

    def item(code):
        return "AB"[code % 2], code // 4, code // 2 % 2

    def begin(zz):
        loaded(pb.at[0, 0:2], "own")
        pl.semaphore_wait(barrier, receivers(zz) + (1 if zz >= EARLY else 0))
        for early_plane, late_plane in LINKS.items():
            if late_plane == zz:
                for yy in (y, mate):
                    to = p_dev(yy, early_plane)
                    pl.semaphore_signal(go_late, inc=1, device_id=to, device_id_type=MESH)
        for kc in (0, 1):
            for to in TREE[zz][zz]:
                if not (zz < EARLY <= to):
                    start(kc, zz, to)
            send(b_send.at[kc], pb.at[lo, zz, kc], ("t", "twin"), dev(x, 1, mate, zz), "own")

    def pass_on(zz):
        seen, missing, held = {}, set(), []
        for code in WAITS[zz]:
            if code < 0:
                pl.semaphore_wait(go_late, 2)
                for kc in (0, 1):
                    for to in TREE[zz][zz]:
                        if zz < EARLY <= to:
                            start(kc, zz, to)
                for one in held:
                    hop(*one)
                held = None
                continue
            typ, src, kc = item(code)
            arrived(pb.at[lane[typ], src, kc], "p", "z", typ, src, kc)
            for to in TREE[src][zz]:
                if zz < EARLY <= to and held is not None:
                    held.append((typ, src, kc, zz, to))
                else:
                    hop(typ, src, kc, zz, to)
            seen[src] = seen.get(src, 0) + 1
            if seen[src] == 4 and zz < FIRST:
                for typ in "AB":
                    ref = pb.at[lane[typ], src]
                    send(ref, ref, ("t", "in", src), w_dev, "fw")

    def probe_sent(zz):
        sent(pb.at[0, 0 : 2 * len(TREE[zz][zz]) + 1], "own")
        passed = [src for src in TREE if src != zz and TREE[src].get(zz)]
        count = sum(len(TREE[src][zz]) for src in passed)
        assert count <= NZ
        sent(pb.at[:, 0:count], "relay")
        if zz < FIRST:
            sent(pb.at[:, 0 : len(passed)], "fw")

    @pl.when(core == hc)
    def _():
        def pushes():
            for i in range(4):
                loaded(pb.at[0], ("in", i))
                out_s[i] = (v_pg[i].astype(F32) + v_comp[i]).astype(BF16)
                send(out_s.at[i], out_s.at[i], ("w", "push", i), w_dev, "push")
            loaded(v_comp.at[0], "state")
            q_s[...] = prm[...] - (RATE * NEST * NEST) * mom[...]
            send(q_s, q_s, ("w", "q"), w_dev, "q")

        @pl.when(jnp.logical_not(late))
        def _():
            pl.semaphore_wait(go, 1)
            pushes()

        for zz in range(NZ):
            pl.when(z == zz)(lambda zz=zz: begin(zz))

        @pl.when(late)
        def _():
            pushes()

        for zz in range(NZ):
            pl.when(z == zz)(lambda zz=zz: pass_on(zz))

    @pl.when(core == 1)
    def _():
        near = z // HALF

        @pl.when(wc == 0)
        def _():
            arrived(w, "t", "wf")

        @pl.when(wc == 1)
        def _():
            loaded(pb.at[0, 0], "own")

        for kc in (0, 1):
            w_t[kc] = w[kc].reshape(256, KC).T

        def wait_blocks(zz, want_near):
            if want_near:
                arrived(pb.at[0, 0], "t", "twin")
            for src in TREE:
                if src != zz and (src // HALF == zz // HALF) == want_near:
                    if zz < FIRST or not TREE[src].get(zz):
                        arrived(pb.at[0, 0:2], "t", "in", src)

        for phase in (0, 1):
            h = near if phase == 0 else 1 - near
            for zz in range(NZ):
                pl.when(z == zz)(lambda zz=zz: wait_blocks(zz, phase == 0))
            acc = jnp.zeros((2 * HALF * 16, 256), F32)
            for kc in (0, 1):
                rows = pb[:, pl.ds(h * HALF, HALF), kc].reshape(2 * HALF * 16, KC)
                acc += jnp.dot(rows, w_t[kc], preferred_element_type=F32)
            for lp in (0, 1):
                for lw in (0, 1):
                    piece = acc[lp * 96 : lp * 96 + 96, lw * 128 : lw * 128 + 128]
                    part[phase, lp, lw] = piece.astype(BF16).reshape(HALF, 16, 128)
            for lp in (0, 1):
                for lw in (0, 1):
                    to = 4 * lp + 2 * h + lw

                    @pl.when(to != y)
                    def _():
                        send(part.at[phase, lp, lw], y_in.at[y], ("t", "y"), dev(x, 1, to, z), "y")

                    @pl.when(to == y)
                    def _():
                        y_in[y] = part[phase, lp, lw]

        arrived(y_in.at[0:7], "t", "y")
        total = y_in[0].astype(F32)
        for i in range(1, NY):
            total += y_in[i].astype(F32)
        outb[:, x] = total.astype(BF16)
        mine = outb.at[:, x]
        for d in (2, 1, 3):
            for cc in (1, 0):
                send(mine, mine, ("t", "out"), dev(xat(d), cc, y, z), "out")
        send(mine, mine, ("t", "out"), dev(x, 0, y, z), "out")

    @pl.when(core == hc)
    def _():
        arrived(sum_s, "p", "sum")
        for i, (kind, kc) in enumerate(ORDER):
            at = columns(kind, kc)
            avg = sum_s[i]
            m = NEST * mom[:, at] + avg
            n_mom[:, at] = m
            n_prm[:, at] = prm[:, at] - RATE * (avg + NEST * m)
        sent(out_s, "push")
        sent(q_s, "q")
        for zz in range(NZ):
            pl.when(z == zz)(lambda zz=zz: probe_sent(zz))

    @pl.when(core == wc)
    def _():
        sent(pb.at[0], "rs")
        sent(pb.at[:, 0:7], "ag")
        sent(sum_s, "sum")

        @pl.when(wc == 0)
        def _():
            sent(w, "wf")

    @pl.when(core == 1)
    def _():
        sent(y_in.at[0:7], "y")
        sent(y_in.at[0:7], "out")
        arrived(y_in.at[0:3], "t", "out")

    @pl.when(core == 0)
    def _():
        arrived(y_in.at[0:4], "t", "out")

    assert max(len(keys[g].at) for g in "wp") <= SHARED and len(keys["t"].at) <= N_RECV - SHARED
    assert len(sk.at) <= N_SEND and len(lk.at) <= N_LOCAL


def store(a, b, c, a_out, b_out, c_out, sem):
    copies = [
        pltpu.make_async_copy(src, dst, sem.at[i])
        for i, (src, dst) in enumerate(((a, a_out), (b, b_out), (c, c_out)))
    ]
    for cp in copies:
        cp.start()
    for cp in copies:
        cp.wait()


def per_device(pseudo_grad, compensation, params, momentum, probe):
    any_space = pl.BlockSpec(memory_space=pl.ANY)
    vmem = pl.BlockSpec(memory_space=pltpu.VMEM)
    shapes = (
        jax.ShapeDtypeStruct((16, K), F32),
        jax.ShapeDtypeStruct((16, K), F32),
        jax.ShapeDtypeStruct((6, NX, 16, 128), BF16),
    )
    outs = pl.pallas_call(
        kernel,
        out_shape=tuple(pltpu.VMEM(s.shape, s.dtype) for s in shapes),
        in_specs=[any_space] * 5,
        out_specs=[vmem] * 3,
        scratch_shapes=[
            pltpu.VMEM((4, 8, 16, KC), BF16),
            pltpu.VMEM((4, 8, 16, KC), F32),
            pltpu.VMEM((4, 8, 16, KC), BF16),
            pltpu.VMEM((4, 8, 16, KC), BF16),
            pltpu.VMEM((4, 2, 16, KC), BF16),
            pltpu.VMEM((4, 2, 2, 16, KC), BF16),
            pltpu.VMEM((4, 2, 16, KC), BF16),
            pltpu.VMEM((16, K), F32),
            pltpu.VMEM((16, K), F32),
            pltpu.VMEM((16, K), F32),
            pltpu.VMEM((4, 16, KC), F32),
            pltpu.VMEM((2, 2, NX, 2, 16, KC), BF16),
            pltpu.VMEM((2, KC, 256), BF16),
            pltpu.VMEM((2, 2, 16, KC), BF16),
            pltpu.VMEM((2, NZ, 2, 16, KC), BF16),
            pltpu.VMEM((2, 16, KC), BF16),
            pltpu.VMEM((2, 2, 2, HALF, 16, 128), BF16),
            pltpu.VMEM((NY, HALF, 16, 128), BF16),
            pltpu.SemaphoreType.DMA((N_SEND,)),
            pltpu.SemaphoreType.DMA((N_RECV,)),
            pltpu.SemaphoreType.DMA((N_LOCAL,)),
            pltpu.SemaphoreType.REGULAR,
            pltpu.SemaphoreType.REGULAR,
        ],
        compiler_params=pltpu.CompilerParams(
            collective_id=0, has_side_effects=True, vmem_limit_bytes=60 * 2**20
        ),
    )(
        pseudo_grad.reshape(8, 16, K),
        compensation.reshape(8, 16, K),
        params,
        momentum,
        probe.reshape(NX, 16, K),
    )
    new_params, new_momentum, out = pl.pallas_call(
        store,
        out_shape=shapes,
        in_specs=[any_space] * 3,
        out_specs=[any_space] * 3,
        scratch_shapes=[pltpu.SemaphoreType.DMA((3,))],
        compiler_params=pltpu.CompilerParams(vmem_limit_bytes=2**20),
    )(*outs)
    return new_params, new_momentum, out.reshape(384, 128)


def solution(mesh):
    in_specs = (
        P("replica", "fsdp", "tensor"),
        P("replica", "fsdp", "tensor"),
        P(("fsdp", "replica"), "tensor"),
        P(("fsdp", "replica"), "tensor"),
        P("fsdp", "tensor"),
    )
    out_specs = (
        P(("fsdp", "replica"), "tensor"),
        P(("fsdp", "replica"), "tensor"),
        P("tensor", "fsdp"),
    )
    return jax.shard_map(
        per_device, mesh=mesh, in_specs=in_specs, out_specs=out_specs, check_vma=False
    )
```

```python
import jax
import jax.numpy as jnp
from jax import lax
from jax.experimental import pallas as pl
from jax.experimental.pallas import tpu as pltpu
from jax.sharding import PartitionSpec as P

MESH = pl.DeviceIdType.MESH
RATE = 0.7
NEST = 0.9
F32, BF16 = jnp.float32, jnp.bfloat16

NX, NY, NZ = 4, 8, 12
K = 4608
KC = K // 4
HALF = NZ // 2
FIRST = 1
EARLY = 6
ORDER = (("P", 0), ("P", 1), ("O", 0), ("O", 1))
TREE = {
    0: {0: (1, 11,), 1: (2,), 2: (3,), 3: (4,), 4: (5,), 5: (6,), 8: (9, 7,), 10: (8,), 11: (10,)},
    1: {0: (11,), 1: (2, 0,), 2: (3,), 3: (4,), 4: (5,), 5: (6,), 6: (7,), 9: (8, 10,), 11: (9,)},
    2: {0: (11,), 1: (0,), 2: (1, 3,), 3: (4,), 4: (5,), 5: (6,), 6: (7,), 7: (8,), 10: (9,), 11: (10,)},
    3: {0: (11,), 1: (0,), 2: (1,), 3: (2, 4,), 4: (5,), 5: (6,), 6: (7,), 7: (8,), 10: (9,), 11: (10,)},
    4: {0: (11,), 1: (0,), 2: (1,), 3: (2,), 4: (3, 5,), 5: (6,), 6: (7,), 7: (8,), 8: (9,), 9: (10,)},
    5: {1: (0,), 2: (1,), 3: (2,), 4: (3,), 5: (4, 6,), 6: (7,), 7: (8,), 8: (11, 9,), 9: (10,)},
    6: {1: (0, 2,), 2: (3,), 4: (5,), 6: (4, 8, 7, 1,), 8: (9,), 9: (10,), 10: (11,)},
    7: {2: (1,), 3: (2, 4,), 4: (5,), 6: (3,), 7: (8, 6,), 8: (9, 10,), 10: (11, 0,)},
    8: {0: (1, 11,), 3: (2,), 4: (5, 3,), 5: (6,), 7: (4,), 8: (7, 9,), 9: (0,), 11: (10,)},
    9: {0: (11, 1,), 1: (2,), 4: (3, 5,), 6: (4,), 7: (6, 8,), 9: (7, 0,), 11: (10,)},
    10: {0: (1,), 1: (2,), 4: (3,), 6: (5,), 7: (6,), 8: (7,), 9: (4,), 10: (9, 8, 11,), 11: (0,)},
    11: {1: (0, 2,), 2: (3,), 3: (4,), 6: (5, 7,), 9: (8,), 10: (9, 6,), 11: (1, 10,)},
}
WAITS = (
    (4, 6, 5, 7, 8, 10, 9, 11, -1, 12, 14, 13, 15, 36, 40, 16, 38, 37, 42, 18, 41, 32, 17, 39, 43, 34, 19, 33, 35),
    (0, 8, 2, 1, 10, 9, 3, 11, 12, 14, 13, 15, 16, 44, 18, 46, 45, 17, 24, 47, 19, 25, 26, 20, 22, 27, 36, 21, 40, 23, 38, 37, 42, 41, 39, 43),
    (4, 6, 5, 12, 7, 0, 14, 2, 13, 1, 15, 3, 16, 18, 17, 19, 20, 22, 21, 44, 23, 46, 45, 24, 47, 28, 30, 25, 26, 29, 31, 27),
    (8, 10, 9, 11, 4, 16, 6, 5, 18, 17, 7, 0, 19, 2, 1, 3, 20, 22, 21, 23, 28, 30, 29, 31, 44, 32, 46, 34, 45, 33, 47, 35),
    (12, 14, 13, 8, 15, 10, 20, 9, 22, 11, 21, 4, 23, 24, 6, 5, 7, 0, 25, 26, 2, 1, 27, 3, 32, 34, 33, 35, 28, 40, 30, 36, 29, 41, 42, 31, 38, 37, 39, 43),
    (16, 18, 17, 12, -1, 19, 14, 13, 8, 15, 10, 9, 11, 4, 6, 5, 0, 7, 2, 1, 32, 3, 34, 33, 35),
    (28, 30, 20, 29, 22, 31, 21, 16, 23, 18, 17, 12, 19, 36, 14, 13, 8, 38, 15, 37, 10, 9, 39, 4, 11, 40, 6, 44, 5, 46, 7, 41, 42, 45, 47, 43),
    (32, 34, 33, 36, 35, 38, 37, 20, 39, 22, 21, 16, 40, 23, 18, 17, 41, 12, 42, 19, 14, 13, 8, 43, 15, 10, 9, 11),
    (28, 30, 29, 24, 31, 26, 25, 40, 27, 41, 42, 43, 20, 22, 21, 16, 23, 18, 17, 0, 19, 2, 1, 3),
    (32, 40, 34, 33, 35, 41, 42, 43, 24, 44, 46, 45, 26, 25, 47, 27, 4, 20, 6, 22, 5, 21, 7, 16, 23, 18, 17, 19),
    (44, 46, 45, 47, 28, 30, 0, 29, 2, 31, 1, 24, 3, 8, 26, 10, 25, 9, 27, 11, 12, 14, 13, 15),
    (40, 42, 41, 43, 0, 2, 1, 3, 4, 6, 8, 5, 7, 10, 9, 11, 12, 14, 13, 15, 36, 38, 37, 32, 39, 34, 33, 35),
)
LINKS = {0: NZ - 1, EARLY - 1: EARLY}
SHARED = 50
N_RECV, N_SEND, N_LOCAL = SHARED + 16, 12, 6


class Keys:
    def __init__(self):
        self.at = {}

    def __call__(self, *key):
        return self.at.setdefault(key, len(self.at))


def kernel(
    pg_hbm, comp_hbm, prm_hbm, mom_hbm, probe_hbm,
    n_prm, n_mom, outb,
    v_pg, v_comp, out_s, cs, r_opp, r_fin, t_acc, prm, mom, q_s, sum_s,
    w, w_t, wy, pb, b_send, part, y_in,
    send_sem, recv_sem, loc_sem, go, go_late,
):
    rep = lax.axis_index("replica")
    fs = lax.axis_index("fsdp")
    t = lax.axis_index("tensor")
    x, core = rep // 2, rep % 2
    lo, z = fs // NZ, fs % NZ
    other = 1 - lo
    y = t * 2 + lo
    mate = t * 2 + other

    def dev(x_, core_, y_, z_):
        return (x_ * 2 + core_, (y_ % 2) * NZ + z_, y_ // 2)

    def xat(d):
        return lax.rem(x + d + NX, NX)

    def yat(d):
        return lax.rem(y + d + NY, NY)

    def zat(d):
        return lax.rem(z + d + NZ, NZ)

    def w_core(z_):
        return jnp.where(z_ < FIRST, 1, 0)

    wc = w_core(z)
    hc = 1 - wc
    w_dev, h_dev, me = dev(x, wc, y, z), dev(x, hc, y, z), dev(x, core, y, z)

    keys, sk, lk = {group: Keys() for group in "wpt"}, Keys(), Keys()

    def rsem(group, *key):
        at = keys[group](*key)
        return recv_sem.at[SHARED + at if group == "t" else at]

    def ssem(group):
        return send_sem.at[sk(group)]

    def send(src, dst, key, to, group):
        pltpu.make_async_remote_copy(
            src_ref=src, dst_ref=dst, send_sem=ssem(group), recv_sem=rsem(*key),
            device_id=to, device_id_type=MESH,
        ).start()

    def arrived(like, *key):
        pltpu.make_async_remote_copy(
            src_ref=like, dst_ref=like, send_sem=send_sem.at[0], recv_sem=rsem(*key),
            device_id=me, device_id_type=MESH,
        ).wait_recv()

    def sent(like, group):
        pltpu.make_async_remote_copy(
            src_ref=like, dst_ref=like, send_sem=ssem(group), recv_sem=recv_sem.at[0],
            device_id=me, device_id_type=MESH,
        ).wait_send()

    def load(src, dst, key):
        pltpu.make_async_copy(src, dst, loc_sem.at[lk(key)]).start()

    def loaded(like, key):
        pltpu.make_async_remote_copy(
            src_ref=like, dst_ref=like, send_sem=send_sem.at[0], recv_sem=loc_sem.at[lk(key)],
            device_id=me, device_id_type=MESH,
        ).wait_recv()

    def columns(kind, kc):
        half = lo if kind == "O" else other
        return pl.ds(pl.multiple_of((half * 2 + kc) * KC, KC), KC)

    def load_chunk(i):
        at = columns(*ORDER[i])
        load(pg_hbm.at[:, :, at], v_pg.at[i], ("in", i))
        load(comp_hbm.at[:, :, at], v_comp.at[i], ("in", i))

    barrier = pltpu.get_barrier_semaphore()

    def greet(to):
        pl.semaphore_signal(barrier, inc=1, device_id=to, device_id_type=MESH)

    def core_of_probe(zz):
        return 0 if zz < FIRST else 1

    def p_dev(y_, zz):
        return dev(x, core_of_probe(zz), y_, zz)

    def goes_to(src, zz):
        return core_of_probe(zz) if TREE[src].get(zz) else 1

    def senders(zz, to_core):
        found = {}
        for src in TREE:
            for q, to in TREE[src].items():
                if zz in to and goes_to(src, zz) == to_core:
                    found[0, q] = y
                    if q == src:
                        found[1, q] = mate
        if to_core == 1:
            found[1, zz] = mate
        if zz in LINKS and to_core == core_of_probe(zz):
            found[0, LINKS[zz]], found[1, LINKS[zz]] = y, mate
        return [(found[key], key[1]) for key in sorted(found)]

    late = z >= EARLY

    @pl.when(core == hc)
    def _():
        @pl.when(jnp.logical_not(late))
        def _():
            load_chunk(0)

        greet(w_dev)
        for zz in range(NZ):

            @pl.when(z == zz)
            def _():
                for yy, q in senders(zz, core_of_probe(zz)):
                    if not (q < EARLY <= zz):
                        greet(p_dev(yy, q))

        for kc in (0, 1):
            load(probe_hbm.at[x, :, columns("O", kc)], pb.at[lo, z, kc], "own")
            load(probe_hbm.at[x, :, columns("P", kc)], b_send.at[kc], "own")

        @pl.when(late)
        def _():
            load_chunk(0)

    @pl.when(core == wc)
    def _():
        for d in (1, -1):
            greet(dev(xat(d), wc, y, z))
            greet(dev(xat(d), wc, mate, z))

        @pl.when(wc == 0)
        def _():
            greet(dev(x, wc, mate, z))

        for zz in range(FIRST):

            @pl.when(z == zz)
            def _():
                for yy, q in senders(zz, 1):
                    greet(p_dev(yy, q))

        @pl.when(wc == 1)
        def _():
            for kc in (0, 1):
                load(probe_hbm.at[x, :, columns("O", kc)], pb.at[lo, z, kc], "own")

        @pl.when(late)
        def _():
            greet(h_dev)

        load_chunk(0)

    @pl.when(core == 1)
    def _():
        for d in range(1, NY):
            greet(dev(x, wc, yat(d), z))

    for i in (1, 2, 3):
        load_chunk(i)
    load(prm_hbm, prm, "state")
    load(mom_hbm, mom, "state")

    @pl.when(core == wc)
    def _():
        right, left, far = xat(1), xat(-1), xat(2)
        rdev, ldev = dev(right, wc, y, z), dev(left, wc, y, z)
        pl.semaphore_wait(barrier, 1 + 4 + 7 + hc)

        @pl.when(jnp.logical_not(late))
        def _():
            pl.semaphore_signal(go, inc=1, device_id=h_dev, device_id_type=MESH)

        def chip_sum(i, s):
            return v_pg[i, s].astype(F32) + v_comp[i, s] + out_s[i, s].astype(F32)

        def opposite(i):
            loaded(pb.at[0], ("in", i))
            arrived(out_s.at[i], "w", "push", i)
            for side, to in ((1, rdev), (0, ldev)):
                s = far * 2 + side
                cs[i, s] = chip_sum(i, s).astype(BF16)
                send(cs.at[i, s], r_opp.at[i, side], ("w", "opp", i, side), to, "rs")

        def direct(i):
            for side, to, xx in ((0, rdev, right), (1, ldev, left)):
                s = xx * 2 + side
                cs[i, s] = chip_sum(i, s).astype(BF16)
                send(cs.at[i, s], r_fin.at[i, side, 0], ("w", "fin", i), to, "rs")

        def on_the_way(i):
            for side, to, xx in ((1, rdev, right), (0, ldev, left)):
                s = xx * 2 + side
                arrived(r_opp.at[i, side], "w", "opp", i, side)
                t_acc[i, side] = (chip_sum(i, s) + r_opp[i, side].astype(F32)).astype(BF16)
                send(t_acc.at[i, side], r_fin.at[i, side, 1], ("w", "fin", i), to, "rs")

        opposite(0)
        opposite(1)
        direct(0)
        direct(1)
        opposite(2)
        opposite(3)
        on_the_way(0)
        on_the_way(1)
        direct(2)
        direct(3)
        on_the_way(2)
        on_the_way(3)

        loaded(v_comp.at[0], "state")
        arrived(q_s, "w", "q")

        def gather(src, kc, y_, rel):
            for side, to, first in ((1, right, True), (0, left, True), (0, right, False), (1, left, False)):
                key = ("w", "ag", kc, rel, side) if first else ("w", "rest", kc, rel)
                send(src.at[side], w.at[kc, lo, x, side], key, dev(to, wc, y_, z), "ag")

        def relay(kc, f, rel):
            for side, to, xx in ((1, rdev, left), (0, ldev, right)):
                ref = w.at[kc, f, xx, side]
                arrived(ref, "w", "ag", kc, rel, side)
                send(ref, ref, ("w", "rest", kc, rel), to, "ag")

        for i, (kind, kc) in enumerate(ORDER):
            at = columns(kind, kc)
            arrived(r_fin.at[i], "w", "fin", i)

            def average(side):
                return (
                    chip_sum(i, x * 2 + side)
                    + r_fin[i, side, 0].astype(F32)
                    + r_fin[i, side, 1].astype(F32)
                ) * 0.125

            avg = average(wc)
            m = NEST * mom[:, at] + avg
            new = prm[:, at] - RATE * (avg + NEST * m)
            n_mom[:, at] = m
            n_prm[:, at] = new
            avg = average(hc)
            sum_s[i] = avg
            new_h = q_s[:, at] - (RATE * (1 + NEST)) * avg
            if kind == "O":
                w[kc, lo, x, wc] = new.astype(BF16)
                w[kc, lo, x, hc] = new_h.astype(BF16)
                gather(w.at[kc, lo, x], kc, y, 0)
            else:
                wy[kc, wc] = new.astype(BF16)
                wy[kc, hc] = new_h.astype(BF16)
                gather(wy.at[kc], kc, mate, 1)
                for side in (0, 1):
                    send(wy.at[kc, side], w.at[kc, lo, x, side], ("w", "rest", kc, 1), dev(x, wc, mate, z), "ag")
            send(sum_s.at[i], sum_s.at[i], ("p", "sum"), h_dev, "sum")

        for rel, f in ((1, other), (0, lo)):
            for kc in (0, 1):
                relay(kc, f, rel)
        for rel, f in ((1, other), (0, lo)):
            for kc in (0, 1):
                arrived(w.at[kc, f, 0 : 2 + rel], "w", "rest", kc, rel)

                @pl.when(wc == 0)
                def _():
                    send(w.at[kc, f], w.at[kc, f], ("t", "wf"), h_dev, "wf")

    lane = {"A": lo, "B": other}

    def receivers(zz):
        found = set()
        for src in TREE:
            for to in TREE[src].get(zz, ()):
                if not (zz < EARLY <= to):
                    found.add((to, 0, goes_to(src, to)))
                    if src == zz:
                        found.add((to, 1, goes_to(src, to)))
        found.add((zz, 1, 1))
        for early_plane, late_plane in LINKS.items():
            if late_plane == zz:
                found |= {(early_plane, i, core_of_probe(early_plane)) for i in (0, 1)}
        return len(found)

    def hop(typ, src, kc, zz, to):
        ref = pb.at[lane[typ], src, kc]
        target = dev(x, goes_to(src, to), y, to)
        if TREE[src].get(to):
            send(ref, ref, ("p", "z", typ, src, kc), target, "relay")
        else:
            send(ref, ref, ("t", "in", src), target, "relay")

    def start(kc, zz, to):
        ref = pb.at[lo, zz, kc]
        core_ = goes_to(zz, to)
        for typ, from_, lane_ in (("A", ref, y), ("B", b_send.at[kc], mate)):
            key = ("p", "z", typ, zz, kc) if TREE[zz].get(to) else ("t", "in", zz)
            send(from_, ref, key, dev(x, core_, lane_, to), "own")

    def item(code):
        return "AB"[code % 2], code // 4, code // 2 % 2

    def begin(zz):
        loaded(pb.at[0, 0:2], "own")
        pl.semaphore_wait(barrier, receivers(zz) + (1 if zz >= EARLY else 0))
        for early_plane, late_plane in LINKS.items():
            if late_plane == zz:
                for yy in (y, mate):
                    to = p_dev(yy, early_plane)
                    pl.semaphore_signal(go_late, inc=1, device_id=to, device_id_type=MESH)
        for kc in (0, 1):
            for to in TREE[zz][zz]:
                if not (zz < EARLY <= to):
                    start(kc, zz, to)
            send(b_send.at[kc], pb.at[lo, zz, kc], ("t", "twin"), dev(x, 1, mate, zz), "own")

    def pass_on(zz):
        seen, missing, held = {}, set(), []
        for code in WAITS[zz]:
            if code < 0:
                pl.semaphore_wait(go_late, 2)
                for kc in (0, 1):
                    for to in TREE[zz][zz]:
                        if zz < EARLY <= to:
                            start(kc, zz, to)
                for one in held:
                    hop(*one)
                held = None
                continue
            typ, src, kc = item(code)
            arrived(pb.at[lane[typ], src, kc], "p", "z", typ, src, kc)
            for to in TREE[src][zz]:
                if zz < EARLY <= to and held is not None:
                    held.append((typ, src, kc, zz, to))
                else:
                    hop(typ, src, kc, zz, to)
            seen[src] = seen.get(src, 0) + 1
            if seen[src] == 4 and zz < FIRST:
                for typ in "AB":
                    ref = pb.at[lane[typ], src]
                    send(ref, ref, ("t", "in", src), w_dev, "fw")

    def probe_sent(zz):
        sent(pb.at[0, 0 : 2 * len(TREE[zz][zz]) + 1], "own")
        passed = [src for src in TREE if src != zz and TREE[src].get(zz)]
        count = sum(len(TREE[src][zz]) for src in passed)
        assert count <= NZ
        sent(pb.at[:, 0:count], "relay")
        if zz < FIRST:
            sent(pb.at[:, 0 : len(passed)], "fw")

    @pl.when(core == hc)
    def _():
        def pushes():
            for i in range(4):
                loaded(pb.at[0], ("in", i))
                out_s[i] = (v_pg[i].astype(F32) + v_comp[i]).astype(BF16)
                send(out_s.at[i], out_s.at[i], ("w", "push", i), w_dev, "push")
            loaded(v_comp.at[0], "state")
            q_s[...] = prm[...] - (RATE * NEST * NEST) * mom[...]
            send(q_s, q_s, ("w", "q"), w_dev, "q")

        def pushes_early():
            pl.semaphore_wait(go, 1)
            pushes()

        pl.when(z < FIRST)(pushes_early)
        for zz in range(NZ):
            pl.when(z == zz)(lambda zz=zz: begin(zz))
        pl.when(jnp.logical_and(z >= FIRST, z < EARLY))(pushes_early)
        pl.when(late)(pushes)
        for zz in range(NZ):
            pl.when(z == zz)(lambda zz=zz: pass_on(zz))

    @pl.when(core == 1)
    def _():
        near = z // HALF

        @pl.when(wc == 0)
        def _():
            arrived(w, "t", "wf")

        @pl.when(wc == 1)
        def _():
            loaded(pb.at[0, 0], "own")

        for kc in (0, 1):
            w_t[kc] = w[kc].reshape(256, KC).T

        def wait_blocks(zz, want_near):
            if want_near:
                arrived(pb.at[0, 0], "t", "twin")
            for src in TREE:
                if src != zz and (src // HALF == zz // HALF) == want_near:
                    if zz < FIRST or not TREE[src].get(zz):
                        arrived(pb.at[0, 0:2], "t", "in", src)

        for phase in (0, 1):
            h = near if phase == 0 else 1 - near
            for zz in range(NZ):
                pl.when(z == zz)(lambda zz=zz: wait_blocks(zz, phase == 0))
            acc = jnp.zeros((2 * HALF * 16, 256), F32)
            for kc in (0, 1):
                rows = pb[:, pl.ds(h * HALF, HALF), kc].reshape(2 * HALF * 16, KC)
                acc += jnp.dot(rows, w_t[kc], preferred_element_type=F32)
            for lp in (0, 1):
                for lw in (0, 1):
                    piece = acc[lp * 96 : lp * 96 + 96, lw * 128 : lw * 128 + 128]
                    part[phase, lp, lw] = piece.astype(BF16).reshape(HALF, 16, 128)
            for lp in (0, 1):
                for lw in (0, 1):
                    to = 4 * lp + 2 * h + lw

                    @pl.when(to != y)
                    def _():
                        send(part.at[phase, lp, lw], y_in.at[y], ("t", "y"), dev(x, 1, to, z), "y")

                    @pl.when(to == y)
                    def _():
                        y_in[y] = part[phase, lp, lw]

        arrived(y_in.at[0:7], "t", "y")
        total = y_in[0].astype(F32)
        for i in range(1, NY):
            total += y_in[i].astype(F32)
        outb[:, x] = total.astype(BF16)
        mine = outb.at[:, x]
        for d in (2, 1, 3):
            for cc in (1, 0):
                send(mine, mine, ("t", "out"), dev(xat(d), cc, y, z), "out")
        send(mine, mine, ("t", "out"), dev(x, 0, y, z), "out")

    @pl.when(core == hc)
    def _():
        arrived(sum_s, "p", "sum")
        for i, (kind, kc) in enumerate(ORDER):
            at = columns(kind, kc)
            avg = sum_s[i]
            m = NEST * mom[:, at] + avg
            n_mom[:, at] = m
            n_prm[:, at] = prm[:, at] - RATE * (avg + NEST * m)
        sent(out_s, "push")
        sent(q_s, "q")
        for zz in range(NZ):
            pl.when(z == zz)(lambda zz=zz: probe_sent(zz))

    @pl.when(core == wc)
    def _():
        sent(pb.at[0], "rs")
        sent(pb.at[:, 0:7], "ag")
        sent(sum_s, "sum")

        @pl.when(wc == 0)
        def _():
            sent(w, "wf")

    @pl.when(core == 1)
    def _():
        sent(y_in.at[0:7], "y")
        sent(y_in.at[0:7], "out")
        arrived(y_in.at[0:3], "t", "out")

    @pl.when(core == 0)
    def _():
        arrived(y_in.at[0:4], "t", "out")

    assert max(len(keys[g].at) for g in "wp") <= SHARED and len(keys["t"].at) <= N_RECV - SHARED
    assert len(sk.at) <= N_SEND and len(lk.at) <= N_LOCAL


def store(a, b, c, a_out, b_out, c_out, sem):
    copies = [
        pltpu.make_async_copy(src, dst, sem.at[i])
        for i, (src, dst) in enumerate(((a, a_out), (b, b_out), (c, c_out)))
    ]
    for cp in copies:
        cp.start()
    for cp in copies:
        cp.wait()


def per_device(pseudo_grad, compensation, params, momentum, probe):
    any_space = pl.BlockSpec(memory_space=pl.ANY)
    vmem = pl.BlockSpec(memory_space=pltpu.VMEM)
    shapes = (
        jax.ShapeDtypeStruct((16, K), F32),
        jax.ShapeDtypeStruct((16, K), F32),
        jax.ShapeDtypeStruct((6, NX, 16, 128), BF16),
    )
    outs = pl.pallas_call(
        kernel,
        out_shape=tuple(pltpu.VMEM(s.shape, s.dtype) for s in shapes),
        in_specs=[any_space] * 5,
        out_specs=[vmem] * 3,
        scratch_shapes=[
            pltpu.VMEM((4, 8, 16, KC), BF16),
            pltpu.VMEM((4, 8, 16, KC), F32),
            pltpu.VMEM((4, 8, 16, KC), BF16),
            pltpu.VMEM((4, 8, 16, KC), BF16),
            pltpu.VMEM((4, 2, 16, KC), BF16),
            pltpu.VMEM((4, 2, 2, 16, KC), BF16),
            pltpu.VMEM((4, 2, 16, KC), BF16),
            pltpu.VMEM((16, K), F32),
            pltpu.VMEM((16, K), F32),
            pltpu.VMEM((16, K), F32),
            pltpu.VMEM((4, 16, KC), F32),
            pltpu.VMEM((2, 2, NX, 2, 16, KC), BF16),
            pltpu.VMEM((2, KC, 256), BF16),
            pltpu.VMEM((2, 2, 16, KC), BF16),
            pltpu.VMEM((2, NZ, 2, 16, KC), BF16),
            pltpu.VMEM((2, 16, KC), BF16),
            pltpu.VMEM((2, 2, 2, HALF, 16, 128), BF16),
            pltpu.VMEM((NY, HALF, 16, 128), BF16),
            pltpu.SemaphoreType.DMA((N_SEND,)),
            pltpu.SemaphoreType.DMA((N_RECV,)),
            pltpu.SemaphoreType.DMA((N_LOCAL,)),
            pltpu.SemaphoreType.REGULAR,
            pltpu.SemaphoreType.REGULAR,
        ],
        compiler_params=pltpu.CompilerParams(
            collective_id=0, has_side_effects=True, vmem_limit_bytes=60 * 2**20
        ),
    )(
        pseudo_grad.reshape(8, 16, K),
        compensation.reshape(8, 16, K),
        params,
        momentum,
        probe.reshape(NX, 16, K),
    )
    new_params, new_momentum, out = pl.pallas_call(
        store,
        out_shape=shapes,
        in_specs=[any_space] * 3,
        out_specs=[any_space] * 3,
        scratch_shapes=[pltpu.SemaphoreType.DMA((3,))],
        compiler_params=pltpu.CompilerParams(vmem_limit_bytes=2**20),
    )(*outs)
    return new_params, new_momentum, out.reshape(384, 128)


def solution(mesh):
    in_specs = (
        P("replica", "fsdp", "tensor"),
        P("replica", "fsdp", "tensor"),
        P(("fsdp", "replica"), "tensor"),
        P(("fsdp", "replica"), "tensor"),
        P("fsdp", "tensor"),
    )
    out_specs = (
        P(("fsdp", "replica"), "tensor"),
        P(("fsdp", "replica"), "tensor"),
        P("tensor", "fsdp"),
    )
    return jax.shard_map(
        per_device, mesh=mesh, in_specs=in_specs, out_specs=out_specs, check_vma=False
    )
```

```python
import jax
import jax.numpy as jnp
from jax import lax
from jax.experimental import pallas as pl
from jax.experimental.pallas import tpu as pltpu
from jax.sharding import PartitionSpec as P

MESH = pl.DeviceIdType.MESH
RATE = 0.7
NEST = 0.9
F32, BF16 = jnp.float32, jnp.bfloat16

NX, NY, NZ = 4, 8, 12
K = 4608
KC = K // 4
HALF = NZ // 2
FIRST = 1
EARLY = 6
ORDER = (("P", 0), ("P", 1), ("O", 0), ("O", 1))
TREE = {
    0: {0: (1, 11,), 1: (2,), 2: (3,), 3: (4,), 4: (5,), 5: (6,), 9: (7, 8,), 10: (9,), 11: (10,)},
    1: {0: (11,), 1: (2, 0,), 2: (3,), 3: (4,), 4: (5,), 5: (6,), 6: (7,), 10: (8, 9,), 11: (10,)},
    2: {0: (11,), 1: (0,), 2: (3, 1,), 3: (4,), 4: (5,), 5: (6,), 6: (7,), 7: (8,), 10: (9,), 11: (10,)},
    3: {0: (11,), 1: (0,), 2: (1,), 3: (4, 2,), 4: (5,), 5: (6,), 6: (7,), 7: (8,), 9: (10,), 11: (9,)},
    4: {0: (11,), 1: (0,), 2: (1,), 3: (2,), 4: (3, 5,), 5: (6,), 6: (8,), 8: (9, 7,), 11: (10,)},
    5: {1: (0,), 2: (1,), 3: (2,), 4: (3,), 5: (6, 4,), 6: (8,), 8: (9, 7,), 9: (10,), 10: (11,)},
    6: {1: (0, 2,), 4: (3, 5,), 6: (7, 4, 1,), 7: (8,), 8: (9,), 9: (10,), 10: (11,)},
    7: {0: (11,), 2: (1,), 3: (2, 4,), 4: (5,), 7: (3, 6, 8,), 8: (0, 9,), 11: (10,)},
    8: {0: (1,), 3: (2, 4,), 6: (7, 3, 5,), 8: (0, 6, 9,), 9: (10,), 10: (11,)},
    9: {1: (2,), 2: (3,), 5: (4,), 6: (5, 7,), 8: (6,), 9: (8, 10,), 10: (1, 11,), 11: (0,)},
    10: {0: (11,), 1: (0, 2,), 2: (3,), 3: (4,), 6: (5,), 7: (6,), 8: (7,), 10: (8, 9, 1,)},
    11: {2: (1, 3,), 5: (4,), 7: (6,), 8: (7,), 9: (0, 5,), 10: (9, 8,), 11: (10, 2,)},
}
WAITS = (
    (4, -1, 5, 15, 13, 6, 10, 7, 11, 14, 8, 9, 12, 33, 32, 42, 41, 35, 43, 34, 40, 16, 28, 19, 30, 17, 29, 18, 31),
    (1, 0, 3, 2, 9, 8, 10, 11, 15, 13, 12, 14, 40, 42, 41, 18, 43, 24, 26, 19, 16, 25, 38, 27, 37, 17, 20, 22, 21, 36, 39, 23),
    (4, 6, 5, 7, 14, 15, 13, 12, 17, 18, 0, 3, 19, 2, 1, 16, 21, 22, 40, 20, 23, 42, 41, 44, 30, 43, 28, 46, 45, 47, 29, 31, 38, 37, 36, 39),
    (10, 8, 18, 9, 11, 17, 16, 19, 4, 21, 7, 6, 5, 22, 23, 20, 28, 0, 30, 3, 1, 2, 29, 31, 40, 32, 34, 35, 41, 42, 33, 43),
    (21, 20, 22, 8, 23, 12, 10, 13, 14, 11, 9, 4, 15, 25, 24, 27, 7, 6, 0, 30, 5, 1, 3, 2, 29, 28, 26, 31),
    (-1, 16, 17, 18, 14, 19, 12, 10, 13, 9, 8, 15, 11, 4, 7, 6, 37, 5, 0, 44, 36, 38, 46, 1, 2, 3, 39, 47, 45),
    (32, 35, 34, 23, 22, 20, 21, 33, 16, 18, 37, 17, 36, 13, 38, 14, 19, 40, 12, 39, 9, 42, 15, 10, 41, 8, 6, 43, 11, 4, 7, 5),
    (24, 26, 25, 27, 40, 42, 41, 43, 44, 46, 47, 14, 45, 12, 13, 15, 9, 8, 10, 11),
    (40, 37, 36, 30, 38, 24, 28, 41, 31, 42, 26, 29, 27, 43, 39, 25, 46, 44, 45, 23, 47, 20, 16, 21, 18, 22, 17, 19),
    (44, 46, 47, 45, 35, 34, 33, 32, 1, 25, 26, 23, 3, 2, 0, 24, 27, 21, 20, 22, 14, 15, 13, 12),
    (36, 38, 44, 46, 45, 37, 39, 47, 1, 2, 0, 3, 4, 5, 10, 35, 33, 11, 34, 25, 32, 6, 26, 7, 23, 9, 27, 24, 21, 8, 22, 20),
    (1, 2, 0, 3, 36, 4, 38, 5, 6, 37, 15, 10, 11, 13, 14, 7, 9, 8, 12, 39, 28, 16, 30, 19, 17, 18, 29, 31),
)
LINKS = {0: NZ - 1, EARLY - 1: EARLY}
SHARED = 50
N_RECV, N_SEND, N_LOCAL = SHARED + 16, 12, 6


class Keys:
    def __init__(self):
        self.at = {}

    def __call__(self, *key):
        return self.at.setdefault(key, len(self.at))


def kernel(
    pg_hbm, comp_hbm, prm_hbm, mom_hbm, probe_hbm,
    n_prm, n_mom, outb,
    v_pg, v_comp, out_s, cs, r_opp, r_fin, t_acc, prm, mom, q_s, sum_s,
    w, w_t, wy, pb, b_send, part, y_in,
    send_sem, recv_sem, loc_sem, go, go_late, token,
):
    rep = lax.axis_index("replica")
    fs = lax.axis_index("fsdp")
    t = lax.axis_index("tensor")
    x, core = rep // 2, rep % 2
    lo, z = fs // NZ, fs % NZ
    other = 1 - lo
    y = t * 2 + lo
    mate = t * 2 + other

    def dev(x_, core_, y_, z_):
        return (x_ * 2 + core_, (y_ % 2) * NZ + z_, y_ // 2)

    def xat(d):
        return lax.rem(x + d + NX, NX)

    def yat(d):
        return lax.rem(y + d + NY, NY)

    def zat(d):
        return lax.rem(z + d + NZ, NZ)

    def w_core(z_):
        return jnp.where(z_ < FIRST, 1, 0)

    wc = w_core(z)
    hc = 1 - wc
    w_dev, h_dev, me = dev(x, wc, y, z), dev(x, hc, y, z), dev(x, core, y, z)

    keys, sk, lk = {group: Keys() for group in "wpt"}, Keys(), Keys()

    def rsem(group, *key):
        at = keys[group](*key)
        return recv_sem.at[SHARED + at if group == "t" else at]

    def ssem(group):
        return send_sem.at[sk(group)]

    def send(src, dst, key, to, group):
        pltpu.make_async_remote_copy(
            src_ref=src, dst_ref=dst, send_sem=ssem(group), recv_sem=rsem(*key),
            device_id=to, device_id_type=MESH,
        ).start()

    def arrived(like, *key):
        pltpu.make_async_remote_copy(
            src_ref=like, dst_ref=like, send_sem=send_sem.at[0], recv_sem=rsem(*key),
            device_id=me, device_id_type=MESH,
        ).wait_recv()

    def sent(like, group):
        pltpu.make_async_remote_copy(
            src_ref=like, dst_ref=like, send_sem=ssem(group), recv_sem=recv_sem.at[0],
            device_id=me, device_id_type=MESH,
        ).wait_send()

    def load(src, dst, key):
        pltpu.make_async_copy(src, dst, loc_sem.at[lk(key)]).start()

    def loaded(like, key):
        pltpu.make_async_remote_copy(
            src_ref=like, dst_ref=like, send_sem=send_sem.at[0], recv_sem=loc_sem.at[lk(key)],
            device_id=me, device_id_type=MESH,
        ).wait_recv()

    def columns(kind, kc):
        half = lo if kind == "O" else other
        return pl.ds(pl.multiple_of((half * 2 + kc) * KC, KC), KC)

    def load_chunk(i):
        at = columns(*ORDER[i])
        load(pg_hbm.at[:, :, at], v_pg.at[i], ("in", i))
        load(comp_hbm.at[:, :, at], v_comp.at[i], ("in", i))

    barrier = pltpu.get_barrier_semaphore()

    def greet(to):
        pl.semaphore_signal(barrier, inc=1, device_id=to, device_id_type=MESH)

    def core_of_probe(zz):
        return 0 if zz < FIRST else 1

    def p_dev(y_, zz):
        return dev(x, core_of_probe(zz), y_, zz)

    def goes_to(src, zz):
        return core_of_probe(zz) if TREE[src].get(zz) else 1

    def senders(zz, to_core):
        found = {}
        for src in TREE:
            for q, to in TREE[src].items():
                if zz in to and goes_to(src, zz) == to_core:
                    found[0, q] = y
                    if q == src:
                        found[1, q] = mate
        if to_core == 1:
            found[1, zz] = mate
        if zz in LINKS and to_core == core_of_probe(zz):
            found[0, LINKS[zz]], found[1, LINKS[zz]] = y, mate
        return [(found[key], key[1]) for key in sorted(found)]

    late = z >= EARLY

    @pl.when(core == hc)
    def _():
        @pl.when(jnp.logical_not(late))
        def _():
            load_chunk(0)

        greet(w_dev)
        for zz in range(NZ):

            @pl.when(z == zz)
            def _():
                for yy, q in senders(zz, core_of_probe(zz)):
                    if not (q < EARLY <= zz):
                        greet(p_dev(yy, q))

        for kc in (0, 1):
            load(probe_hbm.at[x, :, columns("O", kc)], pb.at[lo, z, kc], "own")
            load(probe_hbm.at[x, :, columns("P", kc)], b_send.at[kc], "own")

        @pl.when(late)
        def _():
            load_chunk(0)

    @pl.when(core == wc)
    def _():
        for d in (1, -1):
            greet(dev(xat(d), wc, y, z))
            greet(dev(xat(d), wc, mate, z))
            greet(dev(x, wc, yat(d), z))

        for zz in range(FIRST):

            @pl.when(z == zz)
            def _():
                for yy, q in senders(zz, 1):
                    greet(p_dev(yy, q))

        @pl.when(wc == 1)
        def _():
            for kc in (0, 1):
                load(probe_hbm.at[x, :, columns("O", kc)], pb.at[lo, z, kc], "own")

        @pl.when(late)
        def _():
            greet(h_dev)

        load_chunk(0)

    for i in (1, 2, 3):
        load_chunk(i)
    load(prm_hbm, prm, "state")
    load(mom_hbm, mom, "state")

    @pl.when(core == wc)
    def _():
        right, left, far = xat(1), xat(-1), xat(2)
        rdev, ldev = dev(right, wc, y, z), dev(left, wc, y, z)
        pl.semaphore_wait(barrier, 7)

        def pass_token(step):
            if step:
                pl.semaphore_wait(token.at[step - 1], 2)
            if step < NY // 2:
                for d in (1, -1):
                    to = dev(x, wc, yat(d), z)
                    pl.semaphore_signal(token.at[step], inc=1, device_id=to, device_id_type=MESH)

        pass_token(0)

        @pl.when(jnp.logical_not(late))
        def _():
            pl.semaphore_signal(go, inc=1, device_id=h_dev, device_id_type=MESH)

        def chip_sum(i, s):
            return v_pg[i, s].astype(F32) + v_comp[i, s] + out_s[i, s].astype(F32)

        def opposite(i):
            loaded(pb.at[0], ("in", i))
            arrived(out_s.at[i], "w", "push", i)
            for side, to in ((1, rdev), (0, ldev)):
                s = far * 2 + side
                cs[i, s] = chip_sum(i, s).astype(BF16)
                send(cs.at[i, s], r_opp.at[i, side], ("w", "opp", i, side), to, "rs")

        def direct(i):
            for side, to, xx in ((0, rdev, right), (1, ldev, left)):
                s = xx * 2 + side
                cs[i, s] = chip_sum(i, s).astype(BF16)
                send(cs.at[i, s], r_fin.at[i, side, 0], ("w", "fin", i), to, "rs")

        def on_the_way(i):
            for side, to, xx in ((1, rdev, right), (0, ldev, left)):
                s = xx * 2 + side
                arrived(r_opp.at[i, side], "w", "opp", i, side)
                t_acc[i, side] = (chip_sum(i, s) + r_opp[i, side].astype(F32)).astype(BF16)
                send(t_acc.at[i, side], r_fin.at[i, side, 1], ("w", "fin", i), to, "rs")

        opposite(0)
        opposite(1)
        direct(0)
        direct(1)
        opposite(2)
        opposite(3)
        pass_token(1)
        on_the_way(0)
        on_the_way(1)
        direct(2)
        direct(3)
        on_the_way(2)
        on_the_way(3)
        pass_token(2)

        loaded(v_comp.at[0], "state")
        arrived(q_s, "w", "q")

        def gather(src, kc, y_, rel):
            for side, to, first in ((1, right, True), (0, left, True), (0, right, False), (1, left, False)):
                key = ("w", "ag", kc, rel, side) if first else ("w", "rest", kc, rel)
                send(src.at[side], w.at[kc, lo, x, side], key, dev(to, wc, y_, z), "ag")

        def relay(kc, f, rel):
            for side, to, xx in ((1, rdev, left), (0, ldev, right)):
                ref = w.at[kc, f, xx, side]
                arrived(ref, "w", "ag", kc, rel, side)
                send(ref, ref, ("w", "rest", kc, rel), to, "ag")

        for i, (kind, kc) in enumerate(ORDER):
            at = columns(kind, kc)
            arrived(r_fin.at[i], "w", "fin", i)

            def average(side):
                return (
                    chip_sum(i, x * 2 + side)
                    + r_fin[i, side, 0].astype(F32)
                    + r_fin[i, side, 1].astype(F32)
                ) * 0.125

            avg = average(wc)
            m = NEST * mom[:, at] + avg
            new = prm[:, at] - RATE * (avg + NEST * m)
            n_mom[:, at] = m
            n_prm[:, at] = new
            avg = average(hc)
            sum_s[i] = avg
            new_h = q_s[:, at] - (RATE * (1 + NEST)) * avg
            if kind == "O":
                w[kc, lo, x, wc] = new.astype(BF16)
                w[kc, lo, x, hc] = new_h.astype(BF16)
                gather(w.at[kc, lo, x], kc, y, 0)
            else:
                wy[kc, wc] = new.astype(BF16)
                wy[kc, hc] = new_h.astype(BF16)
                gather(wy.at[kc], kc, mate, 1)
                for side in (0, 1):
                    send(wy.at[kc, side], w.at[kc, lo, x, side], ("w", "rest", kc, 1), dev(x, wc, mate, z), "ag")
            send(sum_s.at[i], sum_s.at[i], ("p", "sum"), h_dev, "sum")

        pass_token(3)
        for rel, f in ((1, other), (0, lo)):
            for kc in (0, 1):
                relay(kc, f, rel)
        pass_token(4)
        for rel, f in ((1, other), (0, lo)):
            for kc in (0, 1):
                arrived(w.at[kc, f, 0 : 2 + rel], "w", "rest", kc, rel)

                @pl.when(wc == 0)
                def _():
                    send(w.at[kc, f], w.at[kc, f], ("t", "wf"), h_dev, "wf")

    lane = {"A": lo, "B": other}

    def receivers(zz):
        found = set()
        for src in TREE:
            for to in TREE[src].get(zz, ()):
                if not (zz < EARLY <= to):
                    found.add((to, 0, goes_to(src, to)))
                    if src == zz:
                        found.add((to, 1, goes_to(src, to)))
        found.add((zz, 1, 1))
        for early_plane, late_plane in LINKS.items():
            if late_plane == zz:
                found |= {(early_plane, i, core_of_probe(early_plane)) for i in (0, 1)}
        return len(found)

    def hop(typ, src, kc, zz, to):
        ref = pb.at[lane[typ], src, kc]
        target = dev(x, goes_to(src, to), y, to)
        if TREE[src].get(to):
            send(ref, ref, ("p", "z", typ, src, kc), target, "relay")
        else:
            send(ref, ref, ("t", "in", src), target, "relay")

    def start(kc, zz, to):
        ref = pb.at[lo, zz, kc]
        core_ = goes_to(zz, to)
        for typ, from_, lane_ in (("A", ref, y), ("B", b_send.at[kc], mate)):
            key = ("p", "z", typ, zz, kc) if TREE[zz].get(to) else ("t", "in", zz)
            send(from_, ref, key, dev(x, core_, lane_, to), "own")

    def item(code):
        return "AB"[code % 2], code // 4, code // 2 % 2

    def begin(zz):
        loaded(pb.at[0, 0:2], "own")
        pl.semaphore_wait(barrier, receivers(zz) + (1 if zz >= EARLY else 0))
        for early_plane, late_plane in LINKS.items():
            if late_plane == zz:
                for yy in (y, mate):
                    to = p_dev(yy, early_plane)
                    pl.semaphore_signal(go_late, inc=1, device_id=to, device_id_type=MESH)
        for kc in (0, 1):
            for to in TREE[zz][zz]:
                if not (zz < EARLY <= to):
                    start(kc, zz, to)
            send(b_send.at[kc], pb.at[lo, zz, kc], ("t", "twin"), dev(x, 1, mate, zz), "own")

    def pass_on(zz):
        seen, missing, held = {}, set(), []
        for code in WAITS[zz]:
            if code < 0:
                pl.semaphore_wait(go_late, 2)
                for kc in (0, 1):
                    for to in TREE[zz][zz]:
                        if zz < EARLY <= to:
                            start(kc, zz, to)
                for one in held:
                    hop(*one)
                held = None
                continue
            typ, src, kc = item(code)
            arrived(pb.at[lane[typ], src, kc], "p", "z", typ, src, kc)
            for to in TREE[src][zz]:
                if zz < EARLY <= to and held is not None:
                    held.append((typ, src, kc, zz, to))
                else:
                    hop(typ, src, kc, zz, to)
            seen[src] = seen.get(src, 0) + 1
            if seen[src] == 4 and zz < FIRST:
                for typ in "AB":
                    ref = pb.at[lane[typ], src]
                    send(ref, ref, ("t", "in", src), w_dev, "fw")

    def probe_sent(zz):
        sent(pb.at[0, 0 : 2 * len(TREE[zz][zz]) + 1], "own")
        passed = [src for src in TREE if src != zz and TREE[src].get(zz)]
        count = sum(len(TREE[src][zz]) for src in passed)
        assert count <= NZ
        sent(pb.at[:, 0:count], "relay")
        if zz < FIRST:
            sent(pb.at[:, 0 : len(passed)], "fw")

    @pl.when(core == hc)
    def _():
        def pushes():
            for i in range(4):
                loaded(pb.at[0], ("in", i))
                out_s[i] = (v_pg[i].astype(F32) + v_comp[i]).astype(BF16)
                send(out_s.at[i], out_s.at[i], ("w", "push", i), w_dev, "push")
            loaded(v_comp.at[0], "state")
            q_s[...] = prm[...] - (RATE * NEST * NEST) * mom[...]
            send(q_s, q_s, ("w", "q"), w_dev, "q")

        def pushes_early():
            pl.semaphore_wait(go, 1)
            pushes()

        pl.when(z < FIRST)(pushes_early)
        for zz in range(NZ):
            pl.when(z == zz)(lambda zz=zz: begin(zz))
        pl.when(jnp.logical_and(z >= FIRST, z < EARLY))(pushes_early)
        pl.when(late)(pushes)
        for zz in range(NZ):
            pl.when(z == zz)(lambda zz=zz: pass_on(zz))

    @pl.when(core == 1)
    def _():
        near = z // HALF

        @pl.when(wc == 0)
        def _():
            arrived(w, "t", "wf")

        @pl.when(wc == 1)
        def _():
            loaded(pb.at[0, 0], "own")

        for kc in (0, 1):
            w_t[kc] = w[kc].reshape(256, KC).T

        def wait_blocks(zz, want_near):
            if want_near:
                arrived(pb.at[0, 0], "t", "twin")
            for src in TREE:
                if src != zz and (src // HALF == zz // HALF) == want_near:
                    if zz < FIRST or not TREE[src].get(zz):
                        arrived(pb.at[0, 0:2], "t", "in", src)

        for phase in (0, 1):
            h = near if phase == 0 else 1 - near
            for zz in range(NZ):
                pl.when(z == zz)(lambda zz=zz: wait_blocks(zz, phase == 0))
            acc = jnp.zeros((2 * HALF * 16, 256), F32)
            for kc in (0, 1):
                rows = pb[:, pl.ds(h * HALF, HALF), kc].reshape(2 * HALF * 16, KC)
                acc += jnp.dot(rows, w_t[kc], preferred_element_type=F32)
            for lp in (0, 1):
                for lw in (0, 1):
                    piece = acc[lp * 96 : lp * 96 + 96, lw * 128 : lw * 128 + 128]
                    part[phase, lp, lw] = piece.astype(BF16).reshape(HALF, 16, 128)
            for lp in (0, 1):
                for lw in (0, 1):
                    to = 4 * lp + 2 * h + lw

                    @pl.when(to != y)
                    def _():
                        send(part.at[phase, lp, lw], y_in.at[y], ("t", "y"), dev(x, 1, to, z), "y")

                    @pl.when(to == y)
                    def _():
                        y_in[y] = part[phase, lp, lw]

        arrived(y_in.at[0:7], "t", "y")
        total = y_in[0].astype(F32)
        for i in range(1, NY):
            total += y_in[i].astype(F32)
        outb[:, x] = total.astype(BF16)
        mine = outb.at[:, x]
        for d in (2, 1, 3):
            for cc in (1, 0):
                send(mine, mine, ("t", "out"), dev(xat(d), cc, y, z), "out")
        send(mine, mine, ("t", "out"), dev(x, 0, y, z), "out")

    @pl.when(core == hc)
    def _():
        arrived(sum_s, "p", "sum")
        for i, (kind, kc) in enumerate(ORDER):
            at = columns(kind, kc)
            avg = sum_s[i]
            m = NEST * mom[:, at] + avg
            n_mom[:, at] = m
            n_prm[:, at] = prm[:, at] - RATE * (avg + NEST * m)
        sent(out_s, "push")
        sent(q_s, "q")
        for zz in range(NZ):
            pl.when(z == zz)(lambda zz=zz: probe_sent(zz))

    @pl.when(core == wc)
    def _():
        sent(pb.at[0], "rs")
        sent(pb.at[:, 0:7], "ag")
        sent(sum_s, "sum")

        @pl.when(wc == 0)
        def _():
            sent(w, "wf")

    @pl.when(core == 1)
    def _():
        sent(y_in.at[0:7], "y")
        sent(y_in.at[0:7], "out")
        arrived(y_in.at[0:3], "t", "out")

    @pl.when(core == 0)
    def _():
        arrived(y_in.at[0:4], "t", "out")

    assert max(len(keys[g].at) for g in "wp") <= SHARED and len(keys["t"].at) <= N_RECV - SHARED
    assert len(sk.at) <= N_SEND and len(lk.at) <= N_LOCAL


def store(a, b, c, a_out, b_out, c_out, sem):
    copies = [
        pltpu.make_async_copy(src, dst, sem.at[i])
        for i, (src, dst) in enumerate(((a, a_out), (b, b_out), (c, c_out)))
    ]
    for cp in copies:
        cp.start()
    for cp in copies:
        cp.wait()


def per_device(pseudo_grad, compensation, params, momentum, probe):
    any_space = pl.BlockSpec(memory_space=pl.ANY)
    vmem = pl.BlockSpec(memory_space=pltpu.VMEM)
    shapes = (
        jax.ShapeDtypeStruct((16, K), F32),
        jax.ShapeDtypeStruct((16, K), F32),
        jax.ShapeDtypeStruct((6, NX, 16, 128), BF16),
    )
    outs = pl.pallas_call(
        kernel,
        out_shape=tuple(pltpu.VMEM(s.shape, s.dtype) for s in shapes),
        in_specs=[any_space] * 5,
        out_specs=[vmem] * 3,
        scratch_shapes=[
            pltpu.VMEM((4, 8, 16, KC), BF16),
            pltpu.VMEM((4, 8, 16, KC), F32),
            pltpu.VMEM((4, 8, 16, KC), BF16),
            pltpu.VMEM((4, 8, 16, KC), BF16),
            pltpu.VMEM((4, 2, 16, KC), BF16),
            pltpu.VMEM((4, 2, 2, 16, KC), BF16),
            pltpu.VMEM((4, 2, 16, KC), BF16),
            pltpu.VMEM((16, K), F32),
            pltpu.VMEM((16, K), F32),
            pltpu.VMEM((16, K), F32),
            pltpu.VMEM((4, 16, KC), F32),
            pltpu.VMEM((2, 2, NX, 2, 16, KC), BF16),
            pltpu.VMEM((2, KC, 256), BF16),
            pltpu.VMEM((2, 2, 16, KC), BF16),
            pltpu.VMEM((2, NZ, 2, 16, KC), BF16),
            pltpu.VMEM((2, 16, KC), BF16),
            pltpu.VMEM((2, 2, 2, HALF, 16, 128), BF16),
            pltpu.VMEM((NY, HALF, 16, 128), BF16),
            pltpu.SemaphoreType.DMA((N_SEND,)),
            pltpu.SemaphoreType.DMA((N_RECV,)),
            pltpu.SemaphoreType.DMA((N_LOCAL,)),
            pltpu.SemaphoreType.REGULAR,
            pltpu.SemaphoreType.REGULAR,
            pltpu.SemaphoreType.REGULAR((NY // 2,)),
        ],
        compiler_params=pltpu.CompilerParams(
            collective_id=0, has_side_effects=True, vmem_limit_bytes=60 * 2**20
        ),
    )(
        pseudo_grad.reshape(8, 16, K),
        compensation.reshape(8, 16, K),
        params,
        momentum,
        probe.reshape(NX, 16, K),
    )
    new_params, new_momentum, out = pl.pallas_call(
        store,
        out_shape=shapes,
        in_specs=[any_space] * 3,
        out_specs=[any_space] * 3,
        scratch_shapes=[pltpu.SemaphoreType.DMA((3,))],
        compiler_params=pltpu.CompilerParams(vmem_limit_bytes=2**20),
    )(*outs)
    return new_params, new_momentum, out.reshape(384, 128)


def solution(mesh):
    in_specs = (
        P("replica", "fsdp", "tensor"),
        P("replica", "fsdp", "tensor"),
        P(("fsdp", "replica"), "tensor"),
        P(("fsdp", "replica"), "tensor"),
        P("fsdp", "tensor"),
    )
    out_specs = (
        P(("fsdp", "replica"), "tensor"),
        P(("fsdp", "replica"), "tensor"),
        P("tensor", "fsdp"),
    )
    return jax.shard_map(
        per_device, mesh=mesh, in_specs=in_specs, out_specs=out_specs, check_vma=False
    )
```

```python
import jax
import jax.numpy as jnp
from jax import lax
from jax.experimental import pallas as pl
from jax.experimental.pallas import tpu as pltpu
from jax.sharding import PartitionSpec as P

MESH = pl.DeviceIdType.MESH
RATE = 0.7
NEST = 0.9
F32, BF16 = jnp.float32, jnp.bfloat16

NX, NY, NZ = 4, 8, 12
K = 4608
KC = K // 4
HALF = NZ // 2
EARLY = 6
ORDER = (("P", 0), ("P", 1), ("O", 0), ("O", 1))
TREE = {
    0: {0: (11, 1,), 1: (2,), 2: (3,), 3: (4,), 4: (5,), 5: (6,), 7: (8,), 9: (7,), 10: (9,), 11: (10,)},
    1: {0: (11,), 1: (0, 2,), 2: (3,), 3: (4,), 4: (5,), 5: (6,), 6: (7,), 9: (8,), 10: (9,), 11: (10,)},
    2: {0: (11,), 1: (0,), 2: (3, 1,), 3: (4,), 4: (5,), 5: (6,), 6: (7,), 7: (8,), 10: (9,), 11: (10,)},
    3: {0: (11,), 1: (0,), 2: (1,), 3: (4, 2,), 4: (5,), 5: (6,), 6: (7,), 9: (10, 8,), 11: (9,)},
    4: {0: (11,), 1: (0,), 2: (1,), 3: (2,), 4: (3, 5,), 5: (6,), 6: (8,), 8: (7, 9,), 11: (10,)},
    5: {0: (11,), 1: (0,), 2: (1,), 3: (2,), 4: (3,), 5: (4, 6,), 6: (7,), 7: (9, 8,), 11: (10,)},
    6: {2: (3, 1,), 4: (5,), 6: (4, 7, 8, 2,), 7: (0,), 8: (9,), 9: (11, 10,)},
    7: {0: (1,), 3: (2,), 4: (3, 5,), 7: (8, 4,), 8: (6, 0, 9,), 9: (10,), 10: (11,)},
    8: {2: (1, 3,), 3: (4,), 6: (2, 7,), 7: (5,), 8: (9, 6, 10,), 9: (0,), 10: (11,)},
    9: {0: (1, 11,), 1: (2,), 5: (4, 6,), 7: (3, 5, 8,), 9: (7, 0,), 11: (10,)},
    10: {0: (11,), 1: (0,), 2: (3, 1,), 3: (4,), 4: (5,), 7: (6,), 8: (7,), 10: (8, 9, 2,)},
    11: {0: (1,), 2: (3,), 3: (4,), 6: (5,), 9: (7, 8,), 10: (0, 6, 9,), 11: (10, 2,)},
}
WAITS = (
    (-1, 5, 8, 7, 4, 6, 9, 15, 10, 11, 36, 39, 12, 38, 37, 14, 47, 28, 45, 19, 31, 13, 30, 17, 29, 18, 46, 44, 22, 16, 42, 21, 20, 23, 40, 41, 43),
    (0, 2, 3, 1, 9, 8, 10, 11, 13, 15, 12, 19, 17, 14, 40, 16, 18, 41, 22, 36, 42, 43, 39, 21, 20, 38, 37, 23),
    (6, 7, 0, 2, 5, 4, 3, 14, 1, 15, 13, 12, 17, 19, 18, 16, 46, 40, 44, 42, 41, 21, 22, 43, 20, 26, 23, 24, 25, 27, 45, 35, 47, 32, 33, 34),
    (11, 8, 6, 7, 10, 18, 9, 0, 5, 17, 19, 16, 4, 2, 20, 3, 22, 21, 23, 1, 46, 30, 42, 44, 40, 31, 41, 43, 29, 28, 45, 35, 47, 32, 33, 34),
    (20, 22, 8, 12, 21, 23, 14, 6, 11, 15, 13, 9, 10, 30, 7, 2, 0, 29, 3, 31, 26, 5, 1, 28, 4, 25, 42, 24, 40, 41, 43, 27),
    (-1, 18, 17, 19, 16, 12, 14, 13, 8, 15, 2, 11, 7, 9, 3, 10, 36, 1, 5, 6, 0, 38, 4, 37, 39),
    (35, 32, 33, 23, 34, 18, 22, 21, 17, 16, 20, 47, 14, 15, 44, 46, 19, 11, 45, 13, 12, 8, 10, 9, 7, 6, 5, 4),
    (36, 38, 37, 24, 25, 26, 39, 27, 35, 32, 23, 40, 34, 21, 33, 22, 42, 41, 43, 20, 3, 11, 2, 8, 0, 1, 9, 10),
    (28, 30, 31, 40, 42, 41, 29, 24, 25, 26, 43, 27, 17, 18, 16, 19),
    (46, 34, 32, 47, 35, 33, 45, 30, 28, 44, 3, 2, 31, 29, 24, 0, 26, 1, 25, 7, 5, 27, 6, 15, 4, 14, 13, 12),
    (46, 47, 45, 32, 44, 33, 3, 34, 2, 35, 0, 1, 5, 7, 6, 4, 8, 10, 11, 30, 9, 29, 31, 28),
    (2, 3, 0, 1, 5, 7, 6, 8, 4, 10, 15, 11, 9, 39, 38, 36, 37, 14, 13, 12, 18, 19, 17, 16, 22, 20, 23, 21),
)
LINKS = {0: NZ - 1, EARLY - 1: EARLY}
SHARED = 50
N_RECV, N_SEND, N_LOCAL = SHARED + 17, 12, 6


class Keys:
    def __init__(self):
        self.at = {}

    def __call__(self, *key):
        return self.at.setdefault(key, len(self.at))


def kernel(
    pg_hbm, comp_hbm, prm_hbm, mom_hbm, probe_hbm,
    n_prm, n_mom, outb,
    v_pg, v_comp, out_s, cs, r_opp, r_fin, t_acc, prm, mom, q_s, sum_s,
    w, w_t, wn, r_ag, pb, b_send, part, y_in,
    send_sem, recv_sem, loc_sem, go, go_late, token,
):
    rep = lax.axis_index("replica")
    fs = lax.axis_index("fsdp")
    t = lax.axis_index("tensor")
    x, core = rep // 2, rep % 2
    lo, z = fs // NZ, fs % NZ
    other = 1 - lo
    y = t * 2 + lo
    mate = t * 2 + other

    def dev(x_, core_, y_, z_):
        return (x_ * 2 + core_, (y_ % 2) * NZ + z_, y_ // 2)

    def xat(d):
        return lax.rem(x + d + NX, NX)

    def yat(d):
        return lax.rem(y + d + NY, NY)

    def zat(d):
        return lax.rem(z + d + NZ, NZ)

    w_dev, h_dev, me = dev(x, 0, y, z), dev(x, 1, y, z), dev(x, core, y, z)

    keys, sk, lk = {group: Keys() for group in "wpt"}, Keys(), Keys()

    def rsem(group, *key):
        at = keys[group](*key)
        return recv_sem.at[SHARED + at if group == "t" else at]

    def ssem(group):
        return send_sem.at[sk(group)]

    def send(src, dst, key, to, group):
        pltpu.make_async_remote_copy(
            src_ref=src, dst_ref=dst, send_sem=ssem(group), recv_sem=rsem(*key),
            device_id=to, device_id_type=MESH,
        ).start()

    def arrived(like, *key):
        pltpu.make_async_remote_copy(
            src_ref=like, dst_ref=like, send_sem=send_sem.at[0], recv_sem=rsem(*key),
            device_id=me, device_id_type=MESH,
        ).wait_recv()

    def sent(like, group):
        pltpu.make_async_remote_copy(
            src_ref=like, dst_ref=like, send_sem=ssem(group), recv_sem=recv_sem.at[0],
            device_id=me, device_id_type=MESH,
        ).wait_send()

    def load(src, dst, key):
        pltpu.make_async_copy(src, dst, loc_sem.at[lk(key)]).start()

    def loaded(like, key):
        pltpu.make_async_remote_copy(
            src_ref=like, dst_ref=like, send_sem=send_sem.at[0], recv_sem=loc_sem.at[lk(key)],
            device_id=me, device_id_type=MESH,
        ).wait_recv()

    def columns(kind, kc):
        half = lo if kind == "O" else other
        return pl.ds(pl.multiple_of((half * 2 + kc) * KC, KC), KC)

    def load_chunk(i):
        at = columns(*ORDER[i])
        load(pg_hbm.at[:, :, at], v_pg.at[i], ("in", i))
        load(comp_hbm.at[:, :, at], v_comp.at[i], ("in", i))

    barrier = pltpu.get_barrier_semaphore()

    def greet(to):
        pl.semaphore_signal(barrier, inc=1, device_id=to, device_id_type=MESH)

    def p_dev(y_, zz):
        return dev(x, 1, y_, zz)

    def senders(zz):
        found = {(1, zz): mate}
        for src in TREE:
            for q, to in TREE[src].items():
                if zz in to:
                    found[0, q] = y
                    if q == src:
                        found[1, q] = mate
        if zz in LINKS:
            found[0, LINKS[zz]], found[1, LINKS[zz]] = y, mate
        return [(found[key], key[1]) for key in sorted(found)]

    late = z >= EARLY

    @pl.when(core == 1)
    def _():
        @pl.when(jnp.logical_not(late))
        def _():
            load_chunk(0)

        greet(w_dev)
        for zz in range(NZ):

            @pl.when(z == zz)
            def _():
                for yy, q in senders(zz):
                    if not (q < EARLY <= zz):
                        greet(p_dev(yy, q))

        for kc in (0, 1):
            load(probe_hbm.at[x, :, columns("O", kc)], pb.at[lo, z, kc], "own")
            load(probe_hbm.at[x, :, columns("P", kc)], b_send.at[kc], "own")

        @pl.when(late)
        def _():
            load_chunk(0)

    @pl.when(core == 0)
    def _():
        load_chunk(0)
        for d in (1, -1):
            greet(dev(xat(d), 0, y, z))
            greet(dev(xat(d), 0, mate, z))
            greet(dev(x, 0, yat(d), z))

        @pl.when(late)
        def _():
            greet(h_dev)

    for i in (1, 2, 3):
        load_chunk(i)
    load(prm_hbm, prm, "state")
    load(mom_hbm, mom, "state")

    @pl.when(core == 0)
    def _():
        right, left, far = xat(1), xat(-1), xat(2)
        rdev, ldev = dev(right, 0, y, z), dev(left, 0, y, z)
        pl.semaphore_wait(barrier, 7)

        @pl.when(jnp.logical_not(late))
        def _():
            pl.semaphore_signal(go, inc=1, device_id=h_dev, device_id_type=MESH)

        def pass_token(step):
            if step:
                pl.semaphore_wait(token.at[step - 1], 2)
            if step < NY // 2:
                for d in (1, -1):
                    to = dev(x, 0, yat(d), z)
                    pl.semaphore_signal(token.at[step], inc=1, device_id=to, device_id_type=MESH)

        pass_token(0)

        def chip_sum(i, s):
            return v_pg[i, s].astype(F32) + v_comp[i, s] + out_s[i, s].astype(F32)

        def opposite(i):
            loaded(pb.at[0], ("in", i))
            arrived(out_s.at[i], "w", "push", i)
            for side, to in ((1, rdev), (0, ldev)):
                s = far * 2 + side
                cs[i, s] = chip_sum(i, s).astype(BF16)
                send(cs.at[i, s], r_opp.at[i, side], ("w", "opp", i, side), to, "rs")

        def direct(i):
            for side, to, xx in ((0, rdev, right), (1, ldev, left)):
                s = xx * 2 + side
                cs[i, s] = chip_sum(i, s).astype(BF16)
                send(cs.at[i, s], r_fin.at[i, side, 0], ("w", "fin", i), to, "rs")

        def on_the_way(i):
            for side, to, xx in ((1, rdev, right), (0, ldev, left)):
                s = xx * 2 + side
                arrived(r_opp.at[i, side], "w", "opp", i, side)
                t_acc[i, side] = (chip_sum(i, s) + r_opp[i, side].astype(F32)).astype(BF16)
                send(t_acc.at[i, side], r_fin.at[i, side, 1], ("w", "fin", i), to, "rs")

        opposite(0)
        opposite(1)
        direct(0)
        direct(1)
        opposite(2)
        opposite(3)
        pass_token(1)
        on_the_way(0)
        on_the_way(1)
        direct(2)
        direct(3)
        on_the_way(2)
        on_the_way(3)
        pass_token(2)

        loaded(v_comp.at[0], "state")
        arrived(q_s, "w", "q")

        def gather(src, kc, kind, first):
            y_, rel = (y, 0) if kind == "O" else (mate, 1)
            for side, xx in ((1, right), (0, left)):
                if first:
                    send(src.at[side], r_ag.at[kc, rel, side], ("w", "ag", kc, rel, side), dev(xx, 0, y_, z), "ag")
            if not first:
                for side, xx in ((0, right), (1, left), (0, x), (1, x)):
                    send(src.at[side], w.at[kc, lo, x, side], ("t", "w", kc), dev(xx, 1, y_, z), "ag")

        def relay(kc, rel):
            f = other if rel else lo
            for side, to, xx in ((1, right, left), (0, left, right)):
                ref = r_ag.at[kc, rel, side]
                arrived(ref, "w", "ag", kc, rel, side)
                for x_ in (to, x):
                    send(ref, w.at[kc, f, xx, side], ("t", "w", kc), dev(x_, 1, y, z), "ag")

        def block(i):
            kind, kc = ORDER[i]
            return wn.at[i], kc, kind

        for i, (kind, kc) in enumerate(ORDER):
            at = columns(kind, kc)
            arrived(r_fin.at[i], "w", "fin", i)

            def average(side):
                return (
                    chip_sum(i, x * 2 + side)
                    + r_fin[i, side, 0].astype(F32)
                    + r_fin[i, side, 1].astype(F32)
                ) * 0.125

            avg = average(0)
            m = NEST * mom[:, at] + avg
            new = prm[:, at] - RATE * (avg + NEST * m)
            n_mom[:, at] = m
            n_prm[:, at] = new
            wn[i, 0] = new.astype(BF16)
            avg = average(1)
            sum_s[i] = avg
            wn[i, 1] = (q_s[:, at] - (RATE * (1 + NEST)) * avg).astype(BF16)
            gather(*block(i), True)
            if i == 1:
                gather(*block(0), False)
        for i in (2, 1, 3):
            gather(*block(i), False)
        for i in range(4):
            send(sum_s.at[i], sum_s.at[i], ("p", "sum"), h_dev, "sum")

        pass_token(3)
        relay(0, 1)
        relay(1, 1)
        relay(0, 0)
        pass_token(4)
        relay(1, 0)

    lane = {"A": lo, "B": other}

    def receivers(zz):
        found = {(zz, 1)}
        for src in TREE:
            for to in TREE[src].get(zz, ()):
                if not (zz < EARLY <= to):
                    found |= {(to, 0), (to, 1)} if src == zz else {(to, 0)}
        for early_plane, late_plane in LINKS.items():
            if late_plane == zz:
                found |= {(early_plane, 0), (early_plane, 1)}
        return len(found)

    def hop(typ, src, kc, zz, to):
        ref = pb.at[lane[typ], src, kc]
        target = dev(x, 1, y, to)
        if TREE[src].get(to):
            send(ref, ref, ("p", "z", typ, src, kc), target, "relay")
        else:
            send(ref, ref, ("t", "in", src), target, "relay")

    def start(kc, zz, to):
        ref = pb.at[lo, zz, kc]
        for typ, from_, lane_ in (("A", ref, y), ("B", b_send.at[kc], mate)):
            key = ("p", "z", typ, zz, kc) if TREE[zz].get(to) else ("t", "in", zz)
            send(from_, ref, key, dev(x, 1, lane_, to), "own")

    def item(code):
        return "AB"[code % 2], code // 4, code // 2 % 2

    def begin(zz):
        loaded(pb.at[0, 0:2], "own")
        pl.semaphore_wait(barrier, receivers(zz) + (1 if zz >= EARLY else 0))
        for early_plane, late_plane in LINKS.items():
            if late_plane == zz:
                for yy in (y, mate):
                    to = p_dev(yy, early_plane)
                    pl.semaphore_signal(go_late, inc=1, device_id=to, device_id_type=MESH)
        for kc in (0, 1):
            for to in TREE[zz][zz]:
                if not (zz < EARLY <= to):
                    start(kc, zz, to)
            send(b_send.at[kc], pb.at[lo, zz, kc], ("t", "twin"), dev(x, 1, mate, zz), "own")

    def pass_on(zz):
        held = []
        for code in WAITS[zz]:
            if code < 0:
                pl.semaphore_wait(go_late, 2)
                for kc in (0, 1):
                    for to in TREE[zz][zz]:
                        if zz < EARLY <= to:
                            start(kc, zz, to)
                for one in held:
                    hop(*one)
                held = None
                continue
            typ, src, kc = item(code)
            arrived(pb.at[lane[typ], src, kc], "p", "z", typ, src, kc)
            for to in TREE[src][zz]:
                if zz < EARLY <= to and held is not None:
                    held.append((typ, src, kc, zz, to))
                else:
                    hop(typ, src, kc, zz, to)

    def probe_sent(zz):
        sent(pb.at[0, 0 : 2 * len(TREE[zz][zz]) + 1], "own")
        passed = [src for src in TREE if src != zz and TREE[src].get(zz)]
        count = sum(len(TREE[src][zz]) for src in passed)
        assert count <= NZ
        sent(pb.at[:, 0:count], "relay")

    @pl.when(core == 1)
    def _():
        def prepare(i):
            loaded(pb.at[0], ("in", i))
            out_s[i] = (v_pg[i].astype(F32) + v_comp[i]).astype(BF16)

        def push(i):
            send(out_s.at[i], out_s.at[i], ("w", "push", i), w_dev, "push")

        prepare(0)

        @pl.when(jnp.logical_not(late))
        def _():
            prepare(1)
            prepare(2)
            prepare(3)

        for zz in range(NZ):
            pl.when(z == zz)(lambda zz=zz: begin(zz))

        @pl.when(jnp.logical_not(late))
        def _():
            pl.semaphore_wait(go, 1)
            for i in range(4):
                push(i)

        @pl.when(late)
        def _():
            push(0)
            for i in (1, 2, 3):
                prepare(i)
                push(i)

        loaded(v_comp.at[0], "state")
        q_s[...] = prm[...] - (RATE * NEST * NEST) * mom[...]
        send(q_s, q_s, ("w", "q"), w_dev, "q")
        for zz in range(NZ):
            pl.when(z == zz)(lambda zz=zz: pass_on(zz))

    @pl.when(core == 1)
    def _():
        near = z // HALF

        for kc in (0, 1):
            arrived(w.at[kc], "t", "w", kc)
            w_t[kc] = w[kc].reshape(256, KC).T

        def wait_blocks(zz, want_near):
            if want_near:
                arrived(pb.at[0, 0], "t", "twin")
            for src in TREE:
                if src != zz and (src // HALF == zz // HALF) == want_near:
                    if not TREE[src].get(zz):
                        arrived(pb.at[0, 0:2], "t", "in", src)

        for phase in (0, 1):
            h = near if phase == 0 else 1 - near
            for zz in range(NZ):
                pl.when(z == zz)(lambda zz=zz: wait_blocks(zz, phase == 0))
            acc = jnp.zeros((2 * HALF * 16, 256), F32)
            for kc in (0, 1):
                rows = pb[:, pl.ds(h * HALF, HALF), kc].reshape(2 * HALF * 16, KC)
                acc += jnp.dot(rows, w_t[kc], preferred_element_type=F32)
            for lp in (0, 1):
                for lw in (0, 1):
                    piece = acc[lp * 96 : lp * 96 + 96, lw * 128 : lw * 128 + 128]
                    part[phase, lp, lw] = piece.astype(BF16).reshape(HALF, 16, 128)
            for lp in (0, 1):
                for lw in (0, 1):
                    to = 4 * lp + 2 * h + lw

                    @pl.when(to != y)
                    def _():
                        send(part.at[phase, lp, lw], y_in.at[y], ("t", "y"), dev(x, 1, to, z), "y")

                    @pl.when(to == y)
                    def _():
                        y_in[y] = part[phase, lp, lw]

        arrived(y_in.at[0:7], "t", "y")
        total = y_in[0].astype(F32)
        for i in range(1, NY):
            total += y_in[i].astype(F32)
        outb[:, x] = total.astype(BF16)
        mine = outb.at[:, x]
        for d in (2, 1, 3):
            for cc in (1, 0):
                send(mine, mine, ("t", "out"), dev(xat(d), cc, y, z), "out")
        send(mine, mine, ("t", "out"), dev(x, 0, y, z), "out")

    @pl.when(core == 1)
    def _():
        arrived(sum_s, "p", "sum")
        for i, (kind, kc) in enumerate(ORDER):
            at = columns(kind, kc)
            avg = sum_s[i]
            m = NEST * mom[:, at] + avg
            n_mom[:, at] = m
            n_prm[:, at] = prm[:, at] - RATE * (avg + NEST * m)
        sent(out_s, "push")
        sent(q_s, "q")
        for zz in range(NZ):
            pl.when(z == zz)(lambda zz=zz: probe_sent(zz))

    @pl.when(core == 0)
    def _():
        sent(pb.at[0], "rs")
        sent(pb.at[:, 0:10], "ag")
        sent(sum_s, "sum")

    @pl.when(core == 1)
    def _():
        sent(y_in.at[0:7], "y")
        sent(y_in.at[0:7], "out")
        arrived(y_in.at[0:3], "t", "out")

    @pl.when(core == 0)
    def _():
        arrived(y_in.at[0:4], "t", "out")

    assert max(len(keys[g].at) for g in "wp") <= SHARED and len(keys["t"].at) <= N_RECV - SHARED
    assert len(sk.at) <= N_SEND and len(lk.at) <= N_LOCAL


def store(a, b, c, a_out, b_out, c_out, sem):
    copies = [
        pltpu.make_async_copy(src, dst, sem.at[i])
        for i, (src, dst) in enumerate(((a, a_out), (b, b_out), (c, c_out)))
    ]
    for cp in copies:
        cp.start()
    for cp in copies:
        cp.wait()


def per_device(pseudo_grad, compensation, params, momentum, probe):
    any_space = pl.BlockSpec(memory_space=pl.ANY)
    vmem = pl.BlockSpec(memory_space=pltpu.VMEM)
    shapes = (
        jax.ShapeDtypeStruct((16, K), F32),
        jax.ShapeDtypeStruct((16, K), F32),
        jax.ShapeDtypeStruct((6, NX, 16, 128), BF16),
    )
    outs = pl.pallas_call(
        kernel,
        out_shape=tuple(pltpu.VMEM(s.shape, s.dtype) for s in shapes),
        in_specs=[any_space] * 5,
        out_specs=[vmem] * 3,
        scratch_shapes=[
            pltpu.VMEM((4, 8, 16, KC), BF16),
            pltpu.VMEM((4, 8, 16, KC), F32),
            pltpu.VMEM((4, 8, 16, KC), BF16),
            pltpu.VMEM((4, 8, 16, KC), BF16),
            pltpu.VMEM((4, 2, 16, KC), BF16),
            pltpu.VMEM((4, 2, 2, 16, KC), BF16),
            pltpu.VMEM((4, 2, 16, KC), BF16),
            pltpu.VMEM((16, K), F32),
            pltpu.VMEM((16, K), F32),
            pltpu.VMEM((16, K), F32),
            pltpu.VMEM((4, 16, KC), F32),
            pltpu.VMEM((2, 2, NX, 2, 16, KC), BF16),
            pltpu.VMEM((2, KC, 256), BF16),
            pltpu.VMEM((4, 2, 16, KC), BF16),
            pltpu.VMEM((2, 2, 2, 16, KC), BF16),
            pltpu.VMEM((2, NZ, 2, 16, KC), BF16),
            pltpu.VMEM((2, 16, KC), BF16),
            pltpu.VMEM((2, 2, 2, HALF, 16, 128), BF16),
            pltpu.VMEM((NY, HALF, 16, 128), BF16),
            pltpu.SemaphoreType.DMA((N_SEND,)),
            pltpu.SemaphoreType.DMA((N_RECV,)),
            pltpu.SemaphoreType.DMA((N_LOCAL,)),
            pltpu.SemaphoreType.REGULAR,
            pltpu.SemaphoreType.REGULAR,
            pltpu.SemaphoreType.REGULAR((NY // 2,)),
        ],
        compiler_params=pltpu.CompilerParams(
            collective_id=0, has_side_effects=True, vmem_limit_bytes=60 * 2**20
        ),
    )(
        pseudo_grad.reshape(8, 16, K),
        compensation.reshape(8, 16, K),
        params,
        momentum,
        probe.reshape(NX, 16, K),
    )
    new_params, new_momentum, out = pl.pallas_call(
        store,
        out_shape=shapes,
        in_specs=[any_space] * 3,
        out_specs=[any_space] * 3,
        scratch_shapes=[pltpu.SemaphoreType.DMA((3,))],
        compiler_params=pltpu.CompilerParams(vmem_limit_bytes=2**20),
    )(*outs)
    return new_params, new_momentum, out.reshape(384, 128)


def solution(mesh):
    in_specs = (
        P("replica", "fsdp", "tensor"),
        P("replica", "fsdp", "tensor"),
        P(("fsdp", "replica"), "tensor"),
        P(("fsdp", "replica"), "tensor"),
        P("fsdp", "tensor"),
    )
    out_specs = (
        P(("fsdp", "replica"), "tensor"),
        P(("fsdp", "replica"), "tensor"),
        P("tensor", "fsdp"),
    )
    return jax.shard_map(
        per_device, mesh=mesh, in_specs=in_specs, out_specs=out_specs, check_vma=False
    )
```

```python
import jax
import jax.numpy as jnp
from jax import lax
from jax.experimental import pallas as pl
from jax.experimental.pallas import tpu as pltpu
from jax.sharding import PartitionSpec as P

MESH = pl.DeviceIdType.MESH
RATE = 0.7
NEST = 0.9
F32, BF16 = jnp.float32, jnp.bfloat16

NX, NY, NZ = 4, 8, 12
K = 4608
KC = K // 4
HALF = NZ // 2
EARLY = 6
ORDER = (("P", 0), ("P", 1), ("O", 0), ("O", 1))
TREE = {
    0: {0: (1, 11,), 1: (2,), 2: (3,), 3: (4,), 4: (5,), 5: (6,), 9: (7, 8,), 10: (9,), 11: (10,)},
    1: {0: (11,), 1: (2, 0,), 2: (3,), 3: (4,), 4: (5,), 5: (6,), 6: (7,), 10: (8, 9,), 11: (10,)},
    2: {0: (11,), 1: (0,), 2: (3, 1,), 3: (4,), 4: (5,), 5: (6,), 6: (7,), 7: (8,), 10: (9,), 11: (10,)},
    3: {0: (11,), 1: (0,), 2: (1,), 3: (4, 2,), 4: (5,), 5: (6,), 6: (7,), 7: (8,), 9: (10,), 11: (9,)},
    4: {0: (11,), 1: (0,), 2: (1,), 3: (2,), 4: (3, 5,), 5: (6,), 6: (8,), 8: (9, 7,), 11: (10,)},
    5: {1: (0,), 2: (1,), 3: (2,), 4: (3,), 5: (6, 4,), 6: (8,), 8: (9, 7,), 9: (10,), 10: (11,)},
    6: {1: (0, 2,), 4: (3, 5,), 6: (7, 4, 1,), 7: (8,), 8: (9,), 9: (10,), 10: (11,)},
    7: {0: (11,), 2: (1,), 3: (2, 4,), 4: (5,), 7: (3, 6, 8,), 8: (0, 9,), 11: (10,)},
    8: {0: (1,), 3: (2, 4,), 6: (7, 3, 5,), 8: (0, 6, 9,), 9: (10,), 10: (11,)},
    9: {1: (2,), 2: (3,), 5: (4,), 6: (5, 7,), 8: (6,), 9: (8, 10,), 10: (1, 11,), 11: (0,)},
    10: {0: (11,), 1: (0, 2,), 2: (3,), 3: (4,), 6: (5,), 7: (6,), 8: (7,), 10: (8, 9, 1,)},
    11: {2: (1, 3,), 5: (4,), 7: (6,), 8: (7,), 9: (0, 5,), 10: (9, 8,), 11: (10, 2,)},
}
WAITS = (
    (4, -1, 5, 15, 13, 6, 10, 7, 11, 14, 8, 9, 12, 33, 32, 42, 41, 35, 43, 34, 40, 16, 28, 19, 30, 17, 29, 18, 31),
    (1, 0, 3, 2, 9, 8, 10, 11, 15, 13, 12, 14, 40, 42, 41, 18, 43, 24, 26, 19, 16, 25, 38, 27, 37, 17, 20, 22, 21, 36, 39, 23),
    (4, 6, 5, 7, 14, 15, 13, 12, 17, 18, 0, 3, 19, 2, 1, 16, 21, 22, 40, 20, 23, 42, 41, 44, 30, 43, 28, 46, 45, 47, 29, 31, 38, 37, 36, 39),
    (10, 8, 18, 9, 11, 17, 16, 19, 4, 21, 7, 6, 5, 22, 23, 20, 28, 0, 30, 3, 1, 2, 29, 31, 40, 32, 34, 35, 41, 42, 33, 43),
    (21, 20, 22, 8, 23, 12, 10, 13, 14, 11, 9, 4, 15, 25, 24, 27, 7, 6, 0, 30, 5, 1, 3, 2, 29, 28, 26, 31),
    (-1, 16, 17, 18, 14, 19, 12, 10, 13, 9, 8, 15, 11, 4, 7, 6, 37, 5, 0, 44, 36, 38, 46, 1, 2, 3, 39, 47, 45),
    (32, 35, 34, 23, 22, 20, 21, 33, 16, 18, 37, 17, 36, 13, 38, 14, 19, 40, 12, 39, 9, 42, 15, 10, 41, 8, 6, 43, 11, 4, 7, 5),
    (24, 26, 25, 27, 40, 42, 41, 43, 44, 46, 47, 14, 45, 12, 13, 15, 9, 8, 10, 11),
    (40, 37, 36, 30, 38, 24, 28, 41, 31, 42, 26, 29, 27, 43, 39, 25, 46, 44, 45, 23, 47, 20, 16, 21, 18, 22, 17, 19),
    (44, 46, 47, 45, 35, 34, 33, 32, 1, 25, 26, 23, 3, 2, 0, 24, 27, 21, 20, 22, 14, 15, 13, 12),
    (36, 38, 44, 46, 45, 37, 39, 47, 1, 2, 0, 3, 4, 5, 10, 35, 33, 11, 34, 25, 32, 6, 26, 7, 23, 9, 27, 24, 21, 8, 22, 20),
    (1, 2, 0, 3, 36, 4, 38, 5, 6, 37, 15, 10, 11, 13, 14, 7, 9, 8, 12, 39, 28, 16, 30, 19, 17, 18, 29, 31),
)
LINKS = {0: NZ - 1, EARLY - 1: EARLY}
SHARED = 50
N_RECV, N_SEND, N_LOCAL = SHARED + 17, 12, 6


class Keys:
    def __init__(self):
        self.at = {}

    def __call__(self, *key):
        return self.at.setdefault(key, len(self.at))


def kernel(
    pg_hbm, comp_hbm, prm_hbm, mom_hbm, probe_hbm,
    n_prm, n_mom, outb,
    v_pg, v_comp, out_s, cs, r_opp, r_fin, t_acc, prm, mom, q_s, sum_s,
    w, w_t, wn, r_ag, pb, b_send, part, y_in,
    send_sem, recv_sem, loc_sem, go, go_late, token,
):
    rep = lax.axis_index("replica")
    fs = lax.axis_index("fsdp")
    t = lax.axis_index("tensor")
    x, core = rep // 2, rep % 2
    lo, z = fs // NZ, fs % NZ
    other = 1 - lo
    y = t * 2 + lo
    mate = t * 2 + other

    def dev(x_, core_, y_, z_):
        return (x_ * 2 + core_, (y_ % 2) * NZ + z_, y_ // 2)

    def xat(d):
        return lax.rem(x + d + NX, NX)

    def yat(d):
        return lax.rem(y + d + NY, NY)

    def zat(d):
        return lax.rem(z + d + NZ, NZ)

    w_dev, h_dev, me = dev(x, 0, y, z), dev(x, 1, y, z), dev(x, core, y, z)

    keys, sk, lk = {group: Keys() for group in "wpt"}, Keys(), Keys()

    def rsem(group, *key):
        at = keys[group](*key)
        return recv_sem.at[SHARED + at if group == "t" else at]

    def ssem(group):
        return send_sem.at[sk(group)]

    def send(src, dst, key, to, group):
        pltpu.make_async_remote_copy(
            src_ref=src, dst_ref=dst, send_sem=ssem(group), recv_sem=rsem(*key),
            device_id=to, device_id_type=MESH,
        ).start()

    def arrived(like, *key):
        pltpu.make_async_remote_copy(
            src_ref=like, dst_ref=like, send_sem=send_sem.at[0], recv_sem=rsem(*key),
            device_id=me, device_id_type=MESH,
        ).wait_recv()

    def sent(like, group):
        pltpu.make_async_remote_copy(
            src_ref=like, dst_ref=like, send_sem=ssem(group), recv_sem=recv_sem.at[0],
            device_id=me, device_id_type=MESH,
        ).wait_send()

    def load(src, dst, key):
        pltpu.make_async_copy(src, dst, loc_sem.at[lk(key)]).start()

    def loaded(like, key):
        pltpu.make_async_remote_copy(
            src_ref=like, dst_ref=like, send_sem=send_sem.at[0], recv_sem=loc_sem.at[lk(key)],
            device_id=me, device_id_type=MESH,
        ).wait_recv()

    def columns(kind, kc):
        half = lo if kind == "O" else other
        return pl.ds(pl.multiple_of((half * 2 + kc) * KC, KC), KC)

    def load_chunk(i):
        at = columns(*ORDER[i])
        load(pg_hbm.at[:, :, at], v_pg.at[i], ("in", i))
        load(comp_hbm.at[:, :, at], v_comp.at[i], ("in", i))

    barrier = pltpu.get_barrier_semaphore()

    def greet(to):
        pl.semaphore_signal(barrier, inc=1, device_id=to, device_id_type=MESH)

    def p_dev(y_, zz):
        return dev(x, 1, y_, zz)

    def senders(zz):
        found = {(1, zz): mate}
        for src in TREE:
            for q, to in TREE[src].items():
                if zz in to:
                    found[0, q] = y
                    if q == src:
                        found[1, q] = mate
        if zz in LINKS:
            found[0, LINKS[zz]], found[1, LINKS[zz]] = y, mate
        return [(found[key], key[1]) for key in sorted(found)]

    late = z >= EARLY

    @pl.when(core == 1)
    def _():
        @pl.when(jnp.logical_not(late))
        def _():
            load_chunk(0)

        greet(w_dev)
        for zz in range(NZ):

            @pl.when(z == zz)
            def _():
                for yy, q in senders(zz):
                    if not (q < EARLY <= zz):
                        greet(p_dev(yy, q))

        for kc in (0, 1):
            load(probe_hbm.at[x, :, columns("O", kc)], pb.at[lo, z, kc], "own")
            load(probe_hbm.at[x, :, columns("P", kc)], b_send.at[kc], "own")

        @pl.when(late)
        def _():
            load_chunk(0)

    @pl.when(core == 0)
    def _():
        load_chunk(0)
        for d in (1, -1):
            greet(dev(xat(d), 0, y, z))
            greet(dev(xat(d), 0, mate, z))
            greet(dev(x, 0, yat(d), z))

        @pl.when(late)
        def _():
            greet(h_dev)

    for i in (1, 2, 3):
        load_chunk(i)
    load(prm_hbm, prm, "state")
    load(mom_hbm, mom, "state")

    @pl.when(core == 0)
    def _():
        right, left, far = xat(1), xat(-1), xat(2)
        rdev, ldev = dev(right, 0, y, z), dev(left, 0, y, z)
        pl.semaphore_wait(barrier, 7)

        @pl.when(jnp.logical_not(late))
        def _():
            pl.semaphore_signal(go, inc=1, device_id=h_dev, device_id_type=MESH)

        def pass_token(step):
            if step:
                pl.semaphore_wait(token.at[step - 1], 2)
            if step < NY // 2:
                for d in (1, -1):
                    to = dev(x, 0, yat(d), z)
                    pl.semaphore_signal(token.at[step], inc=1, device_id=to, device_id_type=MESH)

        pass_token(0)

        def chip_sum(i, s):
            return v_pg[i, s].astype(F32) + v_comp[i, s] + out_s[i, s].astype(F32)

        def opposite(i):
            loaded(pb.at[0], ("in", i))
            arrived(out_s.at[i], "w", "push", i)
            for side, to in ((1, rdev), (0, ldev)):
                s = far * 2 + side
                cs[i, s] = chip_sum(i, s).astype(BF16)
                send(cs.at[i, s], r_opp.at[i, side], ("w", "opp", i, side), to, "rs")

        def direct(i):
            for side, to, xx in ((0, rdev, right), (1, ldev, left)):
                s = xx * 2 + side
                cs[i, s] = chip_sum(i, s).astype(BF16)
                send(cs.at[i, s], r_fin.at[i, side, 0], ("w", "fin", i), to, "rs")

        def on_the_way(i):
            for side, to, xx in ((1, rdev, right), (0, ldev, left)):
                s = xx * 2 + side
                arrived(r_opp.at[i, side], "w", "opp", i, side)
                t_acc[i, side] = (chip_sum(i, s) + r_opp[i, side].astype(F32)).astype(BF16)
                send(t_acc.at[i, side], r_fin.at[i, side, 1], ("w", "fin", i), to, "rs")

        opposite(0)
        opposite(1)
        direct(0)
        direct(1)
        opposite(2)
        opposite(3)
        pass_token(1)
        on_the_way(0)
        on_the_way(1)
        direct(2)
        direct(3)
        on_the_way(2)
        on_the_way(3)
        pass_token(2)

        loaded(v_comp.at[0], "state")
        arrived(q_s, "w", "q")

        def gather(src, kc, kind, first):
            y_, rel = (y, 0) if kind == "O" else (mate, 1)
            for side, xx in ((1, right), (0, left)):
                if first:
                    send(src.at[side], r_ag.at[kc, rel, side], ("w", "ag", kc, rel, side), dev(xx, 0, y_, z), "ag")
            if not first:
                for side, xx in ((0, right), (1, left), (0, x), (1, x)):
                    send(src.at[side], w.at[kc, lo, x, side], ("t", "w", kc), dev(xx, 1, y_, z), "ag")

        def relay(kc, rel):
            f = other if rel else lo
            for side, to, xx in ((1, right, left), (0, left, right)):
                ref = r_ag.at[kc, rel, side]
                arrived(ref, "w", "ag", kc, rel, side)
                for x_ in (to, x):
                    send(ref, w.at[kc, f, xx, side], ("t", "w", kc), dev(x_, 1, y, z), "ag")

        def block(i):
            kind, kc = ORDER[i]
            return wn.at[i], kc, kind

        for i, (kind, kc) in enumerate(ORDER):
            at = columns(kind, kc)
            arrived(r_fin.at[i], "w", "fin", i)

            def average(side):
                return (
                    chip_sum(i, x * 2 + side)
                    + r_fin[i, side, 0].astype(F32)
                    + r_fin[i, side, 1].astype(F32)
                ) * 0.125

            avg = average(0)
            m = NEST * mom[:, at] + avg
            new = prm[:, at] - RATE * (avg + NEST * m)
            n_mom[:, at] = m
            n_prm[:, at] = new
            wn[i, 0] = new.astype(BF16)
            avg = average(1)
            sum_s[i] = avg
            wn[i, 1] = (q_s[:, at] - (RATE * (1 + NEST)) * avg).astype(BF16)
            gather(*block(i), True)
            if i == 1:
                gather(*block(0), False)
        for i in (2, 1, 3):
            gather(*block(i), False)
        for i in range(4):
            send(sum_s.at[i], sum_s.at[i], ("p", "sum"), h_dev, "sum")

        pass_token(3)
        relay(0, 1)
        relay(1, 1)
        relay(0, 0)
        pass_token(4)
        relay(1, 0)

    lane = {"A": lo, "B": other}

    def receivers(zz):
        found = {(zz, 1)}
        for src in TREE:
            for to in TREE[src].get(zz, ()):
                if not (zz < EARLY <= to):
                    found |= {(to, 0), (to, 1)} if src == zz else {(to, 0)}
        for early_plane, late_plane in LINKS.items():
            if late_plane == zz:
                found |= {(early_plane, 0), (early_plane, 1)}
        return len(found)

    def hop(typ, src, kc, zz, to):
        ref = pb.at[lane[typ], src, kc]
        target = dev(x, 1, y, to)
        if TREE[src].get(to):
            send(ref, ref, ("p", "z", typ, src, kc), target, "relay")
        else:
            send(ref, ref, ("t", "in", src), target, "relay")

    def start(kc, zz, to):
        ref = pb.at[lo, zz, kc]
        for typ, from_, lane_ in (("A", ref, y), ("B", b_send.at[kc], mate)):
            key = ("p", "z", typ, zz, kc) if TREE[zz].get(to) else ("t", "in", zz)
            send(from_, ref, key, dev(x, 1, lane_, to), "own")

    def item(code):
        return "AB"[code % 2], code // 4, code // 2 % 2

    def begin(zz):
        loaded(pb.at[0, 0:2], "own")
        pl.semaphore_wait(barrier, receivers(zz) + (1 if zz >= EARLY else 0))
        for early_plane, late_plane in LINKS.items():
            if late_plane == zz:
                for yy in (y, mate):
                    to = p_dev(yy, early_plane)
                    pl.semaphore_signal(go_late, inc=1, device_id=to, device_id_type=MESH)
        for kc in (0, 1):
            for to in TREE[zz][zz]:
                if not (zz < EARLY <= to):
                    start(kc, zz, to)
            send(b_send.at[kc], pb.at[lo, zz, kc], ("t", "twin"), dev(x, 1, mate, zz), "own")

    def pass_on(zz):
        held = []
        for code in WAITS[zz]:
            if code < 0:
                pl.semaphore_wait(go_late, 2)
                for kc in (0, 1):
                    for to in TREE[zz][zz]:
                        if zz < EARLY <= to:
                            start(kc, zz, to)
                for one in held:
                    hop(*one)
                held = None
                continue
            typ, src, kc = item(code)
            arrived(pb.at[lane[typ], src, kc], "p", "z", typ, src, kc)
            for to in TREE[src][zz]:
                if zz < EARLY <= to and held is not None:
                    held.append((typ, src, kc, zz, to))
                else:
                    hop(typ, src, kc, zz, to)

    def probe_sent(zz):
        sent(pb.at[0, 0 : 2 * len(TREE[zz][zz]) + 1], "own")
        passed = [src for src in TREE if src != zz and TREE[src].get(zz)]
        count = sum(len(TREE[src][zz]) for src in passed)
        assert count <= NZ
        sent(pb.at[:, 0:count], "relay")

    @pl.when(core == 1)
    def _():
        def prepare(i):
            loaded(pb.at[0], ("in", i))
            out_s[i] = (v_pg[i].astype(F32) + v_comp[i]).astype(BF16)

        def push(i):
            send(out_s.at[i], out_s.at[i], ("w", "push", i), w_dev, "push")

        prepare(0)

        @pl.when(jnp.logical_not(late))
        def _():
            prepare(1)
            prepare(2)
            prepare(3)

        for zz in range(NZ):
            pl.when(z == zz)(lambda zz=zz: begin(zz))

        @pl.when(jnp.logical_not(late))
        def _():
            pl.semaphore_wait(go, 1)
            for i in range(4):
                push(i)

        @pl.when(late)
        def _():
            push(0)
            for i in (1, 2, 3):
                prepare(i)
                push(i)

        loaded(v_comp.at[0], "state")
        q_s[...] = prm[...] - (RATE * NEST * NEST) * mom[...]
        send(q_s, q_s, ("w", "q"), w_dev, "q")
        for zz in range(NZ):
            pl.when(z == zz)(lambda zz=zz: pass_on(zz))

    @pl.when(core == 1)
    def _():
        near = z // HALF

        for kc in (0, 1):
            arrived(w.at[kc], "t", "w", kc)
            w_t[kc] = w[kc].reshape(256, KC).T

        def wait_blocks(zz, want_near):
            if want_near:
                arrived(pb.at[0, 0], "t", "twin")
            for src in TREE:
                if src != zz and (src // HALF == zz // HALF) == want_near:
                    if not TREE[src].get(zz):
                        arrived(pb.at[0, 0:2], "t", "in", src)

        for phase in (0, 1):
            h = near if phase == 0 else 1 - near
            for zz in range(NZ):
                pl.when(z == zz)(lambda zz=zz: wait_blocks(zz, phase == 0))
            acc = jnp.zeros((2 * HALF * 16, 256), F32)
            for kc in (0, 1):
                rows = pb[:, pl.ds(h * HALF, HALF), kc].reshape(2 * HALF * 16, KC)
                acc += jnp.dot(rows, w_t[kc], preferred_element_type=F32)
            for lp in (0, 1):
                for lw in (0, 1):
                    piece = acc[lp * 96 : lp * 96 + 96, lw * 128 : lw * 128 + 128]
                    part[phase, lp, lw] = piece.astype(BF16).reshape(HALF, 16, 128)
            for lp in (0, 1):
                for lw in (0, 1):
                    to = 4 * lp + 2 * h + lw

                    @pl.when(to != y)
                    def _():
                        send(part.at[phase, lp, lw], y_in.at[y], ("t", "y"), dev(x, 1, to, z), "y")

                    @pl.when(to == y)
                    def _():
                        y_in[y] = part[phase, lp, lw]

        arrived(y_in.at[0:7], "t", "y")
        total = y_in[0].astype(F32)
        for i in range(1, NY):
            total += y_in[i].astype(F32)
        outb[:, x] = total.astype(BF16)
        mine = outb.at[:, x]
        for d in (2, 1, 3):
            for cc in (1, 0):
                send(mine, mine, ("t", "out"), dev(xat(d), cc, y, z), "out")
        send(mine, mine, ("t", "out"), dev(x, 0, y, z), "out")

    @pl.when(core == 1)
    def _():
        arrived(sum_s, "p", "sum")
        for i, (kind, kc) in enumerate(ORDER):
            at = columns(kind, kc)
            avg = sum_s[i]
            m = NEST * mom[:, at] + avg
            n_mom[:, at] = m
            n_prm[:, at] = prm[:, at] - RATE * (avg + NEST * m)
        sent(out_s, "push")
        sent(q_s, "q")
        for zz in range(NZ):
            pl.when(z == zz)(lambda zz=zz: probe_sent(zz))

    @pl.when(core == 0)
    def _():
        sent(pb.at[0], "rs")
        sent(pb.at[:, 0:10], "ag")
        sent(sum_s, "sum")

    @pl.when(core == 1)
    def _():
        sent(y_in.at[0:7], "y")
        sent(y_in.at[0:7], "out")
        arrived(y_in.at[0:3], "t", "out")

    @pl.when(core == 0)
    def _():
        arrived(y_in.at[0:4], "t", "out")

    assert max(len(keys[g].at) for g in "wp") <= SHARED and len(keys["t"].at) <= N_RECV - SHARED
    assert len(sk.at) <= N_SEND and len(lk.at) <= N_LOCAL


def store(a, b, c, a_out, b_out, c_out, sem):
    copies = [
        pltpu.make_async_copy(src, dst, sem.at[i])
        for i, (src, dst) in enumerate(((a, a_out), (b, b_out), (c, c_out)))
    ]
    for cp in copies:
        cp.start()
    for cp in copies:
        cp.wait()


def per_device(pseudo_grad, compensation, params, momentum, probe):
    any_space = pl.BlockSpec(memory_space=pl.ANY)
    vmem = pl.BlockSpec(memory_space=pltpu.VMEM)
    shapes = (
        jax.ShapeDtypeStruct((16, K), F32),
        jax.ShapeDtypeStruct((16, K), F32),
        jax.ShapeDtypeStruct((6, NX, 16, 128), BF16),
    )
    outs = pl.pallas_call(
        kernel,
        out_shape=tuple(pltpu.VMEM(s.shape, s.dtype) for s in shapes),
        in_specs=[any_space] * 5,
        out_specs=[vmem] * 3,
        scratch_shapes=[
            pltpu.VMEM((4, 8, 16, KC), BF16),
            pltpu.VMEM((4, 8, 16, KC), F32),
            pltpu.VMEM((4, 8, 16, KC), BF16),
            pltpu.VMEM((4, 8, 16, KC), BF16),
            pltpu.VMEM((4, 2, 16, KC), BF16),
            pltpu.VMEM((4, 2, 2, 16, KC), BF16),
            pltpu.VMEM((4, 2, 16, KC), BF16),
            pltpu.VMEM((16, K), F32),
            pltpu.VMEM((16, K), F32),
            pltpu.VMEM((16, K), F32),
            pltpu.VMEM((4, 16, KC), F32),
            pltpu.VMEM((2, 2, NX, 2, 16, KC), BF16),
            pltpu.VMEM((2, KC, 256), BF16),
            pltpu.VMEM((4, 2, 16, KC), BF16),
            pltpu.VMEM((2, 2, 2, 16, KC), BF16),
            pltpu.VMEM((2, NZ, 2, 16, KC), BF16),
            pltpu.VMEM((2, 16, KC), BF16),
            pltpu.VMEM((2, 2, 2, HALF, 16, 128), BF16),
            pltpu.VMEM((NY, HALF, 16, 128), BF16),
            pltpu.SemaphoreType.DMA((N_SEND,)),
            pltpu.SemaphoreType.DMA((N_RECV,)),
            pltpu.SemaphoreType.DMA((N_LOCAL,)),
            pltpu.SemaphoreType.REGULAR,
            pltpu.SemaphoreType.REGULAR,
            pltpu.SemaphoreType.REGULAR((NY // 2,)),
        ],
        compiler_params=pltpu.CompilerParams(
            collective_id=0, has_side_effects=True, vmem_limit_bytes=60 * 2**20
        ),
    )(
        pseudo_grad.reshape(8, 16, K),
        compensation.reshape(8, 16, K),
        params,
        momentum,
        probe.reshape(NX, 16, K),
    )
    new_params, new_momentum, out = pl.pallas_call(
        store,
        out_shape=shapes,
        in_specs=[any_space] * 3,
        out_specs=[any_space] * 3,
        scratch_shapes=[pltpu.SemaphoreType.DMA((3,))],
        compiler_params=pltpu.CompilerParams(vmem_limit_bytes=2**20),
    )(*outs)
    return new_params, new_momentum, out.reshape(384, 128)


def solution(mesh):
    in_specs = (
        P("replica", "fsdp", "tensor"),
        P("replica", "fsdp", "tensor"),
        P(("fsdp", "replica"), "tensor"),
        P(("fsdp", "replica"), "tensor"),
        P("fsdp", "tensor"),
    )
    out_specs = (
        P(("fsdp", "replica"), "tensor"),
        P(("fsdp", "replica"), "tensor"),
        P("tensor", "fsdp"),
    )
    return jax.shard_map(
        per_device, mesh=mesh, in_specs=in_specs, out_specs=out_specs, check_vma=False
    )
```

```python
import functools

import jax
import jax.numpy as jnp
from jax import lax
from jax.experimental import pallas as pl
from jax.experimental.pallas import tpu as pltpu
from jax.sharding import PartitionSpec as P

MESH = pl.DeviceIdType.MESH
RATE = 0.7
NEST = 0.9
F32, BF16 = jnp.float32, jnp.bfloat16

NX, NY, NZ = 4, 8, 12
K = 4608
KC = K // 4
HALF = NZ // 2
EARLY = 6
ORDER = (("P", 0), ("P", 1), ("O", 0), ("O", 1))
TREE = {
    0: {0: (1, 11,), 1: (2,), 2: (3,), 3: (4,), 4: (5,), 5: (6,), 8: (9, 7,), 9: (10,), 11: (8,)},
    1: {0: (11,), 1: (2, 0,), 2: (3,), 3: (4,), 4: (5,), 5: (6,), 7: (8,), 9: (10, 7,), 11: (9,)},
    2: {0: (11,), 2: (3, 0, 1,), 3: (4,), 4: (5,), 5: (6,), 6: (7,), 9: (8,), 10: (9,), 11: (10,)},
    3: {0: (11,), 3: (0, 2, 4, 1,), 4: (5,), 5: (6,), 6: (7,), 7: (8,), 10: (9,), 11: (10,)},
    4: {0: (1, 11,), 2: (0, 3,), 4: (5, 2,), 5: (6,), 6: (7,), 7: (8,), 8: (9,), 11: (10,)},
    5: {2: (1,), 3: (0, 2,), 5: (3, 4, 6,), 6: (7,), 7: (10, 8,), 8: (9,), 10: (11,)},
    6: {0: (11,), 1: (2, 0,), 2: (3,), 4: (1, 5,), 6: (4, 7,), 7: (8,), 8: (9,), 9: (10,)},
    7: {4: (5, 2, 3,), 7: (4, 6, 10,), 9: (8,), 10: (9, 11, 0, 1,)},
    8: {0: (1, 11,), 3: (2,), 5: (6, 3, 4,), 6: (7,), 8: (9, 5,), 9: (0,), 11: (10,)},
    9: {0: (1,), 3: (2, 4,), 6: (3, 5, 7,), 7: (8,), 9: (11, 6,), 11: (0, 10,)},
    10: {0: (11,), 1: (0, 2,), 2: (3,), 3: (4,), 6: (5,), 7: (6,), 8: (7,), 10: (1, 9, 8,)},
    11: {1: (0, 2,), 2: (3,), 5: (4,), 7: (6,), 8: (7, 5,), 10: (9,), 11: (8, 1, 10,)},
}
WAITS = (
    (1, 3, 10, 6, 8, 4, 5, -1, 7, 12, 18, 9, 11, 14, 15, 16, 13, 17, 19, 32, 36, 34, 35, 38, 33, 40, 41, 43, 37, 42, 39, 25, 24, 27, 26),
    (5, 7, 0, 3, 2, 1, 46, 40, 41, 43, 47, 44, 45, 42, 26, 25, 24, 27),
    (9, 5, 6, 4, 0, 11, 7, 16, 3, 1, 18, 2, 17, 19, 40, 46, 41, 43, 47, 45, 22, 20, 42, 26, 21, 44, 25, 23, 24, 27),
    (9, 13, 5, 8, 11, 15, 10, 20, 6, 4, 7, 0, 21, 22, 3, 2, 1, 23, 32, 36, 34, 40, 37, 43, 35, 38, 41, 33, 42, 39),
    (14, 17, 12, 19, 13, 9, 5, 24, 26, 11, 8, 15, 10, 25, 27, 28, 7, 4, 3, 30, 0, 1, 2, 6, 31, 29),
    (-1, 21, 23, 19, 16, 14, 18, 34, 12, 32, 17, 9, 13, 10, 35, 33, 15, 11, 8, 4, 7, 0, 3, 5, 1, 2, 6, 44, 47, 46, 45),
    (25, 27, 20, 21, 23, 36, 22, 19, 16, 34, 37, 14, 18, 17, 38, 12, 35, 32, 10, 39, 15, 13, 11, 40, 8, 9, 33, 42, 41, 43),
    (24, 27, 25, 31, 26, 29, 21, 42, 20, 40, 19, 23, 22, 36, 16, 44, 41, 18, 43, 17, 37, 46, 45, 14, 47, 38, 12, 15, 39, 13, 5, 7, 4, 6),
    (35, 33, 40, 42, 44, 25, 41, 47, 27, 24, 43, 26, 46, 45, 2, 0, 20, 3, 1, 21, 23, 22, 19, 18, 17, 16),
    (37, 32, 34, 39, 35, 33, 25, 30, 27, 28, 5, 24, 7, 4, 31, 26, 2, 6, 0, 29, 3, 1, 8, 10, 9, 11),
    (41, 43, 30, 28, 46, 31, 47, 29, 44, 8, 12, 10, 23, 45, 15, 21, 20, 9, 11, 22, 14, 13),
    (45, 47, 36, 38, 2, 3, 1, 6, 0, 10, 37, 4, 5, 7, 8, 12, 39, 15, 9, 13, 11, 14, 32, 17, 16, 19, 33, 35, 34, 18),
)
LINKS = {0: NZ - 1, EARLY - 1: EARLY}
FAR_FIRST, SPLIT = (), {}
SHARED = 49
N_RECV, N_SEND, N_LOCAL = SHARED + 6, 10, 6


class Keys:
    def __init__(self):
        self.at = {}

    def __call__(self, *key):
        return self.at.setdefault(key, len(self.at))


def kernel(
    pg_hbm, comp_hbm, prm_hbm, mom_hbm, probe_hbm,
    n_prm, n_mom, outb,
    v_pg, v_comp, out_s, cs, r_opp, r_fin, t_acc, prm, mom, q_s, sum_s,
    w, w_t, wn, r_ag, pb, b_send, part, y_in,
    send_sem, recv_sem, loc_sem, go, go_late, both, token,
):
    rep = lax.axis_index("replica")
    fs = lax.axis_index("fsdp")
    t = lax.axis_index("tensor")
    x, core = rep // 2, rep % 2
    lo, z = fs // NZ, fs % NZ
    other = 1 - lo
    y = t * 2 + lo
    mate = t * 2 + other

    def dev(x_, core_, y_, z_):
        return (x_ * 2 + core_, (y_ % 2) * NZ + z_, y_ // 2)

    def xat(d):
        return lax.rem(x + d + NX, NX)

    def yat(d):
        return lax.rem(y + d + NY, NY)

    def zat(d):
        return lax.rem(z + d + NZ, NZ)

    w_dev, h_dev, me = dev(x, 0, y, z), dev(x, 1, y, z), dev(x, core, y, z)

    keys, sk, lk = {group: Keys() for group in "wpt"}, Keys(), Keys()

    def rsem(group, *key):
        at = keys[group](*key)
        return recv_sem.at[SHARED + at if group == "t" else at]

    def ssem(group):
        return send_sem.at[sk(group)]

    def send(src, dst, key, to, group):
        pltpu.make_async_remote_copy(
            src_ref=src, dst_ref=dst, send_sem=ssem(group), recv_sem=rsem(*key),
            device_id=to, device_id_type=MESH,
        ).start()

    def arrived(like, *key):
        pltpu.make_async_remote_copy(
            src_ref=like, dst_ref=like, send_sem=send_sem.at[0], recv_sem=rsem(*key),
            device_id=me, device_id_type=MESH,
        ).wait_recv()

    def sent(like, group):
        pltpu.make_async_remote_copy(
            src_ref=like, dst_ref=like, send_sem=ssem(group), recv_sem=recv_sem.at[0],
            device_id=me, device_id_type=MESH,
        ).wait_send()

    def load(src, dst, key):
        pltpu.make_async_copy(src, dst, loc_sem.at[lk(key)]).start()

    def loaded(like, key):
        pltpu.make_async_remote_copy(
            src_ref=like, dst_ref=like, send_sem=send_sem.at[0], recv_sem=loc_sem.at[lk(key)],
            device_id=me, device_id_type=MESH,
        ).wait_recv()

    def columns(kind, kc):
        half = lo if kind == "O" else other
        return pl.ds(pl.multiple_of((half * 2 + kc) * KC, KC), KC)

    def load_chunk(i):
        at = columns(*ORDER[i])
        load(pg_hbm.at[:, :, at], v_pg.at[i], ("in", i))
        load(comp_hbm.at[:, :, at], v_comp.at[i], ("in", i))

    barrier = pltpu.get_barrier_semaphore()

    def greet(to):
        pl.semaphore_signal(barrier, inc=1, device_id=to, device_id_type=MESH)

    def p_dev(y_, zz):
        return dev(x, 1, y_, zz)

    def senders(zz):
        found = {(1, zz): mate, (2, zz): jnp.where(lo == 1, yat(1), yat(-1))}
        for src in TREE:
            for q, to in TREE[src].items():
                if zz in to:
                    found[0, q] = y
        if zz in LINKS:
            found[0, LINKS[zz]] = y
        return [(found[key], key[1]) for key in sorted(found)]

    late = z >= EARLY
    apart = jnp.logical_and(z == 0, jnp.logical_and(x == 0, y == 0))

    @pl.when(core == 1)
    def _():
        @pl.when(jnp.logical_not(late))
        def _():
            load_chunk(0)

        greet(w_dev)
        for zz in range(NZ):

            @pl.when(z == zz)
            def _():
                for yy, q in senders(zz):
                    if not (q < EARLY <= zz):
                        greet(p_dev(yy, q))

        for kc in (0, 1):
            load(probe_hbm.at[x, :, columns("O", kc)], pb.at[lo, z, kc], "own")
            load(probe_hbm.at[x, :, columns("P", kc)], b_send.at[kc], "own")

        @pl.when(late)
        def _():
            load_chunk(0)

    @pl.when(core == 0)
    def _():
        load_chunk(0)
        for d in (1, -1):
            greet(dev(xat(d), 0, y, z))
            greet(dev(xat(d), 0, mate, z))
        greet(dev(x, 0, mate, z))

        @pl.when(jnp.logical_not(apart))
        def _():
            greet(h_dev)

    for i in (1, 2, 3):
        load_chunk(i)
    load(prm_hbm, prm, "state")
    load(mom_hbm, mom, "state")

    @pl.when(core == 0)
    def _():
        right, left, far = xat(1), xat(-1), xat(2)
        rdev, ldev = dev(right, 0, y, z), dev(left, 0, y, z)
        pl.semaphore_wait(barrier, 6)

        @pl.when(apart)
        def _():
            pl.semaphore_signal(go, inc=1, device_id=h_dev, device_id_type=MESH)

        pl.semaphore_signal(both, inc=1, device_id=dev(x, 0, mate, z), device_id_type=MESH)

        def chip_sum(i, s):
            return v_pg[i, s].astype(F32) + v_comp[i, s] + out_s[i, s].astype(F32)

        def opposite(i):
            loaded(pb.at[0], ("in", i))
            arrived(out_s.at[i], "w", "push", i)
            for side, to in ((1, rdev), (0, ldev)):
                s = far * 2 + side
                cs[i, s] = chip_sum(i, s).astype(BF16)
                send(cs.at[i, s], r_opp.at[i, side], ("w", "opp", i, side), to, "rs")

        def direct(i):
            for side, to, xx in ((0, rdev, right), (1, ldev, left)):
                s = xx * 2 + side
                cs[i, s] = chip_sum(i, s).astype(BF16)
                send(cs.at[i, s], r_fin.at[i, side, 0], ("w", "fin", i), to, "rs")

        def on_the_way(i):
            for side, to, xx in ((1, rdev, right), (0, ldev, left)):
                s = xx * 2 + side
                arrived(r_opp.at[i, side], "w", "opp", i, side)
                t_acc[i, side] = (chip_sum(i, s) + r_opp[i, side].astype(F32)).astype(BF16)
                send(t_acc.at[i, side], r_fin.at[i, side, 1], ("w", "fin", i), to, "rs")

        opposite(0)
        opposite(1)
        direct(0)
        direct(1)
        opposite(2)
        opposite(3)
        pl.semaphore_wait(both, 1)
        on_the_way(0)
        on_the_way(1)
        direct(2)
        direct(3)
        on_the_way(2)
        on_the_way(3)

        loaded(v_comp.at[0], "state")
        arrived(q_s, "w", "q")

        def gather(src, kc, kind, first):
            y_, rel = (y, 0) if kind == "O" else (mate, 1)
            for side, xx in ((1, right), (0, left)):
                if first:
                    send(src.at[side], r_ag.at[kc, rel, side], ("w", "ag", kc, rel, side), dev(xx, 0, y_, z), "ag")
            if not first:
                for side, xx in ((0, right), (1, left), (0, x), (1, x)):
                    send(src.at[side], w.at[kc, lo, x, side], ("t", "w", kc), dev(xx, 1, y_, z), "ag")

        def relay(kc, rel):
            f = other if rel else lo
            for side, to, xx in ((1, right, left), (0, left, right)):
                ref = r_ag.at[kc, rel, side]
                arrived(ref, "w", "ag", kc, rel, side)
                for x_ in (to, x):
                    send(ref, w.at[kc, f, xx, side], ("t", "w", kc), dev(x_, 1, y, z), "ag")

        def block(i):
            kind, kc = ORDER[i]
            return wn.at[i], kc, kind

        for i, (kind, kc) in enumerate(ORDER):
            at = columns(kind, kc)
            arrived(r_fin.at[i], "w", "fin", i)

            def average(side):
                return (
                    chip_sum(i, x * 2 + side)
                    + r_fin[i, side, 0].astype(F32)
                    + r_fin[i, side, 1].astype(F32)
                ) * 0.125

            avg = average(0)
            m = NEST * mom[:, at] + avg
            new = prm[:, at] - RATE * (avg + NEST * m)
            n_mom[:, at] = m
            n_prm[:, at] = new
            wn[i, 0] = new.astype(BF16)
            avg = average(1)
            sum_s[i] = avg
            wn[i, 1] = (q_s[:, at] - (RATE * (1 + NEST)) * avg).astype(BF16)
            gather(*block(i), True)
            if i == 1:
                gather(*block(0), False)
        for i in (2, 1, 3):
            gather(*block(i), False)
        for i in range(4):
            send(sum_s.at[i], sum_s.at[i], ("p", "sum"), h_dev, "sum")

        relay(0, 1)
        relay(1, 1)
        relay(0, 0)
        relay(1, 0)

    lane = {"A": lo, "B": other}

    def receivers(zz):
        found = {(zz, 1), (zz, 2)}
        for src in TREE:
            for to in TREE[src].get(zz, ()):
                if not (zz < EARLY <= to):
                    found.add((to, 0))
        for early_plane, late_plane in LINKS.items():
            if late_plane == zz:
                found.add((early_plane, 0))
        return len(found)

    def hop(typ, src, kc, zz, to):
        ref = pb.at[lane[typ], src, kc]
        target = dev(x, 1, y, to)
        key = ("p", "z", typ, src, kc) if TREE[src].get(to) else ("t", "in", src // HALF == to // HALF)
        send(ref, ref, key, target, "twin" if src == zz else "relay")

    def start(kc, zz, to):
        ref = pb.at[lo, zz, kc]
        key = ("p", "z", "A", zz, kc) if TREE[zz].get(to) else ("t", "in", zz // HALF == to // HALF)
        send(ref, ref, key, dev(x, 1, y, to), "own")

    def item(code):
        return "AB"[code % 2], code // 4, code // 2 % 2

    def pass_token(step):
        if step:
            pl.semaphore_wait(token.at[step - 1], 2)
        if step < 3:
            for d in (1, -1):
                to = dev(x, 1, yat(d), z)
                pl.semaphore_signal(token.at[step], inc=1, device_id=to, device_id_type=MESH)

    def begin(zz):
        loaded(pb.at[0, 0:2], "own")
        pl.semaphore_wait(barrier, receivers(zz) + (jnp.where(apart, 0, 1) if zz == 0 else 1))
        for early_plane, late_plane in LINKS.items():
            if late_plane == zz:
                to = p_dev(y, early_plane)
                pl.semaphore_signal(go_late, inc=1, device_id=to, device_id_type=MESH)
        for kc in (0, 1):
            send(b_send.at[kc], pb.at[lo, zz, kc], ("p", "z", "B", zz, kc), dev(x, 1, mate, zz), "own")
            for to in TREE[zz][zz]:
                if not (zz < EARLY <= to):
                    start(kc, zz, to)

    def pass_on(zz):
        steps, held, count = [], [], len(WAITS[zz])

        def late_planes():
            pl.semaphore_wait(go_late, 1)
            for kc in (0, 1):
                for to in TREE[zz][zz]:
                    if zz < EARLY <= to:
                        start(kc, zz, to)

        def one(typ, src, kc, targets):
            arrived(pb.at[lane[typ], src, kc], "p", "z", typ, src, kc)
            for to in targets:
                hop(typ, src, kc, zz, to)

        for n, code in enumerate(WAITS[zz]):
            if n in (count // 3, 2 * count // 3):
                steps.append(functools.partial(pass_token, 1 if n == count // 3 else 2))
            if code < 0:
                steps.append(late_planes)
                steps += [functools.partial(hop, *what) for what in held]
                held = None
                continue
            typ, src, kc = item(code)
            wait = [to for to in TREE[src][zz] if zz < EARLY <= to and held is not None]
            if wait:
                held += [(typ, src, kc, zz, to) for to in wait]
            steps.append(functools.partial(one, typ, src, kc, [to for to in TREE[src][zz] if to not in wait]))
        return steps

    def run(steps):
        for step in steps:
            step()

    def probe_sent(zz):
        sent(pb.at[0, 0 : len(TREE[zz][zz]) + 1], "own")
        sent(pb.at[0, 0 : len(TREE[zz][zz])], "twin")
        passed = [src for src in TREE if src != zz and TREE[src].get(zz)]
        count = sum(len(TREE[src][zz]) for src in passed)
        assert count <= NZ
        sent(pb.at[:, 0:count], "relay")

    @pl.when(core == 1)
    def _():
        def prepare(i):
            loaded(pb.at[0], ("in", i))
            out_s[i] = (v_pg[i].astype(F32) + v_comp[i]).astype(BF16)

        def push(i):
            send(out_s.at[i], out_s.at[i], ("w", "push", i), w_dev, "push")

        prepare(0)

        @pl.when(jnp.logical_not(late))
        def _():
            prepare(1)
            prepare(2)
            prepare(3)

        for zz in range(NZ):
            pl.when(z == zz)(lambda zz=zz: begin(zz))
        pass_token(0)

        @pl.when(apart)
        def _():
            pl.semaphore_wait(go, 1)

        @pl.when(jnp.logical_not(late))
        def _():
            for i in range(4):
                push(i)

        @pl.when(late)
        def _():
            push(0)
            for i in (1, 2, 3):
                prepare(i)
                push(i)

        loaded(v_comp.at[0], "state")
        q_s[...] = prm[...] - (RATE * NEST * NEST) * mom[...]
        send(q_s, q_s, ("w", "q"), w_dev, "q")
        for zz in range(NZ):
            steps = pass_on(zz)
            pl.when(z == zz)(functools.partial(run, steps[: SPLIT.get(zz, len(steps))]))

        near = z // HALF
        far_first = functools.reduce(jnp.logical_or, [z == zz for zz in FAR_FIRST], z < 0)

        def weights():
            for kc in (0, 1):
                arrived(w.at[kc], "t", "w", kc)
                w_t[kc] = w[kc].reshape(256, KC).T

        def wait_blocks(zz, phase):
            want_near = (phase == 0) != (zz in FAR_FIRST)
            stop = [
                src for src in TREE
                if src != zz and (src // HALF == zz // HALF) == want_near and not TREE[src].get(zz)
            ]
            if stop:
                arrived(pb.at[:, 0 : len(stop)], "t", "in", want_near)

        def multiply(phase):
            h = jnp.where(far_first, 1 - near, near)
            if phase:
                h = 1 - h
            for zz in range(NZ):
                pl.when(z == zz)(functools.partial(wait_blocks, zz, phase))
            acc = jnp.zeros((2 * HALF * 16, 256), F32)
            for kc in (0, 1):
                rows = pb[:, pl.ds(h * HALF, HALF), kc].reshape(2 * HALF * 16, KC)
                acc += jnp.dot(rows, w_t[kc], preferred_element_type=F32)
            for lp in (0, 1):
                for lw in (0, 1):
                    piece = acc[lp * 96 : lp * 96 + 96, lw * 128 : lw * 128 + 128]
                    part[phase, lp, lw] = piece.astype(BF16).reshape(HALF, 16, 128)
            for d in (4, 3, 5, 2, 6, 1, 7):
                to = yat(d)

                @pl.when(to // 2 % 2 == h)
                def _():
                    send(part.at[phase, to // 4, to % 2], y_in.at[y], ("t", "y"), dev(x, 1, to, z), "y")

            @pl.when(y // 2 % 2 == h)
            def _():
                y_in[y] = part[phase, y // 4, y % 2]

        soon = jnp.logical_and(functools.reduce(jnp.logical_or, [z == zz for zz in SPLIT], z < 0), y >= 2)

        def first_half():
            pass_token(3)
            weights()
            multiply(0)

        if SPLIT:
            pl.when(soon)(first_half)
            for zz in SPLIT:
                pl.when(z == zz)(functools.partial(run, pass_on(zz)[SPLIT[zz] :]))
        pl.when(jnp.logical_not(soon))(first_half)
        multiply(1)

        arrived(y_in.at[0:7], "t", "y")
        total = y_in[0].astype(F32)
        for i in range(1, NY):
            total += y_in[i].astype(F32)
        outb[:, x] = total.astype(BF16)
        mine = outb.at[:, x]
        for d in (2, 1, 3):
            for cc in (1, 0):
                send(mine, mine, ("t", "out"), dev(xat(d), cc, y, z), "out")
        send(mine, mine, ("t", "out"), dev(x, 0, y, z), "out")

    @pl.when(core == 1)
    def _():
        arrived(sum_s, "p", "sum")
        for i, (kind, kc) in enumerate(ORDER):
            at = columns(kind, kc)
            avg = sum_s[i]
            m = NEST * mom[:, at] + avg
            n_mom[:, at] = m
            n_prm[:, at] = prm[:, at] - RATE * (avg + NEST * m)
        sent(out_s, "push")
        sent(q_s, "q")
        for zz in range(NZ):
            pl.when(z == zz)(lambda zz=zz: probe_sent(zz))

    @pl.when(core == 0)
    def _():
        sent(pb.at[0], "rs")
        sent(pb.at[:, 0:10], "ag")
        sent(sum_s, "sum")

    @pl.when(core == 1)
    def _():
        sent(y_in.at[0:7], "y")
        sent(y_in.at[0:7], "out")
        arrived(y_in.at[0:3], "t", "out")

    @pl.when(core == 0)
    def _():
        arrived(y_in.at[0:4], "t", "out")

    assert max(len(keys[g].at) for g in "wp") <= SHARED and len(keys["t"].at) <= N_RECV - SHARED
    assert len(sk.at) <= N_SEND and len(lk.at) <= N_LOCAL


def store(a, b, c, a_out, b_out, c_out, sem):
    copies = [
        pltpu.make_async_copy(src, dst, sem.at[i])
        for i, (src, dst) in enumerate(((a, a_out), (b, b_out), (c, c_out)))
    ]
    for cp in copies:
        cp.start()
    for cp in copies:
        cp.wait()


def per_device(pseudo_grad, compensation, params, momentum, probe):
    any_space = pl.BlockSpec(memory_space=pl.ANY)
    vmem = pl.BlockSpec(memory_space=pltpu.VMEM)
    shapes = (
        jax.ShapeDtypeStruct((16, K), F32),
        jax.ShapeDtypeStruct((16, K), F32),
        jax.ShapeDtypeStruct((6, NX, 16, 128), BF16),
    )
    outs = pl.pallas_call(
        kernel,
        out_shape=tuple(pltpu.VMEM(s.shape, s.dtype) for s in shapes),
        in_specs=[any_space] * 5,
        out_specs=[vmem] * 3,
        scratch_shapes=[
            pltpu.VMEM((4, 8, 16, KC), BF16),
            pltpu.VMEM((4, 8, 16, KC), F32),
            pltpu.VMEM((4, 8, 16, KC), BF16),
            pltpu.VMEM((4, 8, 16, KC), BF16),
            pltpu.VMEM((4, 2, 16, KC), BF16),
            pltpu.VMEM((4, 2, 2, 16, KC), BF16),
            pltpu.VMEM((4, 2, 16, KC), BF16),
            pltpu.VMEM((16, K), F32),
            pltpu.VMEM((16, K), F32),
            pltpu.VMEM((16, K), F32),
            pltpu.VMEM((4, 16, KC), F32),
            pltpu.VMEM((2, 2, NX, 2, 16, KC), BF16),
            pltpu.VMEM((2, KC, 256), BF16),
            pltpu.VMEM((4, 2, 16, KC), BF16),
            pltpu.VMEM((2, 2, 2, 16, KC), BF16),
            pltpu.VMEM((2, NZ, 2, 16, KC), BF16),
            pltpu.VMEM((2, 16, KC), BF16),
            pltpu.VMEM((2, 2, 2, HALF, 16, 128), BF16),
            pltpu.VMEM((NY, HALF, 16, 128), BF16),
            pltpu.SemaphoreType.DMA((N_SEND,)),
            pltpu.SemaphoreType.DMA((N_RECV,)),
            pltpu.SemaphoreType.DMA((N_LOCAL,)),
            pltpu.SemaphoreType.REGULAR,
            pltpu.SemaphoreType.REGULAR,
            pltpu.SemaphoreType.REGULAR,
            pltpu.SemaphoreType.REGULAR((3,)),
        ],
        compiler_params=pltpu.CompilerParams(
            collective_id=0, has_side_effects=True, vmem_limit_bytes=60 * 2**20
        ),
    )(
        pseudo_grad.reshape(8, 16, K),
        compensation.reshape(8, 16, K),
        params,
        momentum,
        probe.reshape(NX, 16, K),
    )
    new_params, new_momentum, out = pl.pallas_call(
        store,
        out_shape=shapes,
        in_specs=[any_space] * 3,
        out_specs=[any_space] * 3,
        scratch_shapes=[pltpu.SemaphoreType.DMA((3,))],
        compiler_params=pltpu.CompilerParams(vmem_limit_bytes=2**20),
    )(*outs)
    return new_params, new_momentum, out.reshape(384, 128)


def solution(mesh):
    in_specs = (
        P("replica", "fsdp", "tensor"),
        P("replica", "fsdp", "tensor"),
        P(("fsdp", "replica"), "tensor"),
        P(("fsdp", "replica"), "tensor"),
        P("fsdp", "tensor"),
    )
    out_specs = (
        P(("fsdp", "replica"), "tensor"),
        P(("fsdp", "replica"), "tensor"),
        P("tensor", "fsdp"),
    )
    return jax.shard_map(
        per_device, mesh=mesh, in_specs=in_specs, out_specs=out_specs, check_vma=False
    )
```

```python
import functools

import jax
import jax.numpy as jnp
from jax import lax
from jax.experimental import pallas as pl
from jax.experimental.pallas import tpu as pltpu
from jax.sharding import PartitionSpec as P

MESH = pl.DeviceIdType.MESH
RATE = 0.7
NEST = 0.9
F32, BF16 = jnp.float32, jnp.bfloat16

NX, NY, NZ = 4, 8, 12
K = 4608
KC = K // 4
HALF = NZ // 2
EARLY = 6
ORDER = (("P", 0), ("P", 1), ("O", 0), ("O", 1))
TREE = {
    0: {0: (1, 11,), 1: (2,), 2: (3,), 3: (4,), 4: (5,), 7: (6,), 9: (7, 8, 10,), 11: (9,)},
    1: {0: (11,), 1: (2, 0,), 2: (3,), 3: (4,), 4: (5,), 5: (6,), 6: (7,), 9: (8,), 10: (9,), 11: (10,)},
    2: {0: (11,), 2: (0, 1, 3,), 3: (4,), 4: (5,), 5: (6,), 6: (7,), 9: (8,), 10: (9,), 11: (10,)},
    3: {0: (11,), 1: (0,), 3: (1, 2, 4,), 4: (5,), 5: (6,), 6: (7,), 7: (8,), 10: (9,), 11: (10,)},
    4: {0: (11, 1,), 2: (0,), 4: (2, 3, 5,), 5: (6,), 6: (7,), 7: (9, 8,), 11: (10,)},
    5: {0: (11,), 1: (0, 2,), 3: (1, 4,), 5: (3, 6,), 6: (7,), 7: (8,), 8: (9,), 11: (10,)},
    6: {1: (0,), 3: (1, 2,), 4: (3, 5,), 6: (7, 4,), 7: (8, 9,), 9: (10,), 10: (11,)},
    7: {3: (4, 2, 1,), 5: (3, 6,), 7: (5, 9,), 8: (10,), 9: (8, 11,), 11: (0,)},
    8: {0: (1, 11,), 3: (2,), 4: (3, 5,), 6: (4,), 8: (6, 10,), 9: (7,), 10: (0, 9,)},
    9: {1: (2, 0,), 2: (3,), 4: (5,), 6: (4,), 8: (6, 7,), 9: (8, 11,), 11: (1, 10,)},
    10: {0: (1,), 1: (2,), 2: (3,), 5: (4, 6,), 7: (5,), 8: (7, 9,), 9: (11,), 10: (0, 8,)},
    11: {1: (0, 2,), 2: (3,), 5: (4,), 6: (5, 7,), 8: (9, 6,), 10: (8,), 11: (10, 1,)},
}
WAITS = (
    (-1, 1, 4, 3, 14, 10, 7, 9, 5, 40, 6, 8, 11, 12, 15, 42, 13, 43, 18, 41, 16, 22, 17, 21, 19, 32, 20, 34, 33, 23, 35),
    (5, 7, 2, 0, 14, 12, 15, 13, 44, 20, 1, 46, 45, 3, 22, 21, 47, 23, 42, 24, 26, 36, 38, 37, 39, 43, 25, 41, 40, 27),
    (4, 7, 5, 6, 2, 9, 0, 11, 16, 18, 17, 19, 44, 1, 3, 46, 45, 47, 36, 42, 38, 39, 37, 41, 40, 43),
    (13, 15, 8, 6, 20, 10, 22, 4, 5, 9, 7, 2, 21, 11, 23, 24, 0, 26, 28, 25, 27, 30, 29, 31, 1, 3, 34, 32, 35, 33),
    (19, 17, 13, 15, 24, 26, 12, 14, 25, 27, 8, 9, 10, 4, 11, 7, 5, 6, 32, 2, 34, 35, 33, 38, 0, 36, 1, 3, 39, 37),
    (-1, 21, 23, 17, 18, 28, 16, 13, 30, 19, 29, 15, 12, 14, 31, 9, 8, 10, 4, 11, 7, 42, 40, 6, 5, 43, 41, 46, 44, 45, 47),
    (25, 27, 34, 22, 21, 32, 35, 18, 17, 23, 33, 19, 16, 20, 14, 38, 12, 13, 36, 15, 37, 9, 39, 10, 8, 11, 46, 44, 45, 5, 4, 47, 6, 7),
    (29, 31, 27, 26, 24, 40, 42, 25, 21, 22, 43, 41, 23, 18, 17, 19, 20, 16, 13, 12, 15, 1, 14, 0, 2, 3),
    (35, 33, 40, 42, 36, 38, 43, 41, 37, 39, 46, 28, 44, 45, 21, 29, 47, 30, 22, 23, 20, 31),
    (37, 39, 29, 28, 31, 30, 1, 27, 0, 24, 42, 25, 43, 40, 2, 3, 26, 32, 41, 33, 34, 35, 9, 5, 8, 4, 11, 6, 10, 7),
    (43, 41, 46, 44, 45, 47, 32, 34, 33, 35, 9, 6, 5, 8, 4, 11, 10, 14, 7, 27, 12, 13, 15, 24, 25, 26),
    (45, 47, 0, 1, 2, 36, 38, 37, 39, 9, 4, 3, 6, 5, 8, 7, 29, 12, 11, 10, 31, 28, 14, 30, 13, 16, 15, 18, 19, 17, 20, 22, 21, 23),
)
LINKS = {0: NZ - 1, EARLY - 1: EARLY}
FAR = (1, 1, 1, 0, 0, 0, 1, 1, 1, 0, 0, 0)
SOON = 5
SHARED = max(len(order) for order in WAITS)
N_RECV, N_SEND, N_LOCAL = SHARED + 9, 7, 6


class Keys:
    def __init__(self):
        self.at = {}

    def __call__(self, *key):
        return self.at.setdefault(key, len(self.at))


def kernel(
    pg_hbm, comp_hbm, prm_hbm, mom_hbm, probe_hbm,
    n_prm, n_mom, outb,
    v_pg, v_comp, out_s, cs, r_opp, r_fin, t_acc, prm, mom, q_s, sum_s,
    w, w_t, wn, r_ag, pb, b_send, part, y_in,
    send_sem, recv_sem, loc_sem, go, go_late, both, token,
):
    rep = lax.axis_index("replica")
    fs = lax.axis_index("fsdp")
    t = lax.axis_index("tensor")
    x, core = rep // 2, rep % 2
    lo, z = fs // NZ, fs % NZ
    other = 1 - lo
    y = t * 2 + lo
    mate = t * 2 + other

    def dev(x_, core_, y_, z_):
        return (x_ * 2 + core_, (y_ % 2) * NZ + z_, y_ // 2)

    def xat(d):
        return lax.rem(x + d + NX, NX)

    def yat(d):
        return lax.rem(y + d + NY, NY)

    def zat(d):
        return lax.rem(z + d + NZ, NZ)

    w_dev, h_dev, me = dev(x, 0, y, z), dev(x, 1, y, z), dev(x, core, y, z)

    keys, sk, lk = {group: Keys() for group in "wt"}, {core_: Keys() for core_ in (0, 1)}, Keys()

    def rsem(group, *key):
        if group == "p":
            zz, typ, src, kc = key
            return recv_sem.at[WAITS[zz].index(src * 4 + kc * 2 + "AB".index(typ))]
        at = keys[group](*key)
        return recv_sem.at[SHARED + at if group == "t" else at]

    def ssem(group):
        return send_sem.at[sk[0 if group in ("rs", "ag", "sum") else 1](group)]

    def send(src, dst, key, to, group):
        pltpu.make_async_remote_copy(
            src_ref=src, dst_ref=dst, send_sem=ssem(group), recv_sem=rsem(*key),
            device_id=to, device_id_type=MESH,
        ).start()

    def arrived(like, *key):
        pltpu.make_async_remote_copy(
            src_ref=like, dst_ref=like, send_sem=send_sem.at[0], recv_sem=rsem(*key),
            device_id=me, device_id_type=MESH,
        ).wait_recv()

    def sent(like, group):
        pltpu.make_async_remote_copy(
            src_ref=like, dst_ref=like, send_sem=ssem(group), recv_sem=recv_sem.at[0],
            device_id=me, device_id_type=MESH,
        ).wait_send()

    def load(src, dst, key):
        pltpu.make_async_copy(src, dst, loc_sem.at[lk(key)]).start()

    def loaded(like, key):
        pltpu.make_async_remote_copy(
            src_ref=like, dst_ref=like, send_sem=send_sem.at[0], recv_sem=loc_sem.at[lk(key)],
            device_id=me, device_id_type=MESH,
        ).wait_recv()

    def columns(kind, kc):
        half = lo if kind == "O" else other
        return pl.ds(pl.multiple_of((half * 2 + kc) * KC, KC), KC)

    def load_chunk(i):
        at = columns(*ORDER[i])
        load(pg_hbm.at[:, :, at], v_pg.at[i], ("in", i))
        load(comp_hbm.at[:, :, at], v_comp.at[i], ("in", i))

    barrier = pltpu.get_barrier_semaphore()

    def greet(to):
        pl.semaphore_signal(barrier, inc=1, device_id=to, device_id_type=MESH)

    def p_dev(y_, zz):
        return dev(x, 1, y_, zz)

    def turn(src, zz):
        if src // HALF == zz // HALF:
            return 0
        return 1 if src % HALF // 3 == FAR[zz] else 2

    def senders(zz):
        found = {(1, zz): mate, (2, zz): jnp.where(lo == 1, yat(1), yat(-1))}
        for src in TREE:
            for q, to in TREE[src].items():
                if zz in to:
                    found[0, q] = y
        if zz in LINKS:
            found[0, LINKS[zz]] = y
        return [(found[key], key[1]) for key in sorted(found)]

    late = z >= EARLY
    apart = jnp.logical_and(z == 0, jnp.logical_and(x == 0, y == 0))

    @pl.when(core == 1)
    def _():
        @pl.when(jnp.logical_not(late))
        def _():
            load_chunk(0)

        greet(w_dev)
        for zz in range(NZ):

            @pl.when(z == zz)
            def _():
                for yy, q in senders(zz):
                    if not (q < EARLY <= zz):
                        greet(p_dev(yy, q))

        for kc in (0, 1):
            load(probe_hbm.at[x, :, columns("O", kc)], pb.at[lo, z, kc], "own")
            load(probe_hbm.at[x, :, columns("P", kc)], b_send.at[kc], "own")

        @pl.when(late)
        def _():
            load_chunk(0)

    @pl.when(core == 0)
    def _():
        load_chunk(0)
        for d in (-1, 1):
            greet(dev(xat(d), 0, y, z))
        for d in (-1, 1):
            greet(dev(xat(d), 0, mate, z))
        greet(dev(x, 0, mate, z))

        @pl.when(jnp.logical_not(apart))
        def _():
            greet(h_dev)

    for i in (1, 2, 3):
        load_chunk(i)
    load(prm_hbm, prm, "state")
    load(mom_hbm, mom, "state")

    @pl.when(core == 0)
    def _():
        right, left, far = xat(1), xat(-1), xat(2)
        rdev, ldev = dev(right, 0, y, z), dev(left, 0, y, z)
        pl.semaphore_wait(barrier, 6)

        @pl.when(apart)
        def _():
            pl.semaphore_signal(go, inc=1, device_id=h_dev, device_id_type=MESH)

        pl.semaphore_signal(both, inc=1, device_id=dev(x, 0, mate, z), device_id_type=MESH)

        def chip_sum(i, s):
            return v_pg[i, s].astype(F32) + v_comp[i, s] + out_s[i, s].astype(F32)

        def opposite(i):
            loaded(pb.at[0], ("in", i))
            arrived(out_s.at[i], "w", "push", i)
            for side, to in ((1, rdev), (0, ldev)):
                s = far * 2 + side
                cs[i, s] = chip_sum(i, s).astype(BF16)
                send(cs.at[i, s], r_opp.at[i, side], ("w", "opp", i, side), to, "rs")

        def direct(i):
            for side, to, xx in ((0, rdev, right), (1, ldev, left)):
                s = xx * 2 + side
                cs[i, s] = chip_sum(i, s).astype(BF16)
                send(cs.at[i, s], r_fin.at[i, side, 0], ("w", "fin", i), to, "rs")

        def on_the_way(i):
            for side, to, xx in ((1, rdev, right), (0, ldev, left)):
                s = xx * 2 + side
                arrived(r_opp.at[i, side], "w", "opp", i, side)
                t_acc[i, side] = (chip_sum(i, s) + r_opp[i, side].astype(F32)).astype(BF16)
                send(t_acc.at[i, side], r_fin.at[i, side, 1], ("w", "fin", i), to, "rs")

        opposite(0)
        opposite(1)
        direct(0)
        direct(1)
        opposite(2)
        opposite(3)
        pl.semaphore_wait(both, 1)
        on_the_way(0)
        on_the_way(1)
        direct(2)
        direct(3)
        on_the_way(2)
        on_the_way(3)

        loaded(v_comp.at[0], "state")
        arrived(q_s, "w", "q")

        def gather(src, kc, kind, first):
            y_, rel = (y, 0) if kind == "O" else (mate, 1)
            for side, xx in ((1, right), (0, left)):
                if first:
                    send(src.at[side], r_ag.at[kc, rel, side], ("w", "ag", kc, rel, side), dev(xx, 0, y_, z), "ag")
            if not first:
                for side, xx in ((0, right), (1, left), (0, x), (1, x)):
                    send(src.at[side], w.at[kc, lo, x, side], ("t", "w", kc), dev(xx, 1, y_, z), "ag")

        def relay(kc, rel):
            f = other if rel else lo
            for side, to, xx in ((1, right, left), (0, left, right)):
                ref = r_ag.at[kc, rel, side]
                arrived(ref, "w", "ag", kc, rel, side)
                for x_ in (to, x):
                    send(ref, w.at[kc, f, xx, side], ("t", "w", kc), dev(x_, 1, y, z), "ag")

        def block(i):
            kind, kc = ORDER[i]
            return wn.at[i], kc, kind

        for i, (kind, kc) in enumerate(ORDER):
            at = columns(kind, kc)
            arrived(r_fin.at[i], "w", "fin", i)

            def average(side):
                return (
                    chip_sum(i, x * 2 + side)
                    + r_fin[i, side, 0].astype(F32)
                    + r_fin[i, side, 1].astype(F32)
                ) * 0.125

            avg = average(0)
            m = NEST * mom[:, at] + avg
            new = prm[:, at] - RATE * (avg + NEST * m)
            n_mom[:, at] = m
            n_prm[:, at] = new
            wn[i, 0] = new.astype(BF16)
            avg = average(1)
            sum_s[i] = avg
            wn[i, 1] = (q_s[:, at] - (RATE * (1 + NEST)) * avg).astype(BF16)
            gather(*block(i), True)
            if i == 1:
                gather(*block(0), False)
        for i in (2, 1, 3):
            gather(*block(i), False)
        for i in range(4):
            send(sum_s.at[i], sum_s.at[i], ("t", "sum"), h_dev, "sum")

        relay(0, 1)
        relay(1, 1)
        relay(0, 0)
        relay(1, 0)

    lane = {"A": lo, "B": other}

    def receivers(zz):
        found = {(zz, 1), (zz, 2)}
        for src in TREE:
            for to in TREE[src].get(zz, ()):
                if not (zz < EARLY <= to):
                    found.add((to, 0))
        for early_plane, late_plane in LINKS.items():
            if late_plane == zz:
                found.add((early_plane, 0))
        return len(found)

    def hop(typ, src, kc, zz, to):
        ref = pb.at[lane[typ], src, kc]
        target = dev(x, 1, y, to)
        key = ("p", to, typ, src, kc) if TREE[src].get(to) else ("t", "in", turn(src, to))
        send(ref, ref, key, target, "twin" if src == zz else "relay")

    def start(kc, zz, to):
        ref = pb.at[lo, zz, kc]
        key = ("p", to, "A", zz, kc) if TREE[zz].get(to) else ("t", "in", turn(zz, to))
        send(ref, ref, key, dev(x, 1, y, to), "own")

    def item(code):
        return "AB"[code % 2], code // 4, code // 2 % 2

    def pass_token(step):
        if step:
            pl.semaphore_wait(token.at[step - 1], 2)
        if step < 3:
            for d in (1, -1):
                to = dev(x, 1, yat(d), z)
                pl.semaphore_signal(token.at[step], inc=1, device_id=to, device_id_type=MESH)

    def begin(zz):
        loaded(pb.at[0, 0:2], "own")
        pl.semaphore_wait(barrier, receivers(zz) + (jnp.where(apart, 0, 1) if zz == 0 else 1))
        for early_plane, late_plane in LINKS.items():
            if late_plane == zz:
                to = p_dev(y, early_plane)
                pl.semaphore_signal(go_late, inc=1, device_id=to, device_id_type=MESH)
        for kc in (0, 1):
            send(b_send.at[kc], pb.at[lo, zz, kc], ("p", zz, "B", zz, kc), dev(x, 1, mate, zz), "own")
            for to in TREE[zz][zz]:
                if not (zz < EARLY <= to):
                    start(kc, zz, to)

    def pass_on(zz):
        steps, held, count = [], [], len(WAITS[zz])

        def late_planes():
            pl.semaphore_wait(go_late, 1)
            for kc in (0, 1):
                for to in TREE[zz][zz]:
                    if zz < EARLY <= to:
                        start(kc, zz, to)

        def one(typ, src, kc, targets):
            arrived(pb.at[lane[typ], src, kc], "p", zz, typ, src, kc)
            for to in targets:
                hop(typ, src, kc, zz, to)

        for n, code in enumerate(WAITS[zz]):
            if n in (count // 3, 2 * count // 3):
                steps.append(functools.partial(pass_token, 1 if n == count // 3 else 2))
            if code < 0:
                steps.append(late_planes)
                steps += [functools.partial(hop, *what) for what in held]
                held = None
                continue
            typ, src, kc = item(code)
            wait = [to for to in TREE[src][zz] if zz < EARLY <= to and held is not None]
            if wait:
                held += [(typ, src, kc, zz, to) for to in wait]
            steps.append(functools.partial(one, typ, src, kc, [to for to in TREE[src][zz] if to not in wait]))
        return steps

    def run(steps):
        for step in steps:
            step()

    def probe_sent(zz):
        sent(pb.at[0, 0 : len(TREE[zz][zz]) + 1], "own")
        sent(pb.at[0, 0 : len(TREE[zz][zz])], "twin")
        passed = [src for src in TREE if src != zz and TREE[src].get(zz)]
        count = sum(len(TREE[src][zz]) for src in passed)
        assert count <= NZ
        sent(pb.at[:, 0:count], "relay")

    @pl.when(core == 1)
    def _():
        def prepare(i):
            loaded(pb.at[0], ("in", i))
            out_s[i] = (v_pg[i].astype(F32) + v_comp[i]).astype(BF16)

        def push(i):
            send(out_s.at[i], out_s.at[i], ("w", "push", i), w_dev, "push")

        soon = z < SOON

        @pl.when(soon)
        def _():
            for i in range(4):
                prepare(i)

        for zz in range(NZ):
            pl.when(z == zz)(lambda zz=zz: begin(zz))
        pass_token(0)

        @pl.when(apart)
        def _():
            pl.semaphore_wait(go, 1)

        @pl.when(soon)
        def _():
            for i in range(4):
                push(i)

        @pl.when(jnp.logical_not(soon))
        def _():
            for i in range(4):
                prepare(i)
                push(i)

        loaded(v_comp.at[0], "state")
        q_s[...] = prm[...] - (RATE * NEST * NEST) * mom[...]
        send(q_s, q_s, ("w", "q"), w_dev, "q")
        for zz in range(NZ):
            steps = pass_on(zz)
            pl.when(z == zz)(functools.partial(run, steps))

        near = z // HALF
        first = sum(jnp.where(z == zz, FAR[zz], 0) for zz in range(NZ))
        y_at = SHARED + keys["t"]("y", 0)
        assert keys["t"]("y", 1) == y_at - SHARED + 1

        pass_token(3)
        for kc in (0, 1):
            arrived(w.at[kc], "t", "w", kc)
            w_t[kc] = w[kc].reshape(256, KC).T

        def wait_blocks(zz, phase):
            stop = [src for src in TREE if src != zz and turn(src, zz) == phase and not TREE[src].get(zz)]
            if stop:
                arrived(pb.at[:, 0 : len(stop)], "t", "in", phase)

        def put(src, dst, c, to):
            pltpu.make_async_remote_copy(
                src_ref=src, dst_ref=dst, send_sem=ssem("y"), recv_sem=recv_sem.at[y_at + c],
                device_id=dev(x, 1, to, z), device_id_type=MESH,
            ).start()

        def multiply(phase):
            h = 1 - near if phase else near
            q = (None, first, 1 - first)[phase]
            planes = HALF // 2 if phase else HALF
            for zz in range(NZ):
                pl.when(z == zz)(functools.partial(wait_blocks, zz, phase))
            acc = jnp.zeros((2 * planes * 16, 256), F32)
            for kc in (0, 1):
                at = h * HALF + (q * planes if phase else 0)
                rows = pb[:, pl.ds(at, planes), kc].reshape(2 * planes * 16, KC)
                acc += jnp.dot(rows, w_t[kc], preferred_element_type=F32)
            for lp in (0, 1):
                for lw in (0, 1):
                    n = planes * 16
                    piece = acc[lp * n : lp * n + n, lw * 128 : lw * 128 + 128].astype(BF16)
                    if phase:
                        part[1, lp, lw, q] = piece.reshape(3, 16, 128)
                    else:
                        part[0, lp, lw] = piece.reshape(2, 3, 16, 128)
            for d in (4, 3, 5, 2, 6, 1, 7):
                to = yat(d)

                @pl.when(to // 2 % 2 == h)
                def _():
                    if phase:
                        put(part.at[1, to // 4, to % 2, q], y_in.at[q, y], q, to)
                    else:
                        put(part.at[0, to // 4, to % 2], y_in.at[:, y], 0, to)

            @pl.when(y // 2 % 2 == h)
            def _():
                if phase:
                    y_in[q, y] = part[1, y // 4, y % 2, q]
                else:
                    y_in[:, y] = part[0, y // 4, y % 2]

        for phase in (0, 1, 2):
            multiply(phase)

        def share(c, like, quarters, at):
            pltpu.make_async_remote_copy(
                src_ref=like, dst_ref=like, send_sem=send_sem.at[0], recv_sem=recv_sem.at[y_at + c],
                device_id=me, device_id_type=MESH,
            ).wait_recv()
            for q in quarters:
                total = y_in[q, 0].astype(F32)
                for i in range(1, NY):
                    total += y_in[q, i].astype(F32)
                outb[pl.ds(3 * q, 3), x] = total.astype(BF16)
            mine = outb.at[at, x]
            for d in (2, 1, 3):
                for cc in (1, 0):
                    send(mine, mine, ("t", "out"), dev(xat(d), cc, y, z), "out")
            send(mine, mine, ("t", "out"), dev(x, 0, y, z), "out")

        @pl.when(y // 2 % 2 == near)
        def _():
            share(0, y_in.at[:, 0:7], (0, 1), slice(None))

        @pl.when(y // 2 % 2 != near)
        def _():
            for c in (first, 1 - first):
                share(c, y_in.at[0, 0:7], (c,), pl.ds(3 * c, 3))

    @pl.when(core == 1)
    def _():
        arrived(sum_s, "t", "sum")
        for i, (kind, kc) in enumerate(ORDER):
            at = columns(kind, kc)
            avg = sum_s[i]
            m = NEST * mom[:, at] + avg
            n_mom[:, at] = m
            n_prm[:, at] = prm[:, at] - RATE * (avg + NEST * m)
        sent(out_s, "push")
        sent(q_s, "q")
        for zz in range(NZ):
            pl.when(z == zz)(lambda zz=zz: probe_sent(zz))

    @pl.when(core == 0)
    def _():
        sent(pb.at[0], "rs")
        sent(pb.at[:, 0:10], "ag")
        sent(sum_s, "sum")

    @pl.when(core == 1)
    def _():
        sent(y_in.at[:, 0:7], "y")
        sent(y_in.at[:, 0:7], "out")
        arrived(y_in.at[:, 0:3], "t", "out")

    @pl.when(core == 0)
    def _():
        arrived(y_in.at[:, 0:4], "t", "out")

    assert len(keys["w"].at) <= SHARED and len(keys["t"].at) <= N_RECV - SHARED
    assert max(len(k.at) for k in sk.values()) <= N_SEND and len(lk.at) <= N_LOCAL


def store(a, b, c, a_out, b_out, c_out, sem):
    copies = [
        pltpu.make_async_copy(src, dst, sem.at[i])
        for i, (src, dst) in enumerate(((a, a_out), (b, b_out), (c, c_out)))
    ]
    for cp in copies:
        cp.start()
    for cp in copies:
        cp.wait()


def per_device(pseudo_grad, compensation, params, momentum, probe):
    any_space = pl.BlockSpec(memory_space=pl.ANY)
    vmem = pl.BlockSpec(memory_space=pltpu.VMEM)
    shapes = (
        jax.ShapeDtypeStruct((16, K), F32),
        jax.ShapeDtypeStruct((16, K), F32),
        jax.ShapeDtypeStruct((6, NX, 16, 128), BF16),
    )
    outs = pl.pallas_call(
        kernel,
        out_shape=tuple(pltpu.VMEM(s.shape, s.dtype) for s in shapes),
        in_specs=[any_space] * 5,
        out_specs=[vmem] * 3,
        scratch_shapes=[
            pltpu.VMEM((4, 8, 16, KC), BF16),
            pltpu.VMEM((4, 8, 16, KC), F32),
            pltpu.VMEM((4, 8, 16, KC), BF16),
            pltpu.VMEM((4, 8, 16, KC), BF16),
            pltpu.VMEM((4, 2, 16, KC), BF16),
            pltpu.VMEM((4, 2, 2, 16, KC), BF16),
            pltpu.VMEM((4, 2, 16, KC), BF16),
            pltpu.VMEM((16, K), F32),
            pltpu.VMEM((16, K), F32),
            pltpu.VMEM((16, K), F32),
            pltpu.VMEM((4, 16, KC), F32),
            pltpu.VMEM((2, 2, NX, 2, 16, KC), BF16),
            pltpu.VMEM((2, KC, 256), BF16),
            pltpu.VMEM((4, 2, 16, KC), BF16),
            pltpu.VMEM((2, 2, 2, 16, KC), BF16),
            pltpu.VMEM((2, NZ, 2, 16, KC), BF16),
            pltpu.VMEM((2, 16, KC), BF16),
            pltpu.VMEM((2, 2, 2, 2, 3, 16, 128), BF16),
            pltpu.VMEM((2, NY, 3, 16, 128), BF16),
            pltpu.SemaphoreType.DMA((N_SEND,)),
            pltpu.SemaphoreType.DMA((N_RECV,)),
            pltpu.SemaphoreType.DMA((N_LOCAL,)),
            pltpu.SemaphoreType.REGULAR,
            pltpu.SemaphoreType.REGULAR,
            pltpu.SemaphoreType.REGULAR,
            pltpu.SemaphoreType.REGULAR((3,)),
        ],
        compiler_params=pltpu.CompilerParams(
            collective_id=0, has_side_effects=True, vmem_limit_bytes=60 * 2**20
        ),
    )(
        pseudo_grad.reshape(8, 16, K),
        compensation.reshape(8, 16, K),
        params,
        momentum,
        probe.reshape(NX, 16, K),
    )
    new_params, new_momentum, out = pl.pallas_call(
        store,
        out_shape=shapes,
        in_specs=[any_space] * 3,
        out_specs=[any_space] * 3,
        scratch_shapes=[pltpu.SemaphoreType.DMA((3,))],
        compiler_params=pltpu.CompilerParams(vmem_limit_bytes=2**20),
    )(*outs)
    return new_params, new_momentum, out.reshape(384, 128)


def solution(mesh):
    in_specs = (
        P("replica", "fsdp", "tensor"),
        P("replica", "fsdp", "tensor"),
        P(("fsdp", "replica"), "tensor"),
        P(("fsdp", "replica"), "tensor"),
        P("fsdp", "tensor"),
    )
    out_specs = (
        P(("fsdp", "replica"), "tensor"),
        P(("fsdp", "replica"), "tensor"),
        P("tensor", "fsdp"),
    )
    return jax.shard_map(
        per_device, mesh=mesh, in_specs=in_specs, out_specs=out_specs, check_vma=False
    )
```

```python
import functools

import jax
import jax.numpy as jnp
from jax import lax
from jax.experimental import pallas as pl
from jax.experimental.pallas import tpu as pltpu
from jax.sharding import PartitionSpec as P

MESH = pl.DeviceIdType.MESH
RATE = 0.7
NEST = 0.9
F32, BF16 = jnp.float32, jnp.bfloat16

NX, NY, NZ = 4, 8, 12
K = 4608
KC = K // 4
HALF = NZ // 2
EARLY = 6
ORDER = (("P", 0), ("P", 1), ("O", 0), ("O", 1))
TREE = {
    0: {0: (1, 11,), 1: (2,), 2: (3,), 3: (4,), 4: (5,), 7: (6,), 9: (7, 8, 10,), 11: (9,)},
    1: {0: (11,), 1: (2, 0,), 2: (3,), 3: (4,), 4: (5,), 5: (6,), 6: (7,), 9: (8,), 10: (9,), 11: (10,)},
    2: {0: (11,), 2: (0, 1, 3,), 3: (4,), 4: (5,), 5: (6,), 6: (7,), 9: (8,), 10: (9,), 11: (10,)},
    3: {0: (11,), 1: (0,), 3: (1, 2, 4,), 4: (5,), 5: (6,), 6: (7,), 7: (8,), 10: (9,), 11: (10,)},
    4: {0: (11, 1,), 2: (0,), 4: (2, 3, 5,), 5: (6,), 6: (7,), 7: (9, 8,), 11: (10,)},
    5: {0: (11,), 1: (0, 2,), 3: (1, 4,), 5: (3, 6,), 6: (7,), 7: (8,), 8: (9,), 11: (10,)},
    6: {1: (0,), 3: (1, 2,), 4: (3, 5,), 6: (7, 4,), 7: (8, 9,), 9: (10,), 10: (11,)},
    7: {3: (4, 2, 1,), 5: (3, 6,), 7: (5, 9,), 8: (10,), 9: (8, 11,), 11: (0,)},
    8: {0: (1, 11,), 3: (2,), 4: (3, 5,), 6: (4,), 8: (6, 10, 9,), 9: (7,), 10: (0,)},
    9: {1: (2, 0,), 2: (3,), 4: (5,), 6: (4,), 8: (6, 7,), 9: (8, 11,), 11: (1, 10,)},
    10: {0: (1,), 1: (2,), 2: (3,), 5: (4, 6,), 7: (5,), 8: (7, 9,), 9: (11,), 10: (0, 8,)},
    11: {1: (0, 2,), 2: (3,), 5: (4,), 6: (7, 5,), 8: (9, 6,), 10: (8,), 11: (10, 1,)},
}
WAITS = (
    (-1, 1, 4, 3, 14, 10, 7, 9, 5, 40, 6, 8, 11, 12, 15, 42, 13, 43, 18, 41, 16, 22, 17, 21, 19, 32, 20, 34, 33, 23, 35),
    (5, 7, 2, 0, 14, 12, 15, 13, 44, 20, 1, 46, 45, 3, 22, 21, 47, 23, 42, 24, 26, 36, 38, 37, 39, 43, 25, 41, 40, 27),
    (4, 7, 5, 6, 2, 9, 0, 11, 16, 18, 17, 19, 44, 1, 3, 46, 45, 47, 36, 42, 38, 39, 37, 41, 40, 43),
    (13, 15, 8, 6, 20, 10, 22, 4, 5, 9, 7, 2, 21, 11, 23, 24, 0, 26, 28, 25, 27, 30, 29, 31, 1, 3, 34, 32, 35, 33),
    (19, 17, 13, 15, 24, 26, 12, 14, 25, 27, 8, 9, 10, 4, 11, 7, 5, 6, 32, 2, 34, 35, 33, 38, 0, 36, 1, 3, 39, 37),
    (-1, 21, 23, 17, 18, 28, 16, 13, 30, 19, 29, 15, 12, 14, 31, 9, 8, 10, 4, 11, 7, 42, 40, 6, 5, 43, 41, 46, 44, 45, 47),
    (25, 27, 34, 22, 21, 32, 35, 18, 17, 23, 33, 19, 16, 20, 14, 38, 12, 13, 36, 15, 37, 9, 39, 10, 8, 11, 46, 44, 45, 5, 4, 47, 6, 7),
    (29, 31, 27, 26, 24, 40, 42, 25, 21, 22, 43, 41, 23, 18, 17, 19, 20, 16, 13, 12, 15, 1, 14, 0, 2, 3),
    (35, 33, 40, 42, 36, 38, 43, 41, 37, 39, 46, 28, 44, 45, 21, 29, 47, 30, 22, 23, 20, 31),
    (37, 39, 29, 28, 31, 30, 1, 27, 0, 24, 42, 25, 43, 40, 2, 3, 32, 41, 26, 33, 34, 35, 9, 5, 8, 4, 11, 6, 10, 7),
    (43, 41, 46, 44, 45, 47, 32, 34, 33, 35, 9, 6, 5, 8, 4, 11, 10, 14, 7, 27, 12, 13, 15, 24, 25, 26),
    (45, 47, 0, 1, 2, 36, 38, 37, 39, 9, 4, 3, 6, 5, 8, 7, 29, 12, 11, 10, 31, 28, 14, 30, 13, 16, 15, 18, 19, 17, 20, 22, 21, 23),
)
LINKS = {0: NZ - 1, EARLY - 1: EARLY}
FAR = (1, 1, 0, 0, 0, 0, 1, 1, 1, 0, 0, 0)
TURN = {0: 25, 2: 21}
SOON = 5
SHARED = max(len(order) for order in WAITS)
N_RECV, N_SEND, N_LOCAL = SHARED + 9, 7, 6


class Keys:
    def __init__(self):
        self.at = {}

    def __call__(self, *key):
        return self.at.setdefault(key, len(self.at))


def kernel(
    pg_hbm, comp_hbm, prm_hbm, mom_hbm, probe_hbm,
    n_prm, n_mom, outb,
    v_pg, v_comp, out_s, cs, r_opp, r_fin, t_acc, prm, mom, q_s, sum_s,
    w, w_t, wn, r_ag, pb, b_send, part, y_in,
    send_sem, recv_sem, loc_sem, go, go_late, both, token,
):
    rep = lax.axis_index("replica")
    fs = lax.axis_index("fsdp")
    t = lax.axis_index("tensor")
    x, core = rep // 2, rep % 2
    lo, z = fs // NZ, fs % NZ
    other = 1 - lo
    y = t * 2 + lo
    mate = t * 2 + other

    def dev(x_, core_, y_, z_):
        return (x_ * 2 + core_, (y_ % 2) * NZ + z_, y_ // 2)

    def xat(d):
        return lax.rem(x + d + NX, NX)

    def yat(d):
        return lax.rem(y + d + NY, NY)

    def zat(d):
        return lax.rem(z + d + NZ, NZ)

    w_dev, h_dev, me = dev(x, 0, y, z), dev(x, 1, y, z), dev(x, core, y, z)

    keys, sk, lk = {group: Keys() for group in "wt"}, {core_: Keys() for core_ in (0, 1)}, Keys()

    def rsem(group, *key):
        if group == "p":
            zz, typ, src, kc = key
            return recv_sem.at[WAITS[zz].index(src * 4 + kc * 2 + "AB".index(typ))]
        at = keys[group](*key)
        return recv_sem.at[SHARED + at if group == "t" else at]

    def ssem(group):
        return send_sem.at[sk[0 if group in ("rs", "ag", "sum") else 1](group)]

    def send(src, dst, key, to, group):
        pltpu.make_async_remote_copy(
            src_ref=src, dst_ref=dst, send_sem=ssem(group), recv_sem=rsem(*key),
            device_id=to, device_id_type=MESH,
        ).start()

    def arrived(like, *key):
        pltpu.make_async_remote_copy(
            src_ref=like, dst_ref=like, send_sem=send_sem.at[0], recv_sem=rsem(*key),
            device_id=me, device_id_type=MESH,
        ).wait_recv()

    def sent(like, group):
        pltpu.make_async_remote_copy(
            src_ref=like, dst_ref=like, send_sem=ssem(group), recv_sem=recv_sem.at[0],
            device_id=me, device_id_type=MESH,
        ).wait_send()

    def load(src, dst, key):
        pltpu.make_async_copy(src, dst, loc_sem.at[lk(key)]).start()

    def loaded(like, key):
        pltpu.make_async_remote_copy(
            src_ref=like, dst_ref=like, send_sem=send_sem.at[0], recv_sem=loc_sem.at[lk(key)],
            device_id=me, device_id_type=MESH,
        ).wait_recv()

    def columns(kind, kc):
        half = lo if kind == "O" else other
        return pl.ds(pl.multiple_of((half * 2 + kc) * KC, KC), KC)

    def load_chunk(i):
        at = columns(*ORDER[i])
        load(pg_hbm.at[:, :, at], v_pg.at[i], ("in", i))
        load(comp_hbm.at[:, :, at], v_comp.at[i], ("in", i))

    barrier = pltpu.get_barrier_semaphore()

    def greet(to):
        pl.semaphore_signal(barrier, inc=1, device_id=to, device_id_type=MESH)

    def p_dev(y_, zz):
        return dev(x, 1, y_, zz)

    def turn(src, zz):
        if src // HALF == zz // HALF:
            return 0
        return 1 if src % HALF // 3 == FAR[zz] else 2

    def senders(zz):
        found = {(1, zz): mate, (2, zz): jnp.where(lo == 1, yat(1), yat(-1))}
        for src in TREE:
            for q, to in TREE[src].items():
                if zz in to:
                    found[0, q] = y
        if zz in LINKS:
            found[0, LINKS[zz]] = y
        return [(found[key], key[1]) for key in sorted(found)]

    late = z >= EARLY
    apart = jnp.logical_and(z == 0, jnp.logical_and(x == 0, y == 0))

    @pl.when(core == 1)
    def _():
        @pl.when(jnp.logical_not(late))
        def _():
            load_chunk(0)

        greet(w_dev)
        for zz in range(NZ):

            @pl.when(z == zz)
            def _():
                for yy, q in senders(zz):
                    if not (q < EARLY <= zz):
                        greet(p_dev(yy, q))

        for kc in (0, 1):
            load(probe_hbm.at[x, :, columns("O", kc)], pb.at[lo, z, kc], "own")
            load(probe_hbm.at[x, :, columns("P", kc)], b_send.at[kc], "own")

        @pl.when(late)
        def _():
            load_chunk(0)

    @pl.when(core == 0)
    def _():
        load_chunk(0)
        for d in (-1, 1):
            greet(dev(xat(d), 0, y, z))
        for d in (-1, 1):
            greet(dev(xat(d), 0, mate, z))
        greet(dev(x, 0, mate, z))

        @pl.when(jnp.logical_not(apart))
        def _():
            greet(h_dev)

    for i in (1, 2, 3):
        load_chunk(i)
    load(prm_hbm, prm, "state")
    load(mom_hbm, mom, "state")

    @pl.when(core == 0)
    def _():
        right, left, far = xat(1), xat(-1), xat(2)
        rdev, ldev = dev(right, 0, y, z), dev(left, 0, y, z)
        pl.semaphore_wait(barrier, 6)

        @pl.when(apart)
        def _():
            pl.semaphore_signal(go, inc=1, device_id=h_dev, device_id_type=MESH)

        pl.semaphore_signal(both, inc=1, device_id=dev(x, 0, mate, z), device_id_type=MESH)

        def chip_sum(i, s):
            return v_pg[i, s].astype(F32) + v_comp[i, s] + out_s[i, s].astype(F32)

        def opposite(i):
            loaded(pb.at[0], ("in", i))
            arrived(out_s.at[i], "w", "push", i)
            for side, to in ((1, rdev), (0, ldev)):
                s = far * 2 + side
                cs[i, s] = chip_sum(i, s).astype(BF16)
                send(cs.at[i, s], r_opp.at[i, side], ("w", "opp", i, side), to, "rs")

        def direct(i):
            for side, to, xx in ((0, rdev, right), (1, ldev, left)):
                s = xx * 2 + side
                cs[i, s] = chip_sum(i, s).astype(BF16)
                send(cs.at[i, s], r_fin.at[i, side, 0], ("w", "fin", i), to, "rs")

        def on_the_way(i):
            for side, to, xx in ((1, rdev, right), (0, ldev, left)):
                s = xx * 2 + side
                arrived(r_opp.at[i, side], "w", "opp", i, side)
                t_acc[i, side] = (chip_sum(i, s) + r_opp[i, side].astype(F32)).astype(BF16)
                send(t_acc.at[i, side], r_fin.at[i, side, 1], ("w", "fin", i), to, "rs")

        opposite(0)
        opposite(1)
        direct(0)
        direct(1)
        opposite(2)
        opposite(3)
        pl.semaphore_wait(both, 1)
        on_the_way(0)
        on_the_way(1)
        direct(2)
        direct(3)
        on_the_way(2)
        on_the_way(3)

        loaded(v_comp.at[0], "state")
        arrived(q_s, "w", "q")

        def gather(src, kc, kind, first):
            y_, rel = (y, 0) if kind == "O" else (mate, 1)
            for side, xx in ((1, right), (0, left)):
                if first:
                    send(src.at[side], r_ag.at[kc, rel, side], ("w", "ag", kc, rel, side), dev(xx, 0, y_, z), "ag")
            if not first:
                for side, xx in ((0, right), (1, left), (0, x), (1, x)):
                    send(src.at[side], w.at[kc, lo, x, side], ("t", "w", kc), dev(xx, 1, y_, z), "ag")

        def relay(kc, rel):
            f = other if rel else lo
            for side, to, xx in ((1, right, left), (0, left, right)):
                ref = r_ag.at[kc, rel, side]
                arrived(ref, "w", "ag", kc, rel, side)
                for x_ in (to, x):
                    send(ref, w.at[kc, f, xx, side], ("t", "w", kc), dev(x_, 1, y, z), "ag")

        def block(i):
            kind, kc = ORDER[i]
            return wn.at[i], kc, kind

        for i, (kind, kc) in enumerate(ORDER):
            at = columns(kind, kc)
            arrived(r_fin.at[i], "w", "fin", i)

            def average(side):
                return (
                    chip_sum(i, x * 2 + side)
                    + r_fin[i, side, 0].astype(F32)
                    + r_fin[i, side, 1].astype(F32)
                ) * 0.125

            avg = average(0)
            m = NEST * mom[:, at] + avg
            new = prm[:, at] - RATE * (avg + NEST * m)
            n_mom[:, at] = m
            n_prm[:, at] = new
            wn[i, 0] = new.astype(BF16)
            avg = average(1)
            sum_s[i] = avg
            wn[i, 1] = (q_s[:, at] - (RATE * (1 + NEST)) * avg).astype(BF16)
            gather(*block(i), True)
            if i == 1:
                gather(*block(0), False)
        for i in (2, 1, 3):
            gather(*block(i), False)
        for i in range(4):
            send(sum_s.at[i], sum_s.at[i], ("t", "sum"), h_dev, "sum")

        relay(0, 1)
        relay(1, 1)
        relay(0, 0)
        relay(1, 0)

    lane = {"A": lo, "B": other}

    def receivers(zz):
        found = {(zz, 1), (zz, 2)}
        for src in TREE:
            for to in TREE[src].get(zz, ()):
                if not (zz < EARLY <= to):
                    found.add((to, 0))
        for early_plane, late_plane in LINKS.items():
            if late_plane == zz:
                found.add((early_plane, 0))
        return len(found)

    def hop(typ, src, kc, zz, to):
        ref = pb.at[lane[typ], src, kc]
        target = dev(x, 1, y, to)
        key = ("p", to, typ, src, kc) if TREE[src].get(to) else ("t", "in", turn(src, to))
        send(ref, ref, key, target, "twin" if src == zz else "relay")

    def start(kc, zz, to):
        ref = pb.at[lo, zz, kc]
        key = ("p", to, "A", zz, kc) if TREE[zz].get(to) else ("t", "in", turn(zz, to))
        send(ref, ref, key, dev(x, 1, y, to), "own")

    def item(code):
        return "AB"[code % 2], code // 4, code // 2 % 2

    def pass_token(step):
        if step:
            pl.semaphore_wait(token.at[step - 1], 2)
        if step < 3:
            for d in (1, -1):
                to = dev(x, 1, yat(d), z)
                pl.semaphore_signal(token.at[step], inc=1, device_id=to, device_id_type=MESH)

    def begin(zz):
        loaded(pb.at[0, 0:2], "own")
        pl.semaphore_wait(barrier, receivers(zz) + (jnp.where(apart, 0, 1) if zz == 0 else 1))
        for early_plane, late_plane in LINKS.items():
            if late_plane == zz:
                to = p_dev(y, early_plane)
                pl.semaphore_signal(go_late, inc=1, device_id=to, device_id_type=MESH)
        for kc in (0, 1):
            send(b_send.at[kc], pb.at[lo, zz, kc], ("p", zz, "B", zz, kc), dev(x, 1, mate, zz), "own")
            for to in TREE[zz][zz]:
                if not (zz < EARLY <= to):
                    start(kc, zz, to)

    def pass_on(zz):
        steps, held, count = [], [], len(WAITS[zz])

        def late_planes():
            pl.semaphore_wait(go_late, 1)
            for kc in (0, 1):
                for to in TREE[zz][zz]:
                    if zz < EARLY <= to:
                        start(kc, zz, to)

        def one(typ, src, kc, targets):
            arrived(pb.at[lane[typ], src, kc], "p", zz, typ, src, kc)
            for to in targets:
                hop(typ, src, kc, zz, to)

        for n, code in enumerate(WAITS[zz]):
            if n == TURN.get(zz):
                steps.append(weights_soon)
            if n in (count // 3, 2 * count // 3):
                steps.append(functools.partial(pass_token, 1 if n == count // 3 else 2))
            if code < 0:
                steps.append(late_planes)
                steps += [functools.partial(hop, *what) for what in held]
                held = None
                continue
            typ, src, kc = item(code)
            wait = [to for to in TREE[src][zz] if zz < EARLY <= to and held is not None]
            if wait:
                held += [(typ, src, kc, zz, to) for to in wait]
            steps.append(functools.partial(one, typ, src, kc, [to for to in TREE[src][zz] if to not in wait]))
        return steps

    def weights():
        for kc in (0, 1):
            arrived(w.at[kc], "t", "w", kc)
            w_t[kc] = w[kc].reshape(256, KC).T

    turned = jnp.logical_or(jnp.logical_and(z == 0, y >= 2), z == 2)

    def weights_soon():
        pl.when(turned)(weights)

    def run(steps):
        for step in steps:
            step()

    def probe_sent(zz):
        sent(pb.at[0, 0 : len(TREE[zz][zz]) + 1], "own")
        sent(pb.at[0, 0 : len(TREE[zz][zz])], "twin")
        passed = [src for src in TREE if src != zz and TREE[src].get(zz)]
        count = sum(len(TREE[src][zz]) for src in passed)
        assert count <= NZ
        sent(pb.at[:, 0:count], "relay")

    @pl.when(core == 1)
    def _():
        def prepare(i):
            loaded(pb.at[0], ("in", i))
            out_s[i] = (v_pg[i].astype(F32) + v_comp[i]).astype(BF16)

        def push(i):
            send(out_s.at[i], out_s.at[i], ("w", "push", i), w_dev, "push")

        soon = z < SOON

        @pl.when(soon)
        def _():
            for i in range(4):
                prepare(i)

        for zz in range(NZ):
            pl.when(z == zz)(lambda zz=zz: begin(zz))
        pass_token(0)

        @pl.when(apart)
        def _():
            pl.semaphore_wait(go, 1)

        @pl.when(soon)
        def _():
            for i in range(4):
                push(i)

        @pl.when(jnp.logical_not(soon))
        def _():
            for i in range(4):
                prepare(i)
                push(i)

        loaded(v_comp.at[0], "state")
        q_s[...] = prm[...] - (RATE * NEST * NEST) * mom[...]
        send(q_s, q_s, ("w", "q"), w_dev, "q")
        for zz in range(NZ):
            steps = pass_on(zz)
            pl.when(z == zz)(functools.partial(run, steps))

        near = z // HALF
        first = sum(jnp.where(z == zz, FAR[zz], 0) for zz in range(NZ))
        y_at = SHARED + keys["t"]("y", 0)
        assert keys["t"]("y", 1) == y_at - SHARED + 1

        pass_token(3)
        pl.when(jnp.logical_not(turned))(weights)

        def wait_blocks(zz, phase):
            stop = [src for src in TREE if src != zz and turn(src, zz) == phase and not TREE[src].get(zz)]
            if stop:
                arrived(pb.at[:, 0 : len(stop)], "t", "in", phase)

        def put(src, dst, c, to):
            pltpu.make_async_remote_copy(
                src_ref=src, dst_ref=dst, send_sem=ssem("y"), recv_sem=recv_sem.at[y_at + c],
                device_id=dev(x, 1, to, z), device_id_type=MESH,
            ).start()

        def multiply(phase):
            h = 1 - near if phase else near
            q = (None, first, 1 - first)[phase]
            planes = HALF // 2 if phase else HALF
            for zz in range(NZ):
                pl.when(z == zz)(functools.partial(wait_blocks, zz, phase))
            acc = jnp.zeros((2 * planes * 16, 256), F32)
            for kc in (0, 1):
                at = h * HALF + (q * planes if phase else 0)
                rows = pb[:, pl.ds(at, planes), kc].reshape(2 * planes * 16, KC)
                acc += jnp.dot(rows, w_t[kc], preferred_element_type=F32)
            for lp in (0, 1):
                for lw in (0, 1):
                    n = planes * 16
                    piece = acc[lp * n : lp * n + n, lw * 128 : lw * 128 + 128].astype(BF16)
                    if phase:
                        part[1, lp, lw, q] = piece.reshape(3, 16, 128)
                    else:
                        part[0, lp, lw] = piece.reshape(2, 3, 16, 128)
            for d in (4, 3, 5, 2, 6, 1, 7):
                to = yat(d)

                @pl.when(to // 2 % 2 == h)
                def _():
                    if phase:
                        put(part.at[1, to // 4, to % 2, q], y_in.at[q, y], q, to)
                    else:
                        put(part.at[0, to // 4, to % 2], y_in.at[:, y], 0, to)

            @pl.when(y // 2 % 2 == h)
            def _():
                if phase:
                    y_in[q, y] = part[1, y // 4, y % 2, q]
                else:
                    y_in[:, y] = part[0, y // 4, y % 2]

        for phase in (0, 1, 2):
            multiply(phase)

        def share(c, like, quarters, at):
            pltpu.make_async_remote_copy(
                src_ref=like, dst_ref=like, send_sem=send_sem.at[0], recv_sem=recv_sem.at[y_at + c],
                device_id=me, device_id_type=MESH,
            ).wait_recv()
            for q in quarters:
                total = y_in[q, 0].astype(F32)
                for i in range(1, NY):
                    total += y_in[q, i].astype(F32)
                outb[pl.ds(3 * q, 3), x] = total.astype(BF16)
            mine = outb.at[at, x]
            for d in (2, 1, 3):
                for cc in (1, 0):
                    send(mine, mine, ("t", "out"), dev(xat(d), cc, y, z), "out")
            send(mine, mine, ("t", "out"), dev(x, 0, y, z), "out")

        @pl.when(y // 2 % 2 == near)
        def _():
            share(0, y_in.at[:, 0:7], (0, 1), slice(None))

        @pl.when(y // 2 % 2 != near)
        def _():
            for c in (first, 1 - first):
                share(c, y_in.at[0, 0:7], (c,), pl.ds(3 * c, 3))

    @pl.when(core == 1)
    def _():
        arrived(sum_s, "t", "sum")
        for i, (kind, kc) in enumerate(ORDER):
            at = columns(kind, kc)
            avg = sum_s[i]
            m = NEST * mom[:, at] + avg
            n_mom[:, at] = m
            n_prm[:, at] = prm[:, at] - RATE * (avg + NEST * m)
        sent(out_s, "push")
        sent(q_s, "q")
        for zz in range(NZ):
            pl.when(z == zz)(lambda zz=zz: probe_sent(zz))

    @pl.when(core == 0)
    def _():
        sent(pb.at[0], "rs")
        sent(pb.at[:, 0:10], "ag")
        sent(sum_s, "sum")

    @pl.when(core == 1)
    def _():
        sent(y_in.at[:, 0:7], "y")
        sent(y_in.at[:, 0:7], "out")
        arrived(y_in.at[:, 0:3], "t", "out")

    @pl.when(core == 0)
    def _():
        arrived(y_in.at[:, 0:4], "t", "out")

    assert len(keys["w"].at) <= SHARED and len(keys["t"].at) <= N_RECV - SHARED
    assert max(len(k.at) for k in sk.values()) <= N_SEND and len(lk.at) <= N_LOCAL


def store(a, b, c, a_out, b_out, c_out, sem):
    copies = [
        pltpu.make_async_copy(src, dst, sem.at[i])
        for i, (src, dst) in enumerate(((a, a_out), (b, b_out), (c, c_out)))
    ]
    for cp in copies:
        cp.start()
    for cp in copies:
        cp.wait()


def per_device(pseudo_grad, compensation, params, momentum, probe):
    any_space = pl.BlockSpec(memory_space=pl.ANY)
    vmem = pl.BlockSpec(memory_space=pltpu.VMEM)
    shapes = (
        jax.ShapeDtypeStruct((16, K), F32),
        jax.ShapeDtypeStruct((16, K), F32),
        jax.ShapeDtypeStruct((6, NX, 16, 128), BF16),
    )
    outs = pl.pallas_call(
        kernel,
        out_shape=tuple(pltpu.VMEM(s.shape, s.dtype) for s in shapes),
        in_specs=[any_space] * 5,
        out_specs=[vmem] * 3,
        scratch_shapes=[
            pltpu.VMEM((4, 8, 16, KC), BF16),
            pltpu.VMEM((4, 8, 16, KC), F32),
            pltpu.VMEM((4, 8, 16, KC), BF16),
            pltpu.VMEM((4, 8, 16, KC), BF16),
            pltpu.VMEM((4, 2, 16, KC), BF16),
            pltpu.VMEM((4, 2, 2, 16, KC), BF16),
            pltpu.VMEM((4, 2, 16, KC), BF16),
            pltpu.VMEM((16, K), F32),
            pltpu.VMEM((16, K), F32),
            pltpu.VMEM((16, K), F32),
            pltpu.VMEM((4, 16, KC), F32),
            pltpu.VMEM((2, 2, NX, 2, 16, KC), BF16),
            pltpu.VMEM((2, KC, 256), BF16),
            pltpu.VMEM((4, 2, 16, KC), BF16),
            pltpu.VMEM((2, 2, 2, 16, KC), BF16),
            pltpu.VMEM((2, NZ, 2, 16, KC), BF16),
            pltpu.VMEM((2, 16, KC), BF16),
            pltpu.VMEM((2, 2, 2, 2, 3, 16, 128), BF16),
            pltpu.VMEM((2, NY, 3, 16, 128), BF16),
            pltpu.SemaphoreType.DMA((N_SEND,)),
            pltpu.SemaphoreType.DMA((N_RECV,)),
            pltpu.SemaphoreType.DMA((N_LOCAL,)),
            pltpu.SemaphoreType.REGULAR,
            pltpu.SemaphoreType.REGULAR,
            pltpu.SemaphoreType.REGULAR,
            pltpu.SemaphoreType.REGULAR((3,)),
        ],
        compiler_params=pltpu.CompilerParams(
            collective_id=0, has_side_effects=True, vmem_limit_bytes=60 * 2**20
        ),
    )(
        pseudo_grad.reshape(8, 16, K),
        compensation.reshape(8, 16, K),
        params,
        momentum,
        probe.reshape(NX, 16, K),
    )
    new_params, new_momentum, out = pl.pallas_call(
        store,
        out_shape=shapes,
        in_specs=[any_space] * 3,
        out_specs=[any_space] * 3,
        scratch_shapes=[pltpu.SemaphoreType.DMA((3,))],
        compiler_params=pltpu.CompilerParams(vmem_limit_bytes=2**20),
    )(*outs)
    return new_params, new_momentum, out.reshape(384, 128)


def solution(mesh):
    in_specs = (
        P("replica", "fsdp", "tensor"),
        P("replica", "fsdp", "tensor"),
        P(("fsdp", "replica"), "tensor"),
        P(("fsdp", "replica"), "tensor"),
        P("fsdp", "tensor"),
    )
    out_specs = (
        P(("fsdp", "replica"), "tensor"),
        P(("fsdp", "replica"), "tensor"),
        P("tensor", "fsdp"),
    )
    return jax.shard_map(
        per_device, mesh=mesh, in_specs=in_specs, out_specs=out_specs, check_vma=False
    )
```
